128 devices in a mesh: row: 8 (over x, core), col: 16 (over z, y).
Axes of the slice: x: 4, y: 4, z: 4, core: 2. Of those that a mesh axis runs over, the one named last changes fastest.
Arguments:
- concentration: float32 [256, 256, 256], P('row', 'col'), may hold values from 0 to 1
Outputs:
- concentration_next: float32 [256, 256, 256], P('row', 'col')
- strain: float32 [6, 256, 256, 256], P(None, 'row', 'col')
- residual_norms: float32 [2], replicated
The draws below stay inside these ranges and needn't reach their ends.
All inputs are finite; a program needn't handle non-finite values.
Results may differ from the reference program's by a relative error of at most 0.0003.
Values sent between devices are 32-bit elements; how exact they have to be, the bound alone decides.
No kernel may reach another device: no remote copies, remote signals or barrier semaphores. Data moves between devices by JAX's collectives and lax.ppermute only.
A program may use at most 192 MiB of HBM per device.

```python
import math
import jax
import jax.numpy as jnp

GRID = 256
ITERS = 2


def draw_concentration(key, part):
    noise_key = jax.random.fold_in(key, 11)
    index = jnp.arange(GRID, dtype=jnp.int32).astype(jnp.float32)
    ramp = 0.1 + 0.2 * (index[:, None, None] + index[None, :, None]) / (2.0 * (GRID - 1))
    rough = jax.random.uniform(noise_key, (GRID, GRID, GRID), jnp.float32, -1.0, 1.0)
    return 0.5 + ramp * rough


def setup_inputs(seed: int = 0) -> dict:
    streams_of = jax.random.split(jax.random.key(seed), 2)
    return {
        "concentration": draw_concentration(jax.random.fold_in(streams_of[1], 71), 0),
    }


FIRST_LOW = 1.0
FIRST_RISE = 0.6
SHEAR_LOW = 0.7
SHEAR_RISE = 0.8
FIRST_REF = 1.3
SHEAR_REF = 1.1
BETA_REF = 2.4 / 3.5
EIGEN_STRAIN = 0.5
WELL_HEIGHT = 1.0
TIME_STEP = 0.5
GRADIENT_ENERGY = 0.5

def moduli(conc):
    return (FIRST_LOW + FIRST_RISE * conc, SHEAR_LOW + SHEAR_RISE * conc)

def polarization(strain, conc):
    first, shear = moduli(conc)
    trace = strain[0] + strain[1] + strain[2]
    normal = (first - FIRST_REF) * trace - (3.0 * first + 2.0 * shear) * EIGEN_STRAIN * conc
    excess = 2.0 * (shear - SHEAR_REF)
    return jnp.stack([normal + excess * strain[0], normal + excess * strain[1], normal + excess * strain[2], excess * strain[3], excess * strain[4], excess * strain[5]])

def green_operator(tau, wave_x, wave_y, wave_z):
    square = wave_x * wave_x + wave_y * wave_y + wave_z * wave_z
    nonzero = square > 0.0
    safe = jnp.where(nonzero, square, 1.0)
    scale = jnp.where(nonzero, 1.0 / (SHEAR_REF * safe), 0.0)
    force_x = tau[0] * wave_x + tau[5] * wave_y + tau[4] * wave_z
    force_y = tau[5] * wave_x + tau[1] * wave_y + tau[3] * wave_z
    force_z = tau[4] * wave_x + tau[3] * wave_y + tau[2] * wave_z
    along = (wave_x * force_x + wave_y * force_y + wave_z * force_z) * (BETA_REF / safe)
    moved_x = scale * (force_x - along * wave_x)
    moved_y = scale * (force_y - along * wave_y)
    moved_z = scale * (force_z - along * wave_z)
    return jnp.stack([-wave_x * moved_x, -wave_y * moved_y, -wave_z * moved_z, -0.5 * (wave_y * moved_z + wave_z * moved_y), -0.5 * (wave_x * moved_z + wave_z * moved_x), -0.5 * (wave_x * moved_y + wave_y * moved_x)])

def potential(strain, conc):
    first, shear = moduli(conc)
    dilation = EIGEN_STRAIN * conc
    part_x = strain[0] - dilation
    part_y = strain[1] - dilation
    part_z = strain[2] - dilation
    trace = part_x + part_y + part_z
    energy = part_x * part_x + part_y * part_y + part_z * part_z + 2.0 * (strain[3] * strain[3] + strain[4] * strain[4] + strain[5] * strain[5])
    chemical = 2.0 * WELL_HEIGHT * conc * (1.0 - conc) * (1.0 - 2.0 * conc)
    return chemical + 0.5 * FIRST_RISE * trace * trace + SHEAR_RISE * energy - EIGEN_STRAIN * (3.0 * first + 2.0 * shear) * trace

def forward_full(fields, half_length):
    return jnp.fft.rfftn(fields, axes=(-3, -2, -1))[..., :half_length]

def inverse_full(spectrum, length):
    padded = jnp.concatenate([spectrum, jnp.zeros(spectrum.shape[:-1] + (1,), spectrum.dtype)], axis=-1)
    return jnp.fft.irfftn(padded, s=(length, length, length), axes=(-3, -2, -1))

def reference(concentration):
    half_length = GRID // 2
    index = jnp.arange(GRID, dtype=jnp.int32)
    signed = jnp.where(index < half_length, index, index - GRID).astype(jnp.float32) * (2.0 * math.pi / GRID)
    wave_x = signed[:, None, None]
    wave_y = signed[None, :, None]
    wave_z = (jnp.arange(half_length, dtype=jnp.int32).astype(jnp.float32) * (2.0 * math.pi / GRID))[None, None, :]
    strain = jnp.zeros((6, GRID, GRID, GRID), jnp.float32)
    norms = []
    for sweep in range(ITERS):
        tau = polarization(strain, concentration)
        updated = inverse_full(green_operator(forward_full(tau, half_length), wave_x, wave_y, wave_z), GRID)
        change = updated - strain
        norms.append(jnp.sqrt(jnp.sum(change * change) / GRID ** 3))
        strain = updated
    drive = potential(strain, concentration)
    square = wave_x * wave_x + wave_y * wave_y + wave_z * wave_z
    spectrum = (forward_full(concentration, half_length) - TIME_STEP * square * forward_full(drive, half_length)) / (1.0 + TIME_STEP * GRADIENT_ENERGY * square * square)
    concentration_next = inverse_full(spectrum, GRID)
    return (concentration_next, strain, jnp.stack(norms))
```

```python
import math
from functools import partial

import jax
import jax.numpy as jnp
import numpy as np
from jax import lax
from jax.experimental import pallas as pl
from jax.experimental.pallas import tpu as pltpu
from jax.sharding import Mesh
from jax.sharding import PartitionSpec as P

AXES = ("row_0", "row_1", "col_0", "col_1")

FIRST_LOW = 1.0
FIRST_RISE = 0.6
SHEAR_LOW = 0.7
SHEAR_RISE = 0.8
FIRST_REF = 1.3
SHEAR_REF = 1.1
BETA_REF = 2.4 / 3.5
EIGEN_STRAIN = 0.5
WELL_HEIGHT = 1.0
TIME_STEP = 0.5
GRADIENT_ENERGY = 0.5

N = 256
HALF = N // 2
ROWS = 8
COLS = 16
DEVICES = ROWS * COLS
LX = N // ROWS
LY = N // COLS
LOW = 8
HIGH = LX // LOW
CELLS = LX * LY
LANES = 128
UNIT = 2.0 * math.pi / N
F32 = jnp.float32
BF16 = jnp.bfloat16
INTERPRET = False


def pieces_of(table, count):
    rest = table.astype(np.float32)
    pieces = []
    for _ in range(count):
        piece = rest.astype(jnp.bfloat16)
        rest = rest - piece.astype(np.float32)
        pieces.append(piece)
    return np.stack(pieces)


def build_tables():
    index = np.arange(N)
    angle = 2.0 * np.pi / N * (index[:, None] * index[None, :] % N)
    cosine = np.cos(angle)
    sine = np.sin(angle)
    ahead = np.concatenate([cosine[:HALF], -sine[:HALF]], axis=0)
    weight = np.where(np.arange(HALF) == 0, 1.0, 2.0) / float(N) ** 3
    back = np.concatenate([cosine[:, :HALF] * weight, -sine[:, :HALF] * weight], axis=1)
    return pieces_of(cosine, 2), pieces_of(sine, 2), pieces_of(ahead, 3), pieces_of(back, 2)


def split(value, count):
    pieces = []
    for i in range(count):
        piece = value.astype(BF16)
        pieces.append(piece)
        if i + 1 < count:
            value = value - piece.astype(F32)
    return pieces


def product(left, right):
    count = len(right)
    total = None
    for order in reversed(range(count)):
        for i in range(order + 1):
            term = jnp.dot(left[i], right[order - i], preferred_element_type=F32)
            total = term if total is None else total + term
    return total


def table(ref):
    return [ref[i] for i in range(ref.shape[0])]


def swap_lanes(parts, granule):
    parts = list(parts)
    axis = parts[0].ndim - 1
    lane = lax.broadcasted_iota(jnp.int32, parts[0].shape, axis)
    step = 1
    while step < len(parts):
        width = granule * step
        low = (lane & width) == 0
        for i in range(len(parts)):
            if i & step == 0:
                a, b = parts[i], parts[i + step]
                parts[i] = jnp.where(low, a, pltpu.roll(b, width, axis))
                parts[i + step] = jnp.where(low, pltpu.roll(a, LANES - width, axis), b)
        step *= 2
    return parts


def z_ahead(value, f, fields, ahead_ref, out_ref):
    spectrum = product(table(ahead_ref), split(value, 3))
    for t in range(LOW // 2):
        lanes = slice(t * LANES, (t + 1) * LANES)
        parts = swap_lanes([spectrum[:HALF, lanes], spectrum[HALF:, lanes]], LANES // 2)
        for i in range(2):
            out_ref[pl.ds(f * LOW + 2 * t + i, HALF, stride=fields * LOW), :] = parts[i]


def z_back(in_ref, f, fields, back_ref, spec_ref):
    for t in range(LOW // 2):
        lanes = slice(t * LANES, (t + 1) * LANES)
        parts = [
            in_ref[pl.ds(f * LOW + 2 * t + i, HALF, stride=fields * LOW), :] for i in range(2)
        ]
        real, imag = swap_lanes(parts, LANES // 2)
        spec_ref[:HALF, lanes] = real
        spec_ref[HALF:, lanes] = imag
    return product(table(back_ref), split(spec_ref[...], 2))


def x_lines(real, imag, sign, cos_ref, sin_ref):
    data = split(jnp.concatenate([real, imag], axis=1), 2)
    even = product(table(cos_ref), data)
    odd = product(table(sin_ref), data)
    if sign < 0:
        return even[:, :N] + odd[:, N:], even[:, N:] - odd[:, :N]
    return even[:, :N] - odd[:, N:], even[:, N:] + odd[:, :N]


def y_lines(real, imag, sign, cos_ref, sin_ref):
    data = split(jnp.concatenate([real, imag], axis=0), 2)
    even = product(data, table(cos_ref))
    odd = product(data, table(sin_ref))
    if sign < 0:
        return even[:N] + odd[N:], even[N:] - odd[:N]
    return even[:N] - odd[N:], even[N:] + odd[:N]


def rows_of(block, fields, f):
    start = block * fields * LOW + f * LOW
    return pl.ds(start if isinstance(start, int) else pl.multiple_of(start, LOW), LOW)


def plane_gather(in_ref, f, fields, plane_ref):
    for i in range(ROWS):
        for h in range(2):
            parts = [in_ref[rows_of(i * COLS + h * 8 + j, fields, f), :] for j in range(8)]
            parts = swap_lanes(parts, LY)
            for g in range(8):
                x = i * LX + g % HIGH * LOW
                plane_ref[g // HIGH, x : x + LOW, h * LANES : (h + 1) * LANES] = parts[g]


def plane_scatter(plane_ref, f, fields, out_ref):
    for i in range(ROWS):
        for h in range(2):
            parts = []
            for g in range(8):
                x = i * LX + g % HIGH * LOW
                parts.append(plane_ref[g // HIGH, x : x + LOW, h * LANES : (h + 1) * LANES])
            parts = swap_lanes(parts, LY)
            for j in range(8):
                out_ref[rows_of(i * COLS + h * 8 + j, fields, f), :] = parts[j]


def plane_ahead(in_ref, f, fields, cos_ref, sin_ref, plane_ref):
    plane_gather(in_ref, f, fields, plane_ref)
    real, imag = x_lines(plane_ref[0], plane_ref[1], -1, cos_ref, sin_ref)
    return y_lines(real, imag, -1, cos_ref, sin_ref)


def plane_back(real, imag, f, fields, cos_ref, sin_ref, plane_ref, out_ref):
    real, imag = y_lines(real, imag, 1, cos_ref, sin_ref)
    real, imag = x_lines(real, imag, 1, cos_ref, sin_ref)
    plane_ref[0] = real
    plane_ref[1] = imag
    plane_scatter(plane_ref, f, fields, out_ref)


def signed(index):
    return jnp.where(index < HALF, index, index - N).astype(F32) * UNIT


def waves(place_ref, start, count):
    shape = (count, N)
    wave_x = signed(lax.broadcasted_iota(jnp.int32, shape, 0) + start)
    wave_y = signed(lax.broadcasted_iota(jnp.int32, shape, 1))
    wave_z = jnp.full(shape, place_ref[0], jnp.int32).astype(F32) * UNIT
    return wave_x, wave_y, wave_z


def fold(total):
    total = sum(total[:, t * LANES : (t + 1) * LANES] for t in range(CELLS // LANES))
    return total + pltpu.roll(total, 4, 0)


def source_kernel(conc_ref, ahead_ref, cells_ref, out_ref, lines_ref):
    for low in range(LOW):
        for high in range(HIGH):
            start = (low * HIGH + high) * LY
            lines_ref[start : start + LY, :] = conc_ref[high * LOW + low]
    conc = lines_ref[...].T
    cells_ref[...] = conc
    first = FIRST_LOW + FIRST_RISE * conc
    shear = SHEAR_LOW + SHEAR_RISE * conc
    z_ahead(-(3.0 * first + 2.0 * shear) * EIGEN_STRAIN * conc, 0, 2, ahead_ref, out_ref)
    z_ahead(conc, 1, 2, ahead_ref, out_ref)


def plane_first_kernel(
    place_ref, in_ref, cos_ref, sin_ref, out_ref, conc_ref, plane_ref, spec_ref, line_ref
):
    real, imag = plane_ahead(in_ref, 1, 2, cos_ref, sin_ref, plane_ref)
    conc_ref[0] = real
    conc_ref[1] = imag
    real, imag = plane_ahead(in_ref, 0, 2, cos_ref, sin_ref, plane_ref)
    spec_ref[0] = real
    spec_ref[1] = imag
    wave_x, wave_y, wave_z = waves(place_ref, 0, N)
    square = wave_x * wave_x + wave_y * wave_y + wave_z * wave_z
    nonzero = square > 0.0
    safe = jnp.where(nonzero, square, 1.0)
    scale = jnp.where(nonzero, -(1.0 - BETA_REF) / (SHEAR_REF * safe), 0.0)
    real = spec_ref[0] * scale
    imag = spec_ref[1] * scale
    for power in range(3):
        if power:
            real = real * wave_y
            imag = imag * wave_y
        line_ref[power, 0], line_ref[power, 1] = y_lines(real, imag, 1, cos_ref, sin_ref)
    plan = ((2, 0, 0), (0, 2, 0), (0, 0, 2), (0, 1, 1), (1, 0, 1), (1, 1, 0))
    for f, (power_x, power_y, power_z) in enumerate(plan):
        real = line_ref[power_y, 0]
        imag = line_ref[power_y, 1]
        factor = None
        for wave in [wave_x] * power_x + [wave_z] * power_z:
            factor = wave if factor is None else factor * wave
        if factor is not None:
            real = real * factor
            imag = imag * factor
        real, imag = x_lines(real, imag, 1, cos_ref, sin_ref)
        plane_ref[0] = real
        plane_ref[1] = imag
        plane_scatter(plane_ref, f, 6, out_ref)


def plane_green_kernel(place_ref, in_ref, cos_ref, sin_ref, out_ref, plane_ref, spec_ref):
    def ahead(f, carry):
        real, imag = plane_ahead(in_ref, f, 6, cos_ref, sin_ref, plane_ref)
        spec_ref[f, 0] = real
        spec_ref[f, 1] = imag
        return carry

    lax.fori_loop(0, 6, ahead, 0)

    def block(b, carry):
        start = pl.multiple_of(b * 8, 8)
        wave_x, wave_y, wave_z = waves(place_ref, start, 8)
        square = wave_x * wave_x + wave_y * wave_y + wave_z * wave_z
        nonzero = square > 0.0
        safe = jnp.where(nonzero, square, 1.0)
        inverse = 1.0 / safe
        scale = jnp.where(nonzero, inverse * (1.0 / SHEAR_REF), 0.0)
        inverse = inverse * BETA_REF
        rows = pl.ds(start, 8)
        for part in range(2):
            tau = [spec_ref[f, part, rows, :] for f in range(6)]
            force_x = tau[0] * wave_x + tau[5] * wave_y + tau[4] * wave_z
            force_y = tau[5] * wave_x + tau[1] * wave_y + tau[3] * wave_z
            force_z = tau[4] * wave_x + tau[3] * wave_y + tau[2] * wave_z
            along = (wave_x * force_x + wave_y * force_y + wave_z * force_z) * inverse
            moved_x = scale * (along * wave_x - force_x)
            moved_y = scale * (along * wave_y - force_y)
            moved_z = scale * (along * wave_z - force_z)
            spec_ref[0, part, rows, :] = wave_x * moved_x
            spec_ref[1, part, rows, :] = wave_y * moved_y
            spec_ref[2, part, rows, :] = wave_z * moved_z
            spec_ref[3, part, rows, :] = 0.5 * (wave_y * moved_z + wave_z * moved_y)
            spec_ref[4, part, rows, :] = 0.5 * (wave_x * moved_z + wave_z * moved_x)
            spec_ref[5, part, rows, :] = 0.5 * (wave_x * moved_y + wave_y * moved_x)
        return carry

    lax.fori_loop(0, N // 8, block, 0)

    def back(f, carry):
        plane_back(
            spec_ref[f, 0], spec_ref[f, 1], f, 6, cos_ref, sin_ref, plane_ref, out_ref
        )
        return carry

    lax.fori_loop(0, 6, back, 0)


def plane_update_kernel(
    place_ref, in_ref, conc_ref, cos_ref, sin_ref, out_ref, norm_ref, plane_ref
):
    real, imag = plane_ahead(in_ref, 0, 2, cos_ref, sin_ref, plane_ref)
    wave_x, wave_y, wave_z = waves(place_ref, 0, N)
    square = wave_x * wave_x + wave_y * wave_y + wave_z * wave_z
    inverse = 1.0 / (1.0 + TIME_STEP * GRADIENT_ENERGY * square * square)
    real = (conc_ref[0] - TIME_STEP * square * real) * inverse
    imag = (conc_ref[1] - TIME_STEP * square * imag) * inverse
    plane_back(real, imag, 0, 1, cos_ref, sin_ref, plane_ref, out_ref)

    total = in_ref[rows_of(0, 2, 1), :]
    for device in range(1, DEVICES):
        total = total + in_ref[rows_of(device, 2, 1), :]
    total = jnp.broadcast_to(jnp.sum(total, axis=1, keepdims=True), (8, LANES))
    total = total + pltpu.roll(total, 7, 0)
    total = total + pltpu.roll(total, 6, 0)
    norm_ref[...] = jnp.sqrt(total * (1.0 / float(N) ** 3))


def z_sweep_kernel(
    in_ref, conc_ref, back_ref, ahead_ref, strain_ref, out_ref, sum_ref, spec_ref, tau_ref
):
    def inverse(f, carry):
        strain_ref[f] = z_back(in_ref, f, 6, back_ref, spec_ref)
        return carry

    lax.fori_loop(0, 6, inverse, 0)

    def block(b, total):
        rows = pl.ds(pl.multiple_of(b * 8, 8), 8)
        conc = conc_ref[rows, :]
        strain = [strain_ref[f, rows, :] for f in range(6)]
        first = FIRST_LOW + FIRST_RISE * conc
        shear = SHEAR_LOW + SHEAR_RISE * conc
        trace = strain[0] + strain[1] + strain[2]
        normal = (first - FIRST_REF) * trace - (3.0 * first + 2.0 * shear) * EIGEN_STRAIN * conc
        excess = 2.0 * (shear - SHEAR_REF)
        for f in range(6):
            tau = excess * strain[f]
            tau_ref[f, rows, :] = tau + normal if f < 3 else tau
            total = total + strain[f] * strain[f]
        return total

    sum_ref[...] = lax.fori_loop(0, N // 8, block, jnp.zeros((8, CELLS), F32))

    def ahead(f, carry):
        z_ahead(tau_ref[f], f, 6, ahead_ref, out_ref)
        return carry

    lax.fori_loop(0, 6, ahead, 0)


def z_drive_kernel(
    in_ref,
    conc_ref,
    past_ref,
    sum_ref,
    back_ref,
    ahead_ref,
    strain_ref,
    out_ref,
    cells_ref,
    spec_ref,
    drive_ref,
):
    def inverse(f, carry):
        strain = z_back(in_ref, f, 6, back_ref, spec_ref)
        cells_ref[f] = strain
        lines = strain.T
        for low in range(LOW):
            for high in range(HIGH):
                start = (low * HIGH + high) * LY
                strain_ref[f, high * LOW + low] = lines[start : start + LY, :]
        return carry

    lax.fori_loop(0, 6, inverse, 0)

    def block(b, total):
        rows = pl.ds(pl.multiple_of(b * 8, 8), 8)
        conc = conc_ref[rows, :]
        strain = [cells_ref[f, rows, :] for f in range(6)]
        first = FIRST_LOW + FIRST_RISE * conc
        shear = SHEAR_LOW + SHEAR_RISE * conc
        dilation = EIGEN_STRAIN * conc
        part = [strain[f] - dilation for f in range(3)]
        trace = part[0] + part[1] + part[2]
        energy = (
            part[0] * part[0]
            + part[1] * part[1]
            + part[2] * part[2]
            + 2.0 * (strain[3] * strain[3] + strain[4] * strain[4] + strain[5] * strain[5])
        )
        chemical = 2.0 * WELL_HEIGHT * conc * (1.0 - conc) * (1.0 - 2.0 * conc)
        drive_ref[rows, :] = (
            chemical
            + 0.5 * FIRST_RISE * trace * trace
            + SHEAR_RISE * energy
            - EIGEN_STRAIN * (3.0 * first + 2.0 * shear) * trace
        )
        for f in range(6):
            change = strain[f] - past_ref[f, rows, :]
            total = total + change * change
        return total

    total = lax.fori_loop(0, N // 8, block, jnp.zeros((8, CELLS), F32))
    row = lax.broadcasted_iota(jnp.int32, (8, LANES), 0)
    sums = jnp.where(row < 4, fold(sum_ref[...]), fold(total))
    for device in range(DEVICES):
        out_ref[rows_of(device, 2, 1), :] = sums
    z_ahead(drive_ref[...], 0, 2, ahead_ref, out_ref)


def z_last_kernel(in_ref, back_ref, out_ref, spec_ref):
    lines = z_back(in_ref, 0, 1, back_ref, spec_ref).T
    for low in range(LOW):
        for high in range(HIGH):
            start = (low * HIGH + high) * LY
            out_ref[high * LOW + low] = lines[start : start + LY, :]


def call(kernel, name, args, outs, scratch=(), places=0):
    memory = [pltpu.SMEM] * places + [pltpu.VMEM] * (len(args) - places)
    return pl.pallas_call(
        kernel,
        out_shape=[jax.ShapeDtypeStruct(shape, F32) for shape in outs],
        in_specs=[pl.BlockSpec(memory_space=m) for m in memory],
        out_specs=[pl.BlockSpec(memory_space=pltpu.VMEM) for _ in outs],
        scratch_shapes=[pltpu.VMEM(shape, F32) for shape in scratch],
        name=name,
        interpret=INTERPRET,
        compiler_params=pltpu.CompilerParams(vmem_limit_bytes=48 * 1024 * 1024),
    )(*args)


def exchange(array):
    return lax.all_to_all(array, AXES, split_axis=0, concat_axis=0, tiled=True)


def wire(fields):
    return (DEVICES * fields * LOW, LANES)


BLOCK = (LX, LY, N)
CELL = (N, CELLS)
PLANE = (2, N, N)


def shards(concentration):
    cosine, sine, ahead, back = [jnp.asarray(table) for table in build_tables()]
    place = lax.axis_index(AXES).astype(jnp.int32)[None]

    conc, data = call(
        source_kernel, "source", (concentration, ahead), [CELL, wire(2)], [(CELLS, N)]
    )
    data = exchange(data)
    data, conc_spec = call(
        plane_first_kernel,
        "plane_first",
        (place, data, cosine, sine),
        [wire(6), PLANE],
        [PLANE, PLANE, (3, *PLANE)],
        places=1,
    )
    data = exchange(data)
    past, data, sums = call(
        z_sweep_kernel,
        "z_sweep",
        (data, conc, back, ahead),
        [(6, *CELL), wire(6), (8, CELLS)],
        [CELL, (6, *CELL)],
    )
    data = exchange(data)
    (data,) = call(
        plane_green_kernel,
        "plane_green",
        (place, data, cosine, sine),
        [wire(6)],
        [PLANE, (6, *PLANE)],
        places=1,
    )
    data = exchange(data)
    strain, data = call(
        z_drive_kernel,
        "z_drive",
        (data, conc, past, sums, back, ahead),
        [(6, *BLOCK), wire(2)],
        [(6, *CELL), CELL, CELL],
    )
    data = exchange(data)
    data, norms = call(
        plane_update_kernel,
        "plane_update",
        (place, data, conc_spec, cosine, sine),
        [wire(1), (8, LANES)],
        [PLANE],
        places=1,
    )
    data = exchange(data)
    (conc_next,) = call(z_last_kernel, "z_last", (data, back), [BLOCK], [CELL])
    return conc_next, strain, norms[::4, 0]


def solution(mesh):
    whole = Mesh(mesh.devices.reshape(4, 2, 4, 4), AXES)
    row, col = AXES[:2], AXES[2:]
    return jax.shard_map(
        shards,
        mesh=whole,
        in_specs=(P(row, col, None),),
        out_specs=(P(row, col, None), P(None, row, col, None), P()),
        check_vma=False,
    )
```

```python
import math
from functools import partial

import jax
import jax.numpy as jnp
import numpy as np
from jax import lax
from jax.experimental import pallas as pl
from jax.experimental.pallas import tpu as pltpu
from jax.sharding import Mesh
from jax.sharding import PartitionSpec as P

AXES = ("row_0", "row_1", "col_0", "col_1")

FIRST_LOW = 1.0
FIRST_RISE = 0.6
SHEAR_LOW = 0.7
SHEAR_RISE = 0.8
FIRST_REF = 1.3
SHEAR_REF = 1.1
BETA_REF = 2.4 / 3.5
EIGEN_STRAIN = 0.5
WELL_HEIGHT = 1.0
TIME_STEP = 0.5
GRADIENT_ENERGY = 0.5

N = 256
HALF = N // 2
ROWS = 8
COLS = 16
DEVICES = ROWS * COLS
LX = N // ROWS
LY = N // COLS
LOW = 8
HIGH = LX // LOW
CELLS = LX * LY
LANES = 128
UNIT = 2.0 * math.pi / N
F32 = jnp.float32
BF16 = jnp.bfloat16
INTERPRET = False
UNROLL = 1
SOURCE_ROWS = 2 * LOW + 1
FIRST_ROWS = 5 * LOW
SWEEP_ROWS = 6 * LOW
DRIVE_ROWS = LOW
LAST_ROWS = LOW + 1
FIRST_FIELDS = (0, 1, 3, 4, 5)
TRACE = -(1.0 - BETA_REF) / SHEAR_REF


def pieces_of(table, count):
    rest = table.astype(np.float32)
    pieces = []
    for _ in range(count):
        piece = rest.astype(jnp.bfloat16)
        rest = rest - piece.astype(np.float32)
        pieces.append(piece)
    return np.stack(pieces)


def build_tables():
    index = np.arange(N)
    half = np.arange(HALF)
    angle = 2.0 * np.pi / N * (index[:, None] * index[None, :] % N)
    cosine = np.cos(angle)
    sine = np.sin(angle)
    lines = []
    for odd in range(2):
        angle = 2.0 * np.pi / N * ((2 * half[:, None] + odd) * half[None, :] % N)
        lines.append(
            np.block([[np.cos(angle), np.sin(angle)], [-np.sin(angle), np.cos(angle)]])
        )
    line_ahead = np.stack([pieces_of(line, 2) for line in lines])
    line_back = np.stack([pieces_of(line.T, 2) for line in lines])
    ahead = np.concatenate([cosine[:HALF], -sine[:HALF]], axis=0)
    weight = np.where(half == 0, 1.0, 2.0) / float(N) ** 3
    back = np.concatenate([cosine[:, :HALF] * weight, -sine[:, :HALF] * weight], axis=1)
    return line_ahead, line_back, pieces_of(ahead, 3), pieces_of(back, 2)


def split(value, count):
    pieces = []
    for i in range(count):
        piece = value.astype(BF16)
        pieces.append(piece)
        if i + 1 < count:
            value = value - piece.astype(F32)
    return pieces


def product(left, right):
    count = len(right)
    total = None
    for order in reversed(range(count)):
        for i in range(order + 1):
            term = jnp.dot(left[i], right[order - i], preferred_element_type=F32)
            total = term if total is None else total + term
    return total


def table(ref):
    return [ref[i] for i in range(ref.shape[0])]


def swap_lanes(parts, granule):
    parts = list(parts)
    axis = parts[0].ndim - 1
    lane = lax.broadcasted_iota(jnp.int32, parts[0].shape, axis)
    step = 1
    while step < len(parts):
        width = granule * step
        low = (lane & width) == 0
        for i in range(len(parts)):
            if i & step == 0:
                a, b = parts[i], parts[i + step]
                parts[i] = jnp.where(low, a, pltpu.roll(b, width, axis))
                parts[i + step] = jnp.where(low, pltpu.roll(a, LANES - width, axis), b)
        step *= 2
    return parts


def peers_of(row, pitch):
    return pl.ds(row, DEVICES, stride=pitch)


def z_ahead(value, f, pitch, ahead_ref, out_ref):
    spectrum = product(table(ahead_ref), split(value, 3))
    for t in range(LOW // 2):
        lanes = slice(t * LANES, (t + 1) * LANES)
        parts = swap_lanes([spectrum[:HALF, lanes], spectrum[HALF:, lanes]], LANES // 2)
        for i in range(2):
            out_ref[peers_of(f * LOW + 2 * t + i, pitch), :] = parts[i]


def z_back(in_ref, f, pitch, back_ref, spec_ref):
    for t in range(LOW // 2):
        lanes = slice(t * LANES, (t + 1) * LANES)
        parts = [in_ref[peers_of(f * LOW + 2 * t + i, pitch), :] for i in range(2)]
        real, imag = swap_lanes(parts, LANES // 2)
        spec_ref[:HALF, lanes] = real
        spec_ref[HALF:, lanes] = imag
    return product(table(back_ref), split(spec_ref[...], 2))


def rows_of(peer, f, pitch):
    start = peer * pitch + f * LOW
    return pl.ds(start if isinstance(start, int) else pl.multiple_of(start, LOW), LOW)


def plane_row(part, i, high):
    return part * HALF + i % 4 * LX + high * LOW


def plane_ahead(in_ref, f, pitch, ahead_ref, plane_ref):
    for i in range(ROWS // 2):
        for h in range(2):
            near, far = [
                swap_lanes(
                    [in_ref[rows_of(k * COLS + h * 8 + j, f, pitch), :] for j in range(8)], LY
                )
                for k in (i, i + ROWS // 2)
            ]
            for g in range(8):
                row = plane_row(g // HIGH, i, g % HIGH)
                lanes = slice(h * LANES, (h + 1) * LANES)
                plane_ref[0, row : row + LOW, lanes] = near[g] + far[g]
                plane_ref[1, row : row + LOW, lanes] = near[g] - far[g]
    near, far = [], []
    for b in range(2):
        lines = product(table(ahead_ref.at[b]), split(plane_ref[b], 2))
        near.append(jnp.concatenate([lines[:HALF, :HALF], lines[HALF:, :HALF]], axis=1))
        far.append(jnp.concatenate([lines[:HALF, HALF:], lines[HALF:, HALF:]], axis=1))
    near = jnp.concatenate(near, axis=0)
    far = jnp.concatenate(far, axis=0)
    return near + far, near - far


def plane_spectrum(in_ref, f, pitch, ahead_ref, back_ref, plane_ref):
    even, odd = plane_ahead(in_ref, f, pitch, ahead_ref, plane_ref)
    return (
        product(split(even, 2), table(back_ref.at[0])),
        product(split(odd, 2), table(back_ref.at[1])),
    )


def y_back(even, odd, ahead_ref):
    even = product(split(even, 2), table(ahead_ref.at[0]))
    odd = product(split(odd, 2), table(ahead_ref.at[1]))
    near = even + odd
    far = even - odd
    return (
        jnp.concatenate([near[:, :HALF], far[:, :HALF]], axis=1),
        jnp.concatenate([near[:, HALF:], far[:, HALF:]], axis=1),
    )


def x_back(real, imag, f, pitch, back_ref, plane_ref, out_ref):
    lines = []
    for b in range(2):
        rows = slice(b * HALF, (b + 1) * HALF)
        data = jnp.concatenate([real[rows], imag[rows]], axis=0)
        lines.append(product(table(back_ref.at[b]), split(data, 2)))
    plane_ref[0] = lines[0] + lines[1]
    plane_ref[1] = lines[0] - lines[1]
    for i in range(ROWS):
        for h in range(2):
            parts = []
            for g in range(8):
                row = plane_row(g // HIGH, i, g % HIGH)
                parts.append(plane_ref[i // 4, row : row + LOW, h * LANES : (h + 1) * LANES])
            parts = swap_lanes(parts, LY)
            for j in range(8):
                out_ref[rows_of(i * COLS + h * 8 + j, f, pitch), :] = parts[j]


def signed(index):
    return jnp.where(index < HALF, index, index - N).astype(F32) * UNIT


def row_waves(start, count, lanes):
    row = lax.broadcasted_iota(jnp.int32, (count, lanes), 0) + start
    return signed(2 * (row % HALF) + row // HALF)


def waves(place_ref, branch, start, count):
    shape = (count, N)
    lane = lax.broadcasted_iota(jnp.int32, shape, 1)
    wave_y = signed(2 * (lane % HALF) + branch)
    wave_z = jnp.full(shape, place_ref[0], jnp.int32).astype(F32) * UNIT
    return row_waves(start, count, N), wave_y, wave_z


def squares(total):
    total = sum(total[:, t * LANES : (t + 1) * LANES] for t in range(CELLS // LANES))
    total = jnp.sum(total, axis=0, keepdims=True)
    return total + pltpu.roll(total, LANES // 2, 1)


def source_of(conc):
    first = FIRST_LOW + FIRST_RISE * conc
    shear = SHEAR_LOW + SHEAR_RISE * conc
    return -(3.0 * first + 2.0 * shear) * EIGEN_STRAIN * conc


def source_kernel(conc_ref, ahead_ref, cells_ref, out_ref, lines_ref):
    for low in range(LOW):
        for high in range(HIGH):
            start = (low * HIGH + high) * LY
            lines_ref[start : start + LY, :] = conc_ref[high * LOW + low]
    conc = lines_ref[...].T
    cells_ref[...] = conc
    source = source_of(conc)
    total = jnp.sum(source.reshape(N // 8, 8, CELLS), axis=0)
    total = sum(total[:, t * LANES : (t + 1) * LANES] for t in range(CELLS // LANES))
    total = jnp.sum(total, axis=0, keepdims=True)
    out_ref[peers_of(2 * LOW, SOURCE_ROWS), :] = jnp.broadcast_to(total, (DEVICES, LANES))
    z_ahead(source, 0, SOURCE_ROWS, ahead_ref, out_ref)
    z_ahead(conc, 1, SOURCE_ROWS, ahead_ref, out_ref)


def plane_first_kernel(place_ref, in_ref, ahead_ref, back_ref, out_ref, plane_ref, line_ref):
    data = list(plane_spectrum(in_ref, 0, SOURCE_ROWS, ahead_ref, back_ref, plane_ref))
    wave_y = []
    for b in range(2):
        wave_x, wave, wave_z = waves(place_ref, b, 0, N)
        wave_y.append(wave)
        square = wave_x * wave_x + wave * wave + wave_z * wave_z
        nonzero = square > 0.0
        safe = jnp.where(nonzero, square, 1.0)
        data[b] = data[b] * jnp.where(nonzero, TRACE / safe, 0.0)
    for power in range(3):
        if power:
            data = [data[b] * wave_y[b] for b in range(2)]
        line_ref[power, 0], line_ref[power, 1] = y_back(data[0], data[1], ahead_ref)
    wave_x = row_waves(0, N, N)
    wave_z = jnp.full((N, N), place_ref[0], jnp.int32).astype(F32) * UNIT
    plan = ((2, 0, 0), (0, 2, 0), (0, 1, 1), (1, 0, 1), (1, 1, 0))
    for f, (power_x, power_y, power_z) in enumerate(plan):
        real = line_ref[power_y, 0]
        imag = line_ref[power_y, 1]
        factor = None
        for wave in [wave_x] * power_x + [wave_z] * power_z:
            factor = wave if factor is None else factor * wave
        if factor is not None:
            real = real * factor
            imag = imag * factor
        x_back(real, imag, f, FIRST_ROWS, back_ref, plane_ref, out_ref)


def aside_first_kernel(in_ref, cells_ref, ahead_ref, back_ref, conc_ref, trace_ref, plane_ref):
    conc_ref[0], conc_ref[1] = plane_spectrum(
        in_ref, 1, SOURCE_ROWS, ahead_ref, back_ref, plane_ref
    )
    mean = jnp.sum(in_ref[peers_of(2 * LOW, SOURCE_ROWS), :]) * (1.0 / float(N) ** 3)
    source = source_of(cells_ref[...])
    row = lax.broadcasted_iota(jnp.int32, (N, CELLS), 0)
    edge = jnp.where(row % 2 == 0, source, -source)
    edge = jnp.sum(edge, axis=0, keepdims=True) * (1.0 / N)
    edge = jnp.where(row % 2 == 0, edge, -edge)
    trace_ref[...] = TRACE * (source - edge - mean)


def z_sweep_kernel(
    in_ref, cells_ref, trace_ref, back_ref, ahead_ref, strain_ref, out_ref, spec_ref, tau_ref
):
    for f, component in enumerate(FIRST_FIELDS):
        strain_ref[component] = z_back(in_ref, f, FIRST_ROWS, back_ref, spec_ref)

    def block(b, carry):
        rows = pl.ds(pl.multiple_of(b * 8, 8), 8)
        conc = cells_ref[rows, :]
        trace = trace_ref[rows, :]
        strain = [strain_ref[f, rows, :] for f in range(6) if f != 2]
        strain.insert(2, trace - strain[0] - strain[1])
        strain_ref[2, rows, :] = strain[2]
        first = FIRST_LOW + FIRST_RISE * conc
        shear = SHEAR_LOW + SHEAR_RISE * conc
        normal = (first - FIRST_REF) * trace + source_of(conc)
        excess = 2.0 * (shear - SHEAR_REF)
        for f in range(6):
            tau = excess * strain[f]
            tau_ref[f, rows, :] = tau + normal if f < 3 else tau
        return carry

    lax.fori_loop(0, N // 8, block, 0)

    def ahead(f, carry):
        z_ahead(tau_ref[f], f, SWEEP_ROWS, ahead_ref, out_ref)
        return carry

    lax.fori_loop(0, 6, ahead, 0, unroll=UNROLL)


def plane_green_kernel(place_ref, in_ref, ahead_ref, back_ref, out_ref, plane_ref, spec_ref):
    def ahead(f, carry):
        spec_ref[f, 0], spec_ref[f, 1] = plane_spectrum(
            in_ref, f, SWEEP_ROWS, ahead_ref, back_ref, plane_ref
        )
        return carry

    lax.fori_loop(0, 6, ahead, 0, unroll=UNROLL)

    def block(b, carry):
        start = pl.multiple_of(b * 8, 8)
        rows = pl.ds(start, 8)
        for branch in range(2):
            wave_x, wave_y, wave_z = waves(place_ref, branch, start, 8)
            square = wave_x * wave_x + wave_y * wave_y + wave_z * wave_z
            nonzero = square > 0.0
            safe = jnp.where(nonzero, square, 1.0)
            inverse = 1.0 / safe
            scale = jnp.where(nonzero, inverse * (1.0 / SHEAR_REF), 0.0)
            inverse = inverse * BETA_REF
            tau = [spec_ref[f, branch, rows, :] for f in range(6)]
            force_x = tau[0] * wave_x + tau[5] * wave_y + tau[4] * wave_z
            force_y = tau[5] * wave_x + tau[1] * wave_y + tau[3] * wave_z
            force_z = tau[4] * wave_x + tau[3] * wave_y + tau[2] * wave_z
            along = (wave_x * force_x + wave_y * force_y + wave_z * force_z) * inverse
            moved_x = scale * (along * wave_x - force_x)
            moved_y = scale * (along * wave_y - force_y)
            moved_z = scale * (along * wave_z - force_z)
            spec_ref[0, branch, rows, :] = wave_x * moved_x
            spec_ref[1, branch, rows, :] = wave_y * moved_y
            spec_ref[2, branch, rows, :] = wave_z * moved_z
            spec_ref[3, branch, rows, :] = 0.5 * (wave_y * moved_z + wave_z * moved_y)
            spec_ref[4, branch, rows, :] = 0.5 * (wave_x * moved_z + wave_z * moved_x)
            spec_ref[5, branch, rows, :] = 0.5 * (wave_x * moved_y + wave_y * moved_x)
        return carry

    lax.fori_loop(0, N // 8, block, 0)

    def back(f, carry):
        real, imag = y_back(spec_ref[f, 0], spec_ref[f, 1], ahead_ref)
        x_back(real, imag, f, SWEEP_ROWS, back_ref, plane_ref, out_ref)
        return carry

    lax.fori_loop(0, 6, back, 0, unroll=UNROLL)


def z_drive_kernel(in_ref, cells_ref, back_ref, ahead_ref, strain_ref, out_ref, spec_ref, drive_ref):
    def inverse(f, carry):
        strain_ref[f] = z_back(in_ref, f, SWEEP_ROWS, back_ref, spec_ref)
        return carry

    lax.fori_loop(0, 6, inverse, 0, unroll=UNROLL)

    def block(b, carry):
        rows = pl.ds(pl.multiple_of(b * 8, 8), 8)
        conc = cells_ref[rows, :]
        strain = [strain_ref[f, rows, :] for f in range(6)]
        first = FIRST_LOW + FIRST_RISE * conc
        shear = SHEAR_LOW + SHEAR_RISE * conc
        dilation = EIGEN_STRAIN * conc
        part = [strain[f] - dilation for f in range(3)]
        trace = part[0] + part[1] + part[2]
        energy = (
            part[0] * part[0]
            + part[1] * part[1]
            + part[2] * part[2]
            + 2.0 * (strain[3] * strain[3] + strain[4] * strain[4] + strain[5] * strain[5])
        )
        chemical = 2.0 * WELL_HEIGHT * conc * (1.0 - conc) * (1.0 - 2.0 * conc)
        drive_ref[rows, :] = (
            chemical
            + 0.5 * FIRST_RISE * trace * trace
            + SHEAR_RISE * energy
            - EIGEN_STRAIN * (3.0 * first + 2.0 * shear) * trace
        )
        return carry

    lax.fori_loop(0, N // 8, block, 0)
    z_ahead(drive_ref[...], 0, DRIVE_ROWS, ahead_ref, out_ref)


def aside_last_kernel(cells_ref, past_ref, strain_ref, sums_ref):
    def one(f, totals):
        def block(b, totals):
            rows = pl.ds(pl.multiple_of(b * 8, 8), 8)
            past = past_ref[f, rows, :]
            change = cells_ref[f, rows, :] - past
            return totals[0] + past * past, totals[1] + change * change

        lines = cells_ref[f].T
        for low in range(LOW):
            for high in range(HIGH):
                start = (low * HIGH + high) * LY
                strain_ref[f, high * LOW + low] = lines[start : start + LY, :]
        return lax.fori_loop(0, N // 8, block, totals)

    zero = jnp.zeros((8, CELLS), F32)
    totals = lax.fori_loop(0, 6, one, (zero, zero))
    lane = lax.broadcasted_iota(jnp.int32, (1, LANES), 1)
    sums = jnp.where(lane < LANES // 2, squares(totals[0]), squares(totals[1]))
    sums_ref[...] = jnp.broadcast_to(sums, (8, LANES))


def plane_update_kernel(
    place_ref, in_ref, conc_ref, sums_ref, ahead_ref, back_ref, out_ref, plane_ref
):
    data = list(plane_spectrum(in_ref, 0, DRIVE_ROWS, ahead_ref, back_ref, plane_ref))
    for b in range(2):
        wave_x, wave_y, wave_z = waves(place_ref, b, 0, N)
        square = wave_x * wave_x + wave_y * wave_y + wave_z * wave_z
        denominator = 1.0 + TIME_STEP * GRADIENT_ENERGY * square * square
        data[b] = (conc_ref[b] - TIME_STEP * square * data[b]) / denominator
    real, imag = y_back(data[0], data[1], ahead_ref)
    x_back(real, imag, 0, LAST_ROWS, back_ref, plane_ref, out_ref)
    out_ref[peers_of(LOW, LAST_ROWS), :] = jnp.broadcast_to(sums_ref[:1, :], (DEVICES, LANES))


def z_last_kernel(in_ref, back_ref, out_ref, norm_ref, spec_ref):
    sums = in_ref[peers_of(LOW, LAST_ROWS), :]
    lane = lax.broadcasted_iota(jnp.int32, sums.shape, 1)
    row = lax.broadcasted_iota(jnp.int32, (8, LANES), 0)
    first = jnp.sum(jnp.where(lane < LANES // 2, sums, 0.0))
    second = jnp.sum(jnp.where(lane < LANES // 2, 0.0, sums))
    norm_ref[...] = jnp.sqrt(jnp.where(row == 0, first, second) * (1.0 / float(N) ** 3))
    lines = z_back(in_ref, 0, LAST_ROWS, back_ref, spec_ref).T
    for low in range(LOW):
        for high in range(HIGH):
            start = (low * HIGH + high) * LY
            out_ref[high * LOW + low] = lines[start : start + LY, :]


def call(kernel, name, args, outs, scratch=(), places=0, mib=24):
    memory = [pltpu.SMEM] * places + [pltpu.VMEM] * (len(args) - places)
    return pl.pallas_call(
        kernel,
        out_shape=[jax.ShapeDtypeStruct(shape, F32) for shape in outs],
        in_specs=[pl.BlockSpec(memory_space=m) for m in memory],
        out_specs=[pl.BlockSpec(memory_space=pltpu.VMEM) for _ in outs],
        scratch_shapes=[pltpu.VMEM(shape, F32) for shape in scratch],
        name=name,
        interpret=INTERPRET,
        compiler_params=pltpu.CompilerParams(vmem_limit_bytes=mib * 1024 * 1024),
    )(*args)


def exchange(array):
    rows = array.reshape(DEVICES, array.shape[0] // DEVICES * LANES)
    rows = lax.all_to_all(rows, AXES, split_axis=0, concat_axis=0, tiled=True)
    return rows.reshape(array.shape)


def wire(pitch):
    return (DEVICES * pitch, LANES)


BLOCK = (LX, LY, N)
CELL = (N, CELLS)
PLANE = (2, N, N)


def shards(concentration):
    line_ahead, line_back, ahead, back = [jnp.asarray(table) for table in build_tables()]
    place = lax.axis_index(AXES).astype(jnp.int32)[None]

    cells, data = call(
        source_kernel, "source", (concentration, ahead), [CELL, wire(SOURCE_ROWS)], [(CELLS, N)]
    )
    source = exchange(data)
    (data,) = call(
        plane_first_kernel,
        "plane_first",
        (place, source, line_ahead, line_back),
        [wire(FIRST_ROWS)],
        [PLANE, (3, *PLANE)],
        places=1,
    )
    data = exchange(data)
    conc_spec, trace = call(
        aside_first_kernel,
        "aside_first",
        (source, cells, line_ahead, line_back),
        [PLANE, CELL],
        [PLANE],
    )
    past, data = call(
        z_sweep_kernel,
        "z_sweep",
        (data, cells, trace, back, ahead),
        [(6, *CELL), wire(SWEEP_ROWS)],
        [CELL, (6, *CELL)],
    )
    data = exchange(data)
    (data,) = call(
        plane_green_kernel,
        "plane_green",
        (place, data, line_ahead, line_back),
        [wire(SWEEP_ROWS)],
        [PLANE, (6, *PLANE)],
        places=1,
    )
    data = exchange(data)
    strain, data = call(
        z_drive_kernel,
        "z_drive",
        (data, cells, back, ahead),
        [(6, *CELL), wire(DRIVE_ROWS)],
        [CELL, CELL],
    )
    data = exchange(data)
    strain, sums = call(aside_last_kernel, "aside_last", (strain, past), [(6, *BLOCK), (8, LANES)])
    (data,) = call(
        plane_update_kernel,
        "plane_update",
        (place, data, conc_spec, sums, line_ahead, line_back),
        [wire(LAST_ROWS)],
        [PLANE],
        places=1,
    )
    data = exchange(data)
    conc_next, norms = call(
        z_last_kernel, "z_last", (data, back), [BLOCK, (8, LANES)], [CELL]
    )
    return conc_next, strain, norms[:2, 0]


def solution(mesh):
    whole = Mesh(mesh.devices.reshape(4, 2, 4, 4), AXES)
    row, col = AXES[:2], AXES[2:]
    return jax.shard_map(
        shards,
        mesh=whole,
        in_specs=(P(row, col, None),),
        out_specs=(P(row, col, None), P(None, row, col, None), P()),
        check_vma=False,
    )
```

```python
import math
from functools import partial

import jax
import jax.numpy as jnp
import numpy as np
from jax import lax
from jax.experimental import pallas as pl
from jax.experimental.pallas import tpu as pltpu
from jax.sharding import Mesh
from jax.sharding import PartitionSpec as P

AXES = ("row_0", "row_1", "col_0", "col_1")

FIRST_LOW = 1.0
FIRST_RISE = 0.6
SHEAR_LOW = 0.7
SHEAR_RISE = 0.8
FIRST_REF = 1.3
SHEAR_REF = 1.1
BETA_REF = 2.4 / 3.5
EIGEN_STRAIN = 0.5
WELL_HEIGHT = 1.0
TIME_STEP = 0.5
GRADIENT_ENERGY = 0.5

N = 256
HALF = N // 2
ROWS = 8
COLS = 16
DEVICES = ROWS * COLS
LX = N // ROWS
LY = N // COLS
LOW = 8
HIGH = LX // LOW
CELLS = LX * LY
LANES = 128
UNIT = 2.0 * math.pi / N
F32 = jnp.float32
BF16 = jnp.bfloat16
INTERPRET = False
UNROLL = 1
SOURCE_ROWS = 2 * LOW + 1
FIRST_ROWS = 5 * LOW
SWEEP_ROWS = 6 * LOW
DRIVE_ROWS = LOW
LAST_ROWS = LOW + 1
FIRST_FIELDS = (0, 1, 3, 4, 5)
TRACE = -(1.0 - BETA_REF) / SHEAR_REF


def pieces_of(table, count):
    rest = table.astype(np.float32)
    pieces = []
    for _ in range(count):
        piece = rest.astype(jnp.bfloat16)
        rest = rest - piece.astype(np.float32)
        pieces.append(piece)
    return np.stack(pieces)


def build_tables():
    index = np.arange(N)
    half = np.arange(HALF)
    angle = 2.0 * np.pi / N * (index[:, None] * index[None, :] % N)
    cosine = np.cos(angle)
    sine = np.sin(angle)
    lines = []
    for odd in range(2):
        angle = 2.0 * np.pi / N * ((2 * half[:, None] + odd) * half[None, :] % N)
        lines.append(
            np.block([[np.cos(angle), np.sin(angle)], [-np.sin(angle), np.cos(angle)]])
        )
    line_ahead = np.stack([pieces_of(line, 2) for line in lines])
    line_back = np.stack([pieces_of(line.T, 2) for line in lines])
    ahead = np.concatenate([cosine[:HALF], -sine[:HALF]], axis=0)
    weight = np.where(half == 0, 1.0, 2.0) / float(N) ** 3
    back = np.concatenate([cosine[:, :HALF] * weight, -sine[:, :HALF] * weight], axis=1)
    return line_ahead, line_back, pieces_of(ahead, 3), pieces_of(back, 2)


def split(value, count):
    pieces = []
    for i in range(count):
        piece = value.astype(BF16)
        pieces.append(piece)
        if i + 1 < count:
            value = value - piece.astype(F32)
    return pieces


def product(left, right):
    count = len(right)
    total = None
    for order in reversed(range(count)):
        for i in range(order + 1):
            term = jnp.dot(left[i], right[order - i], preferred_element_type=F32)
            total = term if total is None else total + term
    return total


def table(ref):
    return [ref[i] for i in range(ref.shape[0])]


def swap_lanes(parts, granule):
    parts = list(parts)
    axis = parts[0].ndim - 1
    lane = lax.broadcasted_iota(jnp.int32, parts[0].shape, axis)
    step = 1
    while step < len(parts):
        width = granule * step
        low = (lane & width) == 0
        for i in range(len(parts)):
            if i & step == 0:
                a, b = parts[i], parts[i + step]
                parts[i] = jnp.where(low, a, pltpu.roll(b, width, axis))
                parts[i + step] = jnp.where(low, pltpu.roll(a, LANES - width, axis), b)
        step *= 2
    return parts


def peers_of(row, pitch):
    return pl.ds(row, DEVICES, stride=pitch)


def z_ahead(value, f, pitch, ahead_ref, out_ref):
    spectrum = product(table(ahead_ref), split(value, 3))
    for t in range(LOW // 2):
        lanes = slice(t * LANES, (t + 1) * LANES)
        parts = swap_lanes([spectrum[:HALF, lanes], spectrum[HALF:, lanes]], LANES // 2)
        for i in range(2):
            out_ref[peers_of(f * LOW + 2 * t + i, pitch), :] = parts[i]


def z_back(in_ref, f, pitch, back_ref, spec_ref):
    for t in range(LOW // 2):
        lanes = slice(t * LANES, (t + 1) * LANES)
        parts = [in_ref[peers_of(f * LOW + 2 * t + i, pitch), :] for i in range(2)]
        real, imag = swap_lanes(parts, LANES // 2)
        spec_ref[:HALF, lanes] = real
        spec_ref[HALF:, lanes] = imag
    return product(table(back_ref), split(spec_ref[...], 2))


def rows_of(peer, f, pitch):
    start = peer * pitch + f * LOW
    return pl.ds(start if isinstance(start, int) else pl.multiple_of(start, LOW), LOW)


def plane_row(part, i, high):
    return part * HALF + i % 4 * LX + high * LOW


def plane_ahead(in_ref, f, pitch, ahead_ref, plane_ref):
    for i in range(ROWS // 2):
        for h in range(2):
            near, far = [
                swap_lanes(
                    [in_ref[rows_of(k * COLS + h * 8 + j, f, pitch), :] for j in range(8)], LY
                )
                for k in (i, i + ROWS // 2)
            ]
            for g in range(8):
                row = plane_row(g // HIGH, i, g % HIGH)
                lanes = slice(h * LANES, (h + 1) * LANES)
                plane_ref[0, row : row + LOW, lanes] = near[g] + far[g]
                plane_ref[1, row : row + LOW, lanes] = near[g] - far[g]
    near, far = [], []
    for b in range(2):
        lines = product(table(ahead_ref.at[b]), split(plane_ref[b], 2))
        near.append(jnp.concatenate([lines[:HALF, :HALF], lines[HALF:, :HALF]], axis=1))
        far.append(jnp.concatenate([lines[:HALF, HALF:], lines[HALF:, HALF:]], axis=1))
    near = jnp.concatenate(near, axis=0)
    far = jnp.concatenate(far, axis=0)
    return near + far, near - far


def plane_spectrum(in_ref, f, pitch, ahead_ref, back_ref, plane_ref):
    even, odd = plane_ahead(in_ref, f, pitch, ahead_ref, plane_ref)
    return (
        product(split(even, 2), table(back_ref.at[0])),
        product(split(odd, 2), table(back_ref.at[1])),
    )


def y_back(even, odd, ahead_ref):
    even = product(split(even, 2), table(ahead_ref.at[0]))
    odd = product(split(odd, 2), table(ahead_ref.at[1]))
    near = even + odd
    far = even - odd
    return (
        jnp.concatenate([near[:, :HALF], far[:, :HALF]], axis=1),
        jnp.concatenate([near[:, HALF:], far[:, HALF:]], axis=1),
    )


def x_back(real, imag, f, pitch, back_ref, plane_ref, out_ref):
    lines = []
    for b in range(2):
        rows = slice(b * HALF, (b + 1) * HALF)
        data = jnp.concatenate([real[rows], imag[rows]], axis=0)
        lines.append(product(table(back_ref.at[b]), split(data, 2)))
    plane_ref[0] = lines[0] + lines[1]
    plane_ref[1] = lines[0] - lines[1]
    for i in range(ROWS):
        for h in range(2):
            parts = []
            for g in range(8):
                row = plane_row(g // HIGH, i, g % HIGH)
                parts.append(plane_ref[i // 4, row : row + LOW, h * LANES : (h + 1) * LANES])
            parts = swap_lanes(parts, LY)
            for j in range(8):
                out_ref[rows_of(i * COLS + h * 8 + j, f, pitch), :] = parts[j]


def signed(index):
    return jnp.where(index < HALF, index, index - N).astype(F32) * UNIT


def row_waves(start, count, lanes):
    row = lax.broadcasted_iota(jnp.int32, (count, lanes), 0) + start
    return signed(2 * (row % HALF) + row // HALF)


def waves(place_ref, branch, start, count):
    shape = (count, N)
    lane = lax.broadcasted_iota(jnp.int32, shape, 1)
    wave_y = signed(2 * (lane % HALF) + branch)
    wave_z = jnp.full(shape, place_ref[0], jnp.int32).astype(F32) * UNIT
    return row_waves(start, count, N), wave_y, wave_z


def squares(total):
    total = sum(total[:, t * LANES : (t + 1) * LANES] for t in range(CELLS // LANES))
    total = jnp.sum(total, axis=0, keepdims=True)
    return total + pltpu.roll(total, LANES // 2, 1)


def source_of(conc):
    first = FIRST_LOW + FIRST_RISE * conc
    shear = SHEAR_LOW + SHEAR_RISE * conc
    return -(3.0 * first + 2.0 * shear) * EIGEN_STRAIN * conc


def copy_lines(far, lines_ref, sems, inward):
    copies = []
    for high in range(HIGH):
        pair = (far.at[pl.ds(high * LOW, LOW)], lines_ref.at[:, high])
        source, target = pair if inward else pair[::-1]
        copies.append(pltpu.make_async_copy(source, target, sems.at[high]))
    return copies


def source_kernel(
    place_ref,
    conc_ref,
    far_ref,
    cells_ref,
    out_ref,
    edge_ref,
    lines_ref,
    ahead_ref,
    sems,
    far_sem,
):
    copies = copy_lines(conc_ref, lines_ref, sems, True)
    copies.append(pltpu.make_async_copy(far_ref, ahead_ref, far_sem))
    for copy in copies:
        copy.start()
    for copy in copies:
        copy.wait()
    conc = lines_ref[...].reshape(CELLS, N).T
    cells_ref[...] = conc
    source = source_of(conc)
    total = jnp.sum(source.reshape(N // 8, 8, CELLS), axis=0)
    row = lax.broadcasted_iota(jnp.int32, (8, CELLS), 0)
    edge = jnp.where(row % 2 == 0, total, -total)
    edge = jnp.sum(edge, axis=0, keepdims=True) * (1.0 / N)
    edge_ref[...] = jnp.where(row % 2 == 0, edge, -edge)
    total = sum(total[:, t * LANES : (t + 1) * LANES] for t in range(CELLS // LANES))
    total = jnp.sum(total, axis=0, keepdims=True)
    out_ref[peers_of(2 * LOW, SOURCE_ROWS), :] = jnp.broadcast_to(total, (DEVICES, LANES))
    z_ahead(source, 0, SOURCE_ROWS, ahead_ref, out_ref)
    z_ahead(conc, 1, SOURCE_ROWS, ahead_ref, out_ref)


def plane_first_kernel(
    place_ref, in_ref, ahead_ref, back_ref, out_ref, mean_ref, plane_ref, line_ref
):
    mean = jnp.sum(in_ref[peers_of(2 * LOW, SOURCE_ROWS), :]) * (1.0 / float(N) ** 3)
    mean_ref[...] = jnp.full((8, CELLS), mean, F32)
    data = list(plane_spectrum(in_ref, 0, SOURCE_ROWS, ahead_ref, back_ref, plane_ref))
    wave_y = []
    for b in range(2):
        wave_x, wave, wave_z = waves(place_ref, b, 0, N)
        wave_y.append(wave)
        square = wave_x * wave_x + wave * wave + wave_z * wave_z
        nonzero = square > 0.0
        safe = jnp.where(nonzero, square, 1.0)
        data[b] = data[b] * jnp.where(nonzero, TRACE / safe, 0.0)
    for power in range(3):
        if power:
            data = [data[b] * wave_y[b] for b in range(2)]
        line_ref[power, 0], line_ref[power, 1] = y_back(data[0], data[1], ahead_ref)
    wave_x = row_waves(0, N, N)
    wave_z = jnp.full((N, N), place_ref[0], jnp.int32).astype(F32) * UNIT
    plan = ((2, 0, 0), (0, 2, 0), (0, 1, 1), (1, 0, 1), (1, 1, 0))
    for f, (power_x, power_y, power_z) in enumerate(plan):
        real = line_ref[power_y, 0]
        imag = line_ref[power_y, 1]
        factor = None
        for wave in [wave_x] * power_x + [wave_z] * power_z:
            factor = wave if factor is None else factor * wave
        if factor is not None:
            real = real * factor
            imag = imag * factor
        x_back(real, imag, f, FIRST_ROWS, back_ref, plane_ref, out_ref)


def z_sweep_kernel(
    in_ref,
    cells_ref,
    edge_ref,
    mean_ref,
    back_ref,
    ahead_ref,
    past_ref,
    out_ref,
    strain_ref,
    spec_ref,
    tau_ref,
    sem,
):
    for f, component in enumerate(FIRST_FIELDS):
        strain_ref[component] = z_back(in_ref, f, FIRST_ROWS, back_ref, spec_ref)

    def block(b, carry):
        rows = pl.ds(pl.multiple_of(b * 8, 8), 8)
        conc = cells_ref[rows, :]
        source = source_of(conc)
        trace = TRACE * (source - edge_ref[...] - mean_ref[...])
        strain = [strain_ref[f, rows, :] for f in range(6) if f != 2]
        strain.insert(2, trace - strain[0] - strain[1])
        strain_ref[2, rows, :] = strain[2]
        first = FIRST_LOW + FIRST_RISE * conc
        shear = SHEAR_LOW + SHEAR_RISE * conc
        normal = (first - FIRST_REF) * trace + source
        excess = 2.0 * (shear - SHEAR_REF)
        for f in range(6):
            tau = excess * strain[f]
            tau_ref[f, rows, :] = tau + normal if f < 3 else tau
        return carry

    lax.fori_loop(0, N // 8, block, 0)
    past = pltpu.make_async_copy(strain_ref, past_ref, sem)
    past.start()

    def ahead(f, carry):
        z_ahead(tau_ref[f], f, SWEEP_ROWS, ahead_ref, out_ref)
        return carry

    lax.fori_loop(0, 6, ahead, 0, unroll=UNROLL)
    past.wait()


def plane_green_kernel(place_ref, in_ref, ahead_ref, back_ref, out_ref, plane_ref, spec_ref):
    def ahead(f, carry):
        spec_ref[f, 0], spec_ref[f, 1] = plane_spectrum(
            in_ref, f, SWEEP_ROWS, ahead_ref, back_ref, plane_ref
        )
        return carry

    lax.fori_loop(0, 6, ahead, 0, unroll=UNROLL)

    def block(b, carry):
        start = pl.multiple_of(b * 8, 8)
        rows = pl.ds(start, 8)
        for branch in range(2):
            wave_x, wave_y, wave_z = waves(place_ref, branch, start, 8)
            square = wave_x * wave_x + wave_y * wave_y + wave_z * wave_z
            nonzero = square > 0.0
            safe = jnp.where(nonzero, square, 1.0)
            inverse = 1.0 / safe
            scale = jnp.where(nonzero, inverse * (1.0 / SHEAR_REF), 0.0)
            inverse = inverse * BETA_REF
            tau = [spec_ref[f, branch, rows, :] for f in range(6)]
            force_x = tau[0] * wave_x + tau[5] * wave_y + tau[4] * wave_z
            force_y = tau[5] * wave_x + tau[1] * wave_y + tau[3] * wave_z
            force_z = tau[4] * wave_x + tau[3] * wave_y + tau[2] * wave_z
            along = (wave_x * force_x + wave_y * force_y + wave_z * force_z) * inverse
            moved_x = scale * (along * wave_x - force_x)
            moved_y = scale * (along * wave_y - force_y)
            moved_z = scale * (along * wave_z - force_z)
            spec_ref[0, branch, rows, :] = wave_x * moved_x
            spec_ref[1, branch, rows, :] = wave_y * moved_y
            spec_ref[2, branch, rows, :] = wave_z * moved_z
            spec_ref[3, branch, rows, :] = 0.5 * (wave_y * moved_z + wave_z * moved_y)
            spec_ref[4, branch, rows, :] = 0.5 * (wave_x * moved_z + wave_z * moved_x)
            spec_ref[5, branch, rows, :] = 0.5 * (wave_x * moved_y + wave_y * moved_x)
        return carry

    lax.fori_loop(0, N // 8, block, 0)

    def back(f, carry):
        real, imag = y_back(spec_ref[f, 0], spec_ref[f, 1], ahead_ref)
        x_back(real, imag, f, SWEEP_ROWS, back_ref, plane_ref, out_ref)
        return carry

    lax.fori_loop(0, 6, back, 0, unroll=UNROLL)


def z_drive_kernel(
    in_ref,
    cells_ref,
    back_ref,
    ahead_ref,
    far_ref,
    out_ref,
    strain_ref,
    spec_ref,
    drive_ref,
    sems,
):
    def far(f):
        return pltpu.make_async_copy(strain_ref.at[f], far_ref.at[f], sems.at[f])

    def inverse(f, carry):
        strain_ref[f] = z_back(in_ref, f, SWEEP_ROWS, back_ref, spec_ref)
        far(f).start()
        return carry

    lax.fori_loop(0, 6, inverse, 0, unroll=UNROLL)

    def block(b, carry):
        rows = pl.ds(pl.multiple_of(b * 8, 8), 8)
        conc = cells_ref[rows, :]
        strain = [strain_ref[f, rows, :] for f in range(6)]
        first = FIRST_LOW + FIRST_RISE * conc
        shear = SHEAR_LOW + SHEAR_RISE * conc
        dilation = EIGEN_STRAIN * conc
        part = [strain[f] - dilation for f in range(3)]
        trace = part[0] + part[1] + part[2]
        energy = (
            part[0] * part[0]
            + part[1] * part[1]
            + part[2] * part[2]
            + 2.0 * (strain[3] * strain[3] + strain[4] * strain[4] + strain[5] * strain[5])
        )
        chemical = 2.0 * WELL_HEIGHT * conc * (1.0 - conc) * (1.0 - 2.0 * conc)
        drive_ref[rows, :] = (
            chemical
            + 0.5 * FIRST_RISE * trace * trace
            + SHEAR_RISE * energy
            - EIGEN_STRAIN * (3.0 * first + 2.0 * shear) * trace
        )
        return carry

    lax.fori_loop(0, N // 8, block, 0)
    z_ahead(drive_ref[...], 0, DRIVE_ROWS, ahead_ref, out_ref)
    for f in range(6):
        far(f).wait()


def aside_kernel(
    now_ref,
    then_ref,
    source_ref,
    ahead_ref,
    back_ref,
    strain_ref,
    conc_ref,
    sums_ref,
    cells_ref,
    past_ref,
    data_ref,
    lines_ref,
    plane_ref,
    now_sems,
    then_sems,
    source_sem,
    out_sems,
):
    def now(f):
        return pltpu.make_async_copy(now_ref.at[f], cells_ref.at[f], now_sems.at[f])

    def then(f):
        return pltpu.make_async_copy(then_ref.at[f], past_ref.at[f], then_sems.at[f])

    for f in range(6):
        now(f).start()
        then(f).start()
    source = pltpu.make_async_copy(source_ref, data_ref, source_sem)
    source.start()

    def one(f, totals):
        def block(b, totals):
            rows = pl.ds(pl.multiple_of(b * 8, 8), 8)
            past = past_ref[f, rows, :]
            change = cells_ref[f, rows, :] - past
            return totals[0] + past * past, totals[1] + change * change

        now(f).wait()
        lines_ref[f] = cells_ref[f].T.reshape(LOW, HIGH, LY, N)
        for copy in copy_lines(strain_ref.at[f], lines_ref.at[f], out_sems.at[f], False):
            copy.start()
        then(f).wait()
        return lax.fori_loop(0, N // 8, block, totals)

    zero = jnp.zeros((8, CELLS), F32)
    totals = lax.fori_loop(0, 6, one, (zero, zero))
    lane = lax.broadcasted_iota(jnp.int32, (1, LANES), 1)
    sums = jnp.where(lane < LANES // 2, squares(totals[0]), squares(totals[1]))
    sums_ref[...] = jnp.broadcast_to(sums, (8, LANES))
    source.wait()
    conc_ref[0], conc_ref[1] = plane_spectrum(
        data_ref, 1, SOURCE_ROWS, ahead_ref, back_ref, plane_ref
    )
    for f in range(6):
        for copy in copy_lines(strain_ref.at[f], lines_ref.at[f], out_sems.at[f], False):
            copy.wait()


def plane_update_kernel(
    place_ref, in_ref, conc_ref, sums_ref, ahead_ref, back_ref, out_ref, plane_ref
):
    data = list(plane_spectrum(in_ref, 0, DRIVE_ROWS, ahead_ref, back_ref, plane_ref))
    for b in range(2):
        wave_x, wave_y, wave_z = waves(place_ref, b, 0, N)
        square = wave_x * wave_x + wave_y * wave_y + wave_z * wave_z
        denominator = 1.0 + TIME_STEP * GRADIENT_ENERGY * square * square
        data[b] = (conc_ref[b] - TIME_STEP * square * data[b]) / denominator
    real, imag = y_back(data[0], data[1], ahead_ref)
    x_back(real, imag, 0, LAST_ROWS, back_ref, plane_ref, out_ref)
    out_ref[peers_of(LOW, LAST_ROWS), :] = jnp.broadcast_to(sums_ref[:1, :], (DEVICES, LANES))


def z_last_kernel(in_ref, back_ref, out_ref, norm_ref, spec_ref, lines_ref, sems):
    lines = z_back(in_ref, 0, LAST_ROWS, back_ref, spec_ref).T
    lines_ref[...] = lines.reshape(LOW, HIGH, LY, N)
    copies = copy_lines(out_ref, lines_ref, sems, False)
    for copy in copies:
        copy.start()
    sums = in_ref[peers_of(LOW, LAST_ROWS), :]
    lane = lax.broadcasted_iota(jnp.int32, sums.shape, 1)
    row = lax.broadcasted_iota(jnp.int32, (8, LANES), 0)
    first = jnp.sum(jnp.where(lane < LANES // 2, sums, 0.0))
    second = jnp.sum(jnp.where(lane < LANES // 2, 0.0, sums))
    norms = jnp.sqrt(jnp.where(row == 0, first, second) * (1.0 / float(N) ** 3))
    norm_ref[0] = norms[0, 0]
    norm_ref[1] = norms[1, 0]
    for copy in copies:
        copy.wait()


SPACES = {"vmem": pltpu.VMEM, "smem": pltpu.SMEM, "hbm": pltpu.HBM}


def call(kernel, name, args, outs, scratch=(), sems=(), mib=24):
    operands = [
        pltpu.with_memory_space_constraint(value, pltpu.HBM) if space == "hbm" else value
        for space, value in args
    ]
    return pl.pallas_call(
        kernel,
        out_shape=[
            pltpu.HBM(shape, F32) if space == "hbm" else jax.ShapeDtypeStruct(shape, F32)
            for space, shape in outs
        ],
        in_specs=[pl.BlockSpec(memory_space=SPACES[space]) for space, _ in args],
        out_specs=[pl.BlockSpec(memory_space=SPACES[space]) for space, _ in outs],
        scratch_shapes=[
            *[pltpu.VMEM(s, F32) if isinstance(s, tuple) else s for s in scratch],
            *[pltpu.SemaphoreType.DMA(shape) for shape in sems],
        ],
        name=name,
        interpret=INTERPRET,
        compiler_params=pltpu.CompilerParams(vmem_limit_bytes=mib * 1024 * 1024),
    )(*operands)


def exchange(array):
    rows = array.reshape(DEVICES, array.shape[0] // DEVICES * LANES)
    rows = lax.all_to_all(rows, AXES, split_axis=0, concat_axis=0, tiled=True)
    return rows.reshape(array.shape)


def wire(pitch):
    return (DEVICES * pitch, LANES)


BLOCK = (LX, LY, N)
CELL = (N, CELLS)
PLANE = (2, N, N)
LINES = (LOW, HIGH, LY, N)
SMALL = (8, CELLS)


def shards(concentration):
    tables = [jnp.asarray(table) for table in build_tables()]
    line_ahead, line_back, ahead, back = [("vmem", table) for table in tables]
    place = ("smem", lax.axis_index(AXES).astype(jnp.int32)[None])

    cells, data, edge = call(
        source_kernel,
        "source",
        [place, ("hbm", concentration), ("hbm", tables[2])],
        [("vmem", CELL), ("vmem", wire(SOURCE_ROWS)), ("vmem", SMALL)],
        [LINES, pltpu.VMEM((3, N, N), BF16)],
        [(HIGH,), ()],
    )
    source = exchange(data)
    data, mean = call(
        plane_first_kernel,
        "plane_first",
        [place, ("vmem", source), line_ahead, line_back],
        [("vmem", wire(FIRST_ROWS)), ("vmem", SMALL)],
        [PLANE, (3, *PLANE)],
    )
    data = exchange(data)
    past, data = call(
        z_sweep_kernel,
        "z_sweep",
        [("vmem", data), ("vmem", cells), ("vmem", edge), ("vmem", mean), back, ahead],
        [("hbm", (6, *CELL)), ("vmem", wire(SWEEP_ROWS))],
        [(6, *CELL), CELL, (6, *CELL)],
        [()],
    )
    data = exchange(data)
    (data,) = call(
        plane_green_kernel,
        "plane_green",
        [place, ("vmem", data), line_ahead, line_back],
        [("vmem", wire(SWEEP_ROWS))],
        [PLANE, (6, *PLANE)],
    )
    data = exchange(data)
    now, data = call(
        z_drive_kernel,
        "z_drive",
        [("vmem", data), ("vmem", cells), back, ahead],
        [("hbm", (6, *CELL)), ("vmem", wire(DRIVE_ROWS))],
        [(6, *CELL), CELL, CELL],
        [(6,)],
    )
    data = exchange(data)
    strain, conc_spec, sums = call(
        aside_kernel,
        "aside",
        [("hbm", now), ("hbm", past), ("hbm", source), line_ahead, line_back],
        [("hbm", (6, *BLOCK)), ("vmem", PLANE), ("vmem", (8, LANES))],
        [(6, *CELL), (6, *CELL), wire(SOURCE_ROWS), (6, *LINES), PLANE],
        [(6,), (6,), (), (6, HIGH)],
    )
    (data,) = call(
        plane_update_kernel,
        "plane_update",
        [place, ("vmem", data), ("vmem", conc_spec), ("vmem", sums), line_ahead, line_back],
        [("vmem", wire(LAST_ROWS))],
        [PLANE],
    )
    data = exchange(data)
    conc_next, norms = call(
        z_last_kernel,
        "z_last",
        [("vmem", data), back],
        [("hbm", BLOCK), ("smem", (2,))],
        [CELL, LINES],
        [(HIGH,)],
    )
    return conc_next, strain, norms


def solution(mesh):
    whole = Mesh(mesh.devices.reshape(4, 2, 4, 4), AXES)
    row, col = AXES[:2], AXES[2:]
    return jax.shard_map(
        shards,
        mesh=whole,
        in_specs=(P(row, col, None),),
        out_specs=(P(row, col, None), P(None, row, col, None), P()),
        check_vma=False,
    )
```

```python
import math
from functools import partial

import jax
import jax.numpy as jnp
import numpy as np
from jax import lax
from jax.experimental import pallas as pl
from jax.experimental.pallas import tpu as pltpu
from jax.sharding import Mesh
from jax.sharding import PartitionSpec as P

AXES = ("row_0", "row_1", "col_0", "col_1")

FIRST_LOW = 1.0
FIRST_RISE = 0.6
SHEAR_LOW = 0.7
SHEAR_RISE = 0.8
FIRST_REF = 1.3
SHEAR_REF = 1.1
BETA_REF = 2.4 / 3.5
EIGEN_STRAIN = 0.5
WELL_HEIGHT = 1.0
TIME_STEP = 0.5
GRADIENT_ENERGY = 0.5

N = 256
HALF = N // 2
ROWS = 8
COLS = 16
DEVICES = ROWS * COLS
LX = N // ROWS
LY = N // COLS
LOW = 8
HIGH = LX // LOW
CELLS = LX * LY
LANES = 128
UNIT = 2.0 * math.pi / N
F32 = jnp.float32
BF16 = jnp.bfloat16
INTERPRET = False
PLANE_UNROLL = 6
SWEEP_UNROLL = 3
DRIVE_UNROLL = 6
SOURCE_ROWS = 2 * LOW + 1
FIRST_ROWS = 5 * LOW
SWEEP_ROWS = 6 * LOW
DRIVE_ROWS = LOW
LAST_ROWS = LOW + 1
FIRST_FIELDS = (0, 1, 3, 4, 5)
TRACE = -(1.0 - BETA_REF) / SHEAR_REF


def pieces_of(table, count):
    rest = table.astype(np.float32)
    pieces = []
    for _ in range(count):
        piece = rest.astype(jnp.bfloat16)
        rest = rest - piece.astype(np.float32)
        pieces.append(piece)
    return np.stack(pieces)


def build_tables():
    index = np.arange(N)
    half = np.arange(HALF)
    angle = 2.0 * np.pi / N * (index[:, None] * index[None, :] % N)
    cosine = np.cos(angle)
    sine = np.sin(angle)
    lines = []
    for odd in range(2):
        angle = 2.0 * np.pi / N * ((2 * half[:, None] + odd) * half[None, :] % N)
        lines.append(
            np.block([[np.cos(angle), np.sin(angle)], [-np.sin(angle), np.cos(angle)]])
        )
    line_ahead = np.stack([pieces_of(line, 2) for line in lines])
    ahead = np.concatenate([cosine[:HALF], -sine[:HALF]], axis=0)
    return line_ahead, pieces_of(ahead, 3)


def split(value, count):
    pieces = []
    for i in range(count):
        piece = value.astype(BF16)
        pieces.append(piece)
        if i + 1 < count:
            value = value - piece.astype(F32)
    return pieces


def product(left, right):
    count = len(right)
    total = None
    for order in reversed(range(count)):
        for i in range(order + 1):
            term = jnp.dot(left[i], right[order - i], preferred_element_type=F32)
            total = term if total is None else total + term
    return total


def table(ref):
    return [ref[i] for i in range(ref.shape[0])]


def swap_lanes(parts, granule):
    parts = list(parts)
    axis = parts[0].ndim - 1
    lane = lax.broadcasted_iota(jnp.int32, parts[0].shape, axis)
    step = 1
    while step < len(parts):
        width = granule * step
        low = (lane & width) == 0
        for i in range(len(parts)):
            if i & step == 0:
                a, b = parts[i], parts[i + step]
                parts[i] = jnp.where(low, a, pltpu.roll(b, width, axis))
                parts[i + step] = jnp.where(low, pltpu.roll(a, LANES - width, axis), b)
        step *= 2
    return parts


def peers_of(row, pitch):
    return pl.ds(row, DEVICES, stride=pitch)


def z_ahead(value, f, pitch, ahead_ref, out_ref):
    spectrum = product(table(ahead_ref), split(value, 3))
    for t in range(LOW // 2):
        lanes = slice(t * LANES, (t + 1) * LANES)
        parts = swap_lanes([spectrum[:HALF, lanes], spectrum[HALF:, lanes]], LANES // 2)
        for i in range(2):
            out_ref[peers_of(f * LOW + 2 * t + i, pitch), :] = parts[i]


def z_back(in_ref, f, pitch, back_ref, spec_ref):
    for t in range(LOW // 2):
        lanes = slice(t * LANES, (t + 1) * LANES)
        parts = [in_ref[peers_of(f * LOW + 2 * t + i, pitch), :] for i in range(2)]
        real, imag = swap_lanes(parts, LANES // 2)
        spec_ref[:HALF, lanes] = real
        spec_ref[HALF:, lanes] = imag
    return product(table(back_ref), split(spec_ref[...], 2))


def rows_of(peer, f, pitch):
    start = peer * pitch + f * LOW
    return pl.ds(start if isinstance(start, int) else pl.multiple_of(start, LOW), LOW)


def plane_row(part, i, high):
    return part * HALF + i % 4 * LX + high * LOW


def plane_ahead(in_ref, f, pitch, ahead_ref, plane_ref):
    for i in range(ROWS // 2):
        for h in range(2):
            near, far = [
                swap_lanes(
                    [in_ref[rows_of(k * COLS + h * 8 + j, f, pitch), :] for j in range(8)], LY
                )
                for k in (i, i + ROWS // 2)
            ]
            for g in range(8):
                row = plane_row(g // HIGH, i, g % HIGH)
                lanes = slice(h * LANES, (h + 1) * LANES)
                plane_ref[0, row : row + LOW, lanes] = near[g] + far[g]
                plane_ref[1, row : row + LOW, lanes] = near[g] - far[g]
    near, far = [], []
    for b in range(2):
        lines = product(table(ahead_ref.at[b]), split(plane_ref[b], 2))
        near.append(jnp.concatenate([lines[:HALF, :HALF], lines[HALF:, :HALF]], axis=1))
        far.append(jnp.concatenate([lines[:HALF, HALF:], lines[HALF:, HALF:]], axis=1))
    near = jnp.concatenate(near, axis=0)
    far = jnp.concatenate(far, axis=0)
    return near + far, near - far


def plane_spectrum(in_ref, f, pitch, ahead_ref, back_ref, plane_ref):
    even, odd = plane_ahead(in_ref, f, pitch, ahead_ref, plane_ref)
    return (
        product(split(even, 2), table(back_ref.at[0])),
        product(split(odd, 2), table(back_ref.at[1])),
    )


def y_back(even, odd, ahead_ref):
    even = product(split(even, 2), table(ahead_ref.at[0]))
    odd = product(split(odd, 2), table(ahead_ref.at[1]))
    near = even + odd
    far = even - odd
    return (
        jnp.concatenate([near[:, :HALF], far[:, :HALF]], axis=1),
        jnp.concatenate([near[:, HALF:], far[:, HALF:]], axis=1),
    )


def x_back(real, imag, f, pitch, back_ref, plane_ref, out_ref):
    lines = []
    for b in range(2):
        rows = slice(b * HALF, (b + 1) * HALF)
        data = jnp.concatenate([real[rows], imag[rows]], axis=0)
        lines.append(product(table(back_ref.at[b]), split(data, 2)))
    plane_ref[0] = lines[0] + lines[1]
    plane_ref[1] = lines[0] - lines[1]
    for i in range(ROWS):
        for h in range(2):
            parts = []
            for g in range(8):
                row = plane_row(g // HIGH, i, g % HIGH)
                parts.append(plane_ref[i // 4, row : row + LOW, h * LANES : (h + 1) * LANES])
            parts = swap_lanes(parts, LY)
            for j in range(8):
                out_ref[rows_of(i * COLS + h * 8 + j, f, pitch), :] = parts[j]


def each(count, unroll, body):
    def step(i, carry):
        for slot in range(unroll):
            body(i * unroll + slot, slot)
        return carry

    if count == unroll:
        step(0, 0)
    else:
        lax.fori_loop(0, count // unroll, step, 0)


def signed(index):
    return jnp.where(index < HALF, index, index - N).astype(F32) * UNIT


def row_waves(start, count, lanes):
    row = lax.broadcasted_iota(jnp.int32, (count, lanes), 0) + start
    return signed(2 * (row % HALF) + row // HALF)


def waves(place_ref, branch, start, count):
    shape = (count, N)
    lane = lax.broadcasted_iota(jnp.int32, shape, 1)
    wave_y = signed(2 * (lane % HALF) + branch)
    wave_z = jnp.full(shape, place_ref[0], jnp.int32).astype(F32) * UNIT
    return row_waves(start, count, N), wave_y, wave_z


def squares(total):
    total = sum(total[:, t * LANES : (t + 1) * LANES] for t in range(CELLS // LANES))
    total = jnp.sum(total, axis=0, keepdims=True)
    return total + pltpu.roll(total, LANES // 2, 1)


def source_of(conc):
    first = FIRST_LOW + FIRST_RISE * conc
    shear = SHEAR_LOW + SHEAR_RISE * conc
    return -(3.0 * first + 2.0 * shear) * EIGEN_STRAIN * conc


def copy_lines(far, lines_ref, sems, inward):
    copies = []
    for high in range(HIGH):
        pair = (far.at[pl.ds(high * LOW, LOW)], lines_ref.at[:, high])
        source, target = pair if inward else pair[::-1]
        copies.append(pltpu.make_async_copy(source, target, sems.at[high]))
    return copies


def source_kernel(
    place_ref,
    conc_ref,
    far_ref,
    far_line_ref,
    cells_ref,
    out_ref,
    edge_ref,
    back_ref,
    ahead_ref,
    line_ref,
    line_back_ref,
    lines_ref,
    sems,
    far_sem,
    line_sem,
):
    copies = copy_lines(conc_ref, lines_ref, sems, True)
    copies.append(pltpu.make_async_copy(far_ref, ahead_ref, far_sem))
    line = pltpu.make_async_copy(far_line_ref, line_ref, line_sem)
    for copy in copies:
        copy.start()
    line.start()
    for copy in copies:
        copy.wait()
    conc = lines_ref[...].reshape(CELLS, N).T
    cells_ref[...] = conc
    source = source_of(conc)
    total = jnp.sum(source.reshape(N // 8, 8, CELLS), axis=0)
    row = lax.broadcasted_iota(jnp.int32, (8, CELLS), 0)
    edge = jnp.where(row % 2 == 0, total, -total)
    edge = jnp.sum(edge, axis=0, keepdims=True) * (1.0 / N)
    edge_ref[...] = jnp.where(row % 2 == 0, edge, -edge)
    total = sum(total[:, t * LANES : (t + 1) * LANES] for t in range(CELLS // LANES))
    total = jnp.sum(total, axis=0, keepdims=True)
    out_ref[peers_of(2 * LOW, SOURCE_ROWS), :] = jnp.broadcast_to(total, (DEVICES, LANES))
    z_ahead(source, 0, SOURCE_ROWS, ahead_ref, out_ref)
    z_ahead(conc, 1, SOURCE_ROWS, ahead_ref, out_ref)
    lane = lax.broadcasted_iota(jnp.int32, (N, N), 1)
    weight = jnp.where(lane % HALF == 0, 1.0, 2.0) * (1.0 / float(N) ** 3)
    for i in range(2):
        back_ref[i] = (ahead_ref[i].astype(F32).T * weight).astype(BF16)
    line.wait()
    for b in range(2):
        for i in range(2):
            line_back_ref[b, i] = line_ref[b, i].astype(F32).T.astype(BF16)


def plane_first_kernel(
    place_ref, in_ref, ahead_ref, back_ref, out_ref, mean_ref, plane_ref, line_ref
):
    mean = jnp.sum(in_ref[peers_of(2 * LOW, SOURCE_ROWS), :]) * (1.0 / float(N) ** 3)
    mean_ref[...] = jnp.full((8, CELLS), mean, F32)
    data = list(plane_spectrum(in_ref, 0, SOURCE_ROWS, ahead_ref, back_ref, plane_ref.at[5]))
    wave_y = []
    for b in range(2):
        wave_x, wave, wave_z = waves(place_ref, b, 0, N)
        wave_y.append(wave)
        square = wave_x * wave_x + wave * wave + wave_z * wave_z
        nonzero = square > 0.0
        safe = jnp.where(nonzero, square, 1.0)
        data[b] = data[b] * jnp.where(nonzero, TRACE / safe, 0.0)
    for power in range(3):
        if power:
            data = [data[b] * wave_y[b] for b in range(2)]
        line_ref[power, 0], line_ref[power, 1] = y_back(data[0], data[1], ahead_ref)
    wave_x = row_waves(0, N, N)
    wave_z = jnp.full((N, N), place_ref[0], jnp.int32).astype(F32) * UNIT
    plan = ((2, 0, 0), (0, 2, 0), (0, 1, 1), (1, 0, 1), (1, 1, 0))
    for f, (power_x, power_y, power_z) in enumerate(plan):
        real = line_ref[power_y, 0]
        imag = line_ref[power_y, 1]
        factor = None
        for wave in [wave_x] * power_x + [wave_z] * power_z:
            factor = wave if factor is None else factor * wave
        if factor is not None:
            real = real * factor
            imag = imag * factor
        x_back(real, imag, f, FIRST_ROWS, back_ref, plane_ref.at[f], out_ref)


def z_sweep_kernel(
    in_ref,
    cells_ref,
    edge_ref,
    mean_ref,
    back_ref,
    ahead_ref,
    past_ref,
    out_ref,
    strain_ref,
    spec_ref,
    tau_ref,
    sem,
):
    for f, component in enumerate(FIRST_FIELDS):
        spec = spec_ref.at[f]
        strain_ref[component] = z_back(in_ref, f, FIRST_ROWS, back_ref, spec)

    def block(b, carry):
        rows = pl.ds(pl.multiple_of(b * 8, 8), 8)
        conc = cells_ref[rows, :]
        source = source_of(conc)
        trace = TRACE * (source - edge_ref[...] - mean_ref[...])
        strain = [strain_ref[f, rows, :] for f in range(6) if f != 2]
        strain.insert(2, trace - strain[0] - strain[1])
        strain_ref[2, rows, :] = strain[2]
        first = FIRST_LOW + FIRST_RISE * conc
        shear = SHEAR_LOW + SHEAR_RISE * conc
        normal = (first - FIRST_REF) * trace + source
        excess = 2.0 * (shear - SHEAR_REF)
        for f in range(6):
            tau = excess * strain[f]
            tau_ref[f, rows, :] = tau + normal if f < 3 else tau
        return carry

    lax.fori_loop(0, N // 8, block, 0)
    past = pltpu.make_async_copy(strain_ref, past_ref, sem)
    past.start()

    def ahead(f, slot):
        z_ahead(tau_ref[f], f, SWEEP_ROWS, ahead_ref, out_ref)

    each(6, SWEEP_UNROLL, ahead)
    past.wait()


def plane_green_kernel(place_ref, in_ref, ahead_ref, back_ref, out_ref, plane_ref, spec_ref):
    def ahead(f, slot):
        spec_ref[f, 0], spec_ref[f, 1] = plane_spectrum(
            in_ref, f, SWEEP_ROWS, ahead_ref, back_ref, plane_ref.at[slot]
        )

    each(6, PLANE_UNROLL, ahead)

    def block(b, carry):
        start = pl.multiple_of(b * 8, 8)
        rows = pl.ds(start, 8)
        for branch in range(2):
            wave_x, wave_y, wave_z = waves(place_ref, branch, start, 8)
            square = wave_x * wave_x + wave_y * wave_y + wave_z * wave_z
            nonzero = square > 0.0
            safe = jnp.where(nonzero, square, 1.0)
            inverse = 1.0 / safe
            scale = jnp.where(nonzero, inverse * (1.0 / SHEAR_REF), 0.0)
            inverse = inverse * BETA_REF
            tau = [spec_ref[f, branch, rows, :] for f in range(6)]
            force_x = tau[0] * wave_x + tau[5] * wave_y + tau[4] * wave_z
            force_y = tau[5] * wave_x + tau[1] * wave_y + tau[3] * wave_z
            force_z = tau[4] * wave_x + tau[3] * wave_y + tau[2] * wave_z
            along = (wave_x * force_x + wave_y * force_y + wave_z * force_z) * inverse
            moved_x = scale * (along * wave_x - force_x)
            moved_y = scale * (along * wave_y - force_y)
            moved_z = scale * (along * wave_z - force_z)
            spec_ref[0, branch, rows, :] = wave_x * moved_x
            spec_ref[1, branch, rows, :] = wave_y * moved_y
            spec_ref[2, branch, rows, :] = wave_z * moved_z
            spec_ref[3, branch, rows, :] = 0.5 * (wave_y * moved_z + wave_z * moved_y)
            spec_ref[4, branch, rows, :] = 0.5 * (wave_x * moved_z + wave_z * moved_x)
            spec_ref[5, branch, rows, :] = 0.5 * (wave_x * moved_y + wave_y * moved_x)
        return carry

    lax.fori_loop(0, N // 8, block, 0)

    def back(f, slot):
        real, imag = y_back(spec_ref[f, 0], spec_ref[f, 1], ahead_ref)
        x_back(real, imag, f, SWEEP_ROWS, back_ref, plane_ref.at[slot], out_ref)

    each(6, PLANE_UNROLL, back)


def z_drive_kernel(
    in_ref,
    cells_ref,
    back_ref,
    ahead_ref,
    far_ref,
    out_ref,
    strain_ref,
    spec_ref,
    drive_ref,
    sems,
):
    def far(f):
        return pltpu.make_async_copy(strain_ref.at[f], far_ref.at[f], sems.at[f])

    def inverse(f, slot):
        strain_ref[f] = z_back(in_ref, f, SWEEP_ROWS, back_ref, spec_ref.at[slot])
        far(f).start()

    each(6, DRIVE_UNROLL, inverse)

    def block(b, carry):
        rows = pl.ds(pl.multiple_of(b * 8, 8), 8)
        conc = cells_ref[rows, :]
        strain = [strain_ref[f, rows, :] for f in range(6)]
        first = FIRST_LOW + FIRST_RISE * conc
        shear = SHEAR_LOW + SHEAR_RISE * conc
        dilation = EIGEN_STRAIN * conc
        part = [strain[f] - dilation for f in range(3)]
        trace = part[0] + part[1] + part[2]
        energy = (
            part[0] * part[0]
            + part[1] * part[1]
            + part[2] * part[2]
            + 2.0 * (strain[3] * strain[3] + strain[4] * strain[4] + strain[5] * strain[5])
        )
        chemical = 2.0 * WELL_HEIGHT * conc * (1.0 - conc) * (1.0 - 2.0 * conc)
        drive_ref[rows, :] = (
            chemical
            + 0.5 * FIRST_RISE * trace * trace
            + SHEAR_RISE * energy
            - EIGEN_STRAIN * (3.0 * first + 2.0 * shear) * trace
        )
        return carry

    lax.fori_loop(0, N // 8, block, 0)
    z_ahead(drive_ref[...], 0, DRIVE_ROWS, ahead_ref, out_ref)
    for f in range(6):
        far(f).wait()


def aside_kernel(
    now_ref,
    then_ref,
    source_ref,
    ahead_ref,
    back_ref,
    strain_ref,
    conc_ref,
    sums_ref,
    cells_ref,
    past_ref,
    data_ref,
    lines_ref,
    plane_ref,
    now_sems,
    then_sems,
    source_sem,
    out_sems,
):
    def now(f):
        return pltpu.make_async_copy(now_ref.at[f], cells_ref.at[f], now_sems.at[f])

    def then(f):
        return pltpu.make_async_copy(then_ref.at[f], past_ref.at[f], then_sems.at[f])

    for f in range(6):
        now(f).start()
        then(f).start()
    source = pltpu.make_async_copy(source_ref, data_ref, source_sem)
    source.start()

    def one(f, totals):
        def block(b, totals):
            rows = pl.ds(pl.multiple_of(b * 8, 8), 8)
            past = past_ref[f, rows, :]
            change = cells_ref[f, rows, :] - past
            return totals[0] + past * past, totals[1] + change * change

        now(f).wait()
        lines_ref[f] = cells_ref[f].T.reshape(LOW, HIGH, LY, N)
        for copy in copy_lines(strain_ref.at[f], lines_ref.at[f], out_sems.at[f], False):
            copy.start()
        then(f).wait()
        return lax.fori_loop(0, N // 8, block, totals)

    zero = jnp.zeros((8, CELLS), F32)
    totals = lax.fori_loop(0, 6, one, (zero, zero))
    lane = lax.broadcasted_iota(jnp.int32, (1, LANES), 1)
    sums = jnp.where(lane < LANES // 2, squares(totals[0]), squares(totals[1]))
    sums_ref[...] = jnp.broadcast_to(sums, (8, LANES))
    source.wait()
    conc_ref[0], conc_ref[1] = plane_spectrum(
        data_ref, 1, SOURCE_ROWS, ahead_ref, back_ref, plane_ref
    )
    for f in range(6):
        for copy in copy_lines(strain_ref.at[f], lines_ref.at[f], out_sems.at[f], False):
            copy.wait()


def plane_update_kernel(
    place_ref, in_ref, conc_ref, sums_ref, ahead_ref, back_ref, out_ref, plane_ref
):
    data = list(plane_spectrum(in_ref, 0, DRIVE_ROWS, ahead_ref, back_ref, plane_ref))
    for b in range(2):
        wave_x, wave_y, wave_z = waves(place_ref, b, 0, N)
        square = wave_x * wave_x + wave_y * wave_y + wave_z * wave_z
        denominator = 1.0 + TIME_STEP * GRADIENT_ENERGY * square * square
        data[b] = (conc_ref[b] - TIME_STEP * square * data[b]) / denominator
    real, imag = y_back(data[0], data[1], ahead_ref)
    x_back(real, imag, 0, LAST_ROWS, back_ref, plane_ref, out_ref)
    out_ref[peers_of(LOW, LAST_ROWS), :] = jnp.broadcast_to(sums_ref[:1, :], (DEVICES, LANES))


def z_last_kernel(in_ref, back_ref, out_ref, norm_ref, spec_ref, lines_ref, sems):
    lines = z_back(in_ref, 0, LAST_ROWS, back_ref, spec_ref).T
    lines_ref[...] = lines.reshape(LOW, HIGH, LY, N)
    copies = copy_lines(out_ref, lines_ref, sems, False)
    for copy in copies:
        copy.start()
    sums = in_ref[peers_of(LOW, LAST_ROWS), :]
    lane = lax.broadcasted_iota(jnp.int32, sums.shape, 1)
    row = lax.broadcasted_iota(jnp.int32, (8, LANES), 0)
    first = jnp.sum(jnp.where(lane < LANES // 2, sums, 0.0))
    second = jnp.sum(jnp.where(lane < LANES // 2, 0.0, sums))
    norms = jnp.sqrt(jnp.where(row == 0, first, second) * (1.0 / float(N) ** 3))
    norm_ref[0] = norms[0, 0]
    norm_ref[1] = norms[1, 0]
    for copy in copies:
        copy.wait()


SPACES = {"vmem": pltpu.VMEM, "smem": pltpu.SMEM, "hbm": pltpu.HBM}


def call(kernel, name, args, outs, scratch=(), sems=(), mib=24):
    operands = [
        pltpu.with_memory_space_constraint(value, pltpu.HBM) if space == "hbm" else value
        for space, value in args
    ]
    return pl.pallas_call(
        kernel,
        out_shape=[
            pltpu.HBM(shape, F32) if space == "hbm" else jax.ShapeDtypeStruct(shape, *kind or (F32,))
            for space, shape, *kind in outs
        ],
        in_specs=[pl.BlockSpec(memory_space=SPACES[space]) for space, _ in args],
        out_specs=[pl.BlockSpec(memory_space=SPACES[space]) for space, *_ in outs],
        scratch_shapes=[
            *[pltpu.VMEM(s, F32) if isinstance(s, tuple) else s for s in scratch],
            *[pltpu.SemaphoreType.DMA(shape) for shape in sems],
        ],
        name=name,
        interpret=INTERPRET,
        compiler_params=pltpu.CompilerParams(vmem_limit_bytes=mib * 1024 * 1024),
    )(*operands)


def exchange(array):
    rows = array.reshape(DEVICES, array.shape[0] // DEVICES * LANES)
    rows = lax.all_to_all(rows, AXES, split_axis=0, concat_axis=0, tiled=True)
    return rows.reshape(array.shape)


def wire(pitch):
    return (DEVICES * pitch, LANES)


BLOCK = (LX, LY, N)
CELL = (N, CELLS)
PLANE = (2, N, N)
LINES = (LOW, HIGH, LY, N)
SMALL = (8, CELLS)


def shards(concentration):
    tables = [jnp.asarray(table) for table in build_tables()]
    place = ("smem", lax.axis_index(AXES).astype(jnp.int32)[None])

    cells, data, edge, *tables = call(
        source_kernel,
        "source",
        [place, ("hbm", concentration), ("hbm", tables[1]), ("hbm", tables[0])],
        [
            ("vmem", CELL),
            ("vmem", wire(SOURCE_ROWS)),
            ("vmem", SMALL),
            ("vmem", (2, N, N), BF16),
            ("vmem", (3, N, N), BF16),
            ("vmem", (2, 2, N, N), BF16),
            ("vmem", (2, 2, N, N), BF16),
        ],
        [LINES],
        [(HIGH,), (), ()],
    )
    back, ahead, line_ahead, line_back = [("vmem", table) for table in tables]
    source = exchange(data)
    data, mean = call(
        plane_first_kernel,
        "plane_first",
        [place, ("vmem", source), line_ahead, line_back],
        [("vmem", wire(FIRST_ROWS)), ("vmem", SMALL)],
        [(6, *PLANE), (3, *PLANE)],
    )
    data = exchange(data)
    past, data = call(
        z_sweep_kernel,
        "z_sweep",
        [("vmem", data), ("vmem", cells), ("vmem", edge), ("vmem", mean), back, ahead],
        [("hbm", (6, *CELL)), ("vmem", wire(SWEEP_ROWS))],
        [(6, *CELL), (5, *CELL), (6, *CELL)],
        [()],
    )
    data = exchange(data)
    (data,) = call(
        plane_green_kernel,
        "plane_green",
        [place, ("vmem", data), line_ahead, line_back],
        [("vmem", wire(SWEEP_ROWS))],
        [(PLANE_UNROLL, *PLANE), (6, *PLANE)],
    )
    data = exchange(data)
    now, data = call(
        z_drive_kernel,
        "z_drive",
        [("vmem", data), ("vmem", cells), back, ahead],
        [("hbm", (6, *CELL)), ("vmem", wire(DRIVE_ROWS))],
        [(6, *CELL), (DRIVE_UNROLL, *CELL), CELL],
        [(6,)],
    )
    data = exchange(data)
    strain, conc_spec, sums = call(
        aside_kernel,
        "aside",
        [("hbm", now), ("hbm", past), ("hbm", source), line_ahead, line_back],
        [("hbm", (6, *BLOCK)), ("vmem", PLANE), ("vmem", (8, LANES))],
        [(6, *CELL), (6, *CELL), wire(SOURCE_ROWS), (6, *LINES), PLANE],
        [(6,), (6,), (), (6, HIGH)],
    )
    (data,) = call(
        plane_update_kernel,
        "plane_update",
        [place, ("vmem", data), ("vmem", conc_spec), ("vmem", sums), line_ahead, line_back],
        [("vmem", wire(LAST_ROWS))],
        [PLANE],
    )
    data = exchange(data)
    conc_next, norms = call(
        z_last_kernel,
        "z_last",
        [("vmem", data), back],
        [("hbm", BLOCK), ("smem", (2,))],
        [CELL, LINES],
        [(HIGH,)],
    )
    return conc_next, strain, norms


def solution(mesh):
    whole = Mesh(mesh.devices.reshape(4, 2, 4, 4), AXES)
    row, col = AXES[:2], AXES[2:]
    return jax.shard_map(
        shards,
        mesh=whole,
        in_specs=(P(row, col, None),),
        out_specs=(P(row, col, None), P(None, row, col, None), P()),
        check_vma=False,
    )
```

```python
import math
from functools import partial

import jax
import jax.numpy as jnp
import numpy as np
from jax import lax
from jax.experimental import pallas as pl
from jax.experimental.pallas import tpu as pltpu
from jax.sharding import Mesh
from jax.sharding import PartitionSpec as P

AXES = ("row_0", "row_1", "col_0", "col_1")

FIRST_LOW = 1.0
FIRST_RISE = 0.6
SHEAR_LOW = 0.7
SHEAR_RISE = 0.8
FIRST_REF = 1.3
SHEAR_REF = 1.1
BETA_REF = 2.4 / 3.5
EIGEN_STRAIN = 0.5
WELL_HEIGHT = 1.0
TIME_STEP = 0.5
GRADIENT_ENERGY = 0.5

N = 256
HALF = N // 2
ROWS = 8
COLS = 16
DEVICES = ROWS * COLS
LX = N // ROWS
LY = N // COLS
LOW = 8
HIGH = LX // LOW
CELLS = LX * LY
LANES = 128
UNIT = 2.0 * math.pi / N
F32 = jnp.float32
BF16 = jnp.bfloat16
INTERPRET = False
PLANE_UNROLL = 6
SWEEP_UNROLL = 3
DRIVE_UNROLL = 6
BLOCK_UNROLL = 2
SOURCE_ROWS = 2 * LOW + 1
FIRST_ROWS = 5 * LOW
SWEEP_ROWS = 6 * LOW
DRIVE_ROWS = LOW
LAST_ROWS = LOW + 1
FIRST_FIELDS = (0, 1, 3, 4, 5)
TRACE = -(1.0 - BETA_REF) / SHEAR_REF


def pieces_of(table, count):
    rest = table.astype(np.float32)
    pieces = []
    for _ in range(count):
        piece = rest.astype(jnp.bfloat16)
        rest = rest - piece.astype(np.float32)
        pieces.append(piece)
    return np.stack(pieces)


def build_tables():
    index = np.arange(N)
    half = np.arange(HALF)
    angle = 2.0 * np.pi / N * (index[:, None] * index[None, :] % N)
    cosine = np.cos(angle)
    sine = np.sin(angle)
    lines = []
    for odd in range(2):
        angle = 2.0 * np.pi / N * ((2 * half[:, None] + odd) * half[None, :] % N)
        lines.append(
            np.block([[np.cos(angle), np.sin(angle)], [-np.sin(angle), np.cos(angle)]])
        )
    line_ahead = np.stack([pieces_of(line, 2) for line in lines])
    ahead = np.concatenate([cosine[:HALF], -sine[:HALF]], axis=0)
    return line_ahead, pieces_of(ahead, 3)


def split(value, count):
    pieces = []
    for i in range(count):
        piece = value.astype(BF16)
        pieces.append(piece)
        if i + 1 < count:
            value = value - piece.astype(F32)
    return pieces


def product(left, right):
    count = len(right)
    total = None
    for order in reversed(range(count)):
        for i in range(order + 1):
            term = jnp.dot(left[i], right[order - i], preferred_element_type=F32)
            total = term if total is None else total + term
    return total


def table(ref):
    return [ref[i] for i in range(ref.shape[0])]


def swap_lanes(parts, granule):
    parts = list(parts)
    axis = parts[0].ndim - 1
    lane = lax.broadcasted_iota(jnp.int32, parts[0].shape, axis)
    step = 1
    while step < len(parts):
        width = granule * step
        low = (lane & width) == 0
        for i in range(len(parts)):
            if i & step == 0:
                a, b = parts[i], parts[i + step]
                parts[i] = jnp.where(low, a, pltpu.roll(b, width, axis))
                parts[i + step] = jnp.where(low, pltpu.roll(a, LANES - width, axis), b)
        step *= 2
    return parts


def peers_of(row, pitch):
    return pl.ds(row, DEVICES, stride=pitch)


def z_ahead(value, f, pitch, pieces, ahead_ref, out_ref):
    spectrum = product(table(ahead_ref), split(value, pieces))
    for t in range(LOW // 2):
        lanes = slice(t * LANES, (t + 1) * LANES)
        parts = swap_lanes([spectrum[:HALF, lanes], spectrum[HALF:, lanes]], LANES // 2)
        for i in range(2):
            out_ref[peers_of(f * LOW + 2 * t + i, pitch), :] = parts[i]


def z_back(in_ref, f, pitch, back_ref, spec_ref):
    for t in range(LOW // 2):
        lanes = slice(t * LANES, (t + 1) * LANES)
        parts = [in_ref[peers_of(f * LOW + 2 * t + i, pitch), :] for i in range(2)]
        real, imag = swap_lanes(parts, LANES // 2)
        spec_ref[:HALF, lanes] = real
        spec_ref[HALF:, lanes] = imag
    return product(table(back_ref), split(spec_ref[...], 2))


def rows_of(peer, f, pitch):
    start = peer * pitch + f * LOW
    return pl.ds(start if isinstance(start, int) else pl.multiple_of(start, LOW), LOW)


def plane_row(part, i, high):
    return part * HALF + i % 4 * LX + high * LOW


def plane_ahead(in_ref, f, pitch, ahead_ref, plane_ref):
    for i in range(ROWS // 2):
        for h in range(2):
            near, far = [
                swap_lanes(
                    [in_ref[rows_of(k * COLS + h * 8 + j, f, pitch), :] for j in range(8)], LY
                )
                for k in (i, i + ROWS // 2)
            ]
            for g in range(8):
                row = plane_row(g // HIGH, i, g % HIGH)
                lanes = slice(h * LANES, (h + 1) * LANES)
                plane_ref[0, row : row + LOW, lanes] = near[g] + far[g]
                plane_ref[1, row : row + LOW, lanes] = near[g] - far[g]
    near, far = [], []
    for b in range(2):
        lines = product(table(ahead_ref.at[b]), split(plane_ref[b], 2))
        near.append(jnp.concatenate([lines[:HALF, :HALF], lines[HALF:, :HALF]], axis=1))
        far.append(jnp.concatenate([lines[:HALF, HALF:], lines[HALF:, HALF:]], axis=1))
    near = jnp.concatenate(near, axis=0)
    far = jnp.concatenate(far, axis=0)
    return near + far, near - far


def plane_spectrum(in_ref, f, pitch, ahead_ref, back_ref, plane_ref):
    even, odd = plane_ahead(in_ref, f, pitch, ahead_ref, plane_ref)
    return (
        product(split(even, 2), table(back_ref.at[0])),
        product(split(odd, 2), table(back_ref.at[1])),
    )


def y_back(even, odd, ahead_ref):
    even = product(split(even, 2), table(ahead_ref.at[0]))
    odd = product(split(odd, 2), table(ahead_ref.at[1]))
    near = even + odd
    far = even - odd
    return (
        jnp.concatenate([near[:, :HALF], far[:, :HALF]], axis=1),
        jnp.concatenate([near[:, HALF:], far[:, HALF:]], axis=1),
    )


def x_back(real, imag, f, pitch, back_ref, plane_ref, out_ref):
    lines = []
    for b in range(2):
        rows = slice(b * HALF, (b + 1) * HALF)
        data = jnp.concatenate([real[rows], imag[rows]], axis=0)
        lines.append(product(table(back_ref.at[b]), split(data, 2)))
    plane_ref[0] = lines[0] + lines[1]
    plane_ref[1] = lines[0] - lines[1]
    for i in range(ROWS):
        for h in range(2):
            parts = []
            for g in range(8):
                row = plane_row(g // HIGH, i, g % HIGH)
                parts.append(plane_ref[i // 4, row : row + LOW, h * LANES : (h + 1) * LANES])
            parts = swap_lanes(parts, LY)
            for j in range(8):
                out_ref[rows_of(i * COLS + h * 8 + j, f, pitch), :] = parts[j]


def each(count, unroll, body):
    def step(i, carry):
        for slot in range(unroll):
            body(i * unroll + slot, slot)
        return carry

    if count == unroll:
        step(0, 0)
    else:
        lax.fori_loop(0, count // unroll, step, 0)


def signed(index):
    return jnp.where(index < HALF, index, index - N).astype(F32) * UNIT


def row_waves(start, count):
    row = lax.broadcasted_iota(jnp.int32, (count, LANES), 0) + start
    return signed(2 * (row % HALF) + row // HALF)


def lane_waves(branch, count):
    return signed(2 * lax.broadcasted_iota(jnp.int32, (count, LANES), 1) + branch)


def depth_wave(place_ref, count):
    return jnp.full((count, LANES), place_ref[0], jnp.int32).astype(F32) * UNIT


def twice(half):
    return jnp.concatenate([half, half], axis=1)


def squares(total):
    total = sum(total[:, t * LANES : (t + 1) * LANES] for t in range(CELLS // LANES))
    total = jnp.sum(total, axis=0, keepdims=True)
    return total + pltpu.roll(total, LANES // 2, 1)


def source_of(conc):
    rise = -EIGEN_STRAIN * (3.0 * FIRST_RISE + 2.0 * SHEAR_RISE)
    low = -EIGEN_STRAIN * (3.0 * FIRST_LOW + 2.0 * SHEAR_LOW)
    return (low + rise * conc) * conc


def copy_lines(far, lines_ref, sems, inward):
    copies = []
    for high in range(HIGH):
        pair = (far.at[pl.ds(high * LOW, LOW)], lines_ref.at[:, high])
        source, target = pair if inward else pair[::-1]
        copies.append(pltpu.make_async_copy(source, target, sems.at[high]))
    return copies


def source_kernel(
    place_ref,
    conc_ref,
    far_ref,
    far_line_ref,
    cells_ref,
    out_ref,
    edge_ref,
    back_ref,
    ahead_ref,
    line_ref,
    line_back_ref,
    lines_ref,
    sems,
    far_sem,
    line_sem,
):
    copies = copy_lines(conc_ref, lines_ref, sems, True)
    copies.append(pltpu.make_async_copy(far_ref, ahead_ref, far_sem))
    line = pltpu.make_async_copy(far_line_ref, line_ref, line_sem)
    for copy in copies:
        copy.start()
    line.start()
    for copy in copies:
        copy.wait()
    conc = lines_ref[...].reshape(CELLS, N).T
    cells_ref[...] = conc
    source = source_of(conc)
    total = jnp.sum(source.reshape(N // 8, 8, CELLS), axis=0)
    row = lax.broadcasted_iota(jnp.int32, (8, CELLS), 0)
    edge = jnp.where(row % 2 == 0, total, -total)
    edge = jnp.sum(edge, axis=0, keepdims=True) * (1.0 / N)
    edge_ref[...] = jnp.where(row % 2 == 0, edge, -edge)
    total = sum(total[:, t * LANES : (t + 1) * LANES] for t in range(CELLS // LANES))
    total = jnp.sum(total, axis=0, keepdims=True)
    out_ref[peers_of(2 * LOW, SOURCE_ROWS), :] = jnp.broadcast_to(total, (DEVICES, LANES))
    z_ahead(source, 0, SOURCE_ROWS, 3, ahead_ref, out_ref)
    z_ahead(conc, 1, SOURCE_ROWS, 2, ahead_ref, out_ref)
    lane = lax.broadcasted_iota(jnp.int32, (N, N), 1)
    weight = jnp.where(lane % HALF == 0, 1.0, 2.0) * (1.0 / float(N) ** 3)
    for i in range(2):
        back_ref[i] = (ahead_ref[i].astype(F32).T * weight).astype(BF16)
    line.wait()
    for b in range(2):
        for i in range(2):
            line_back_ref[b, i] = line_ref[b, i].astype(F32).T.astype(BF16)


def plane_first_kernel(
    place_ref, in_ref, ahead_ref, back_ref, out_ref, mean_ref, plane_ref, line_ref
):
    mean = jnp.sum(in_ref[peers_of(2 * LOW, SOURCE_ROWS), :]) * (1.0 / float(N) ** 3)
    mean_ref[...] = jnp.full((8, CELLS), mean, F32)
    data = list(plane_spectrum(in_ref, 0, SOURCE_ROWS, ahead_ref, back_ref, plane_ref.at[5]))
    wave_x = row_waves(0, N)
    wave_z = depth_wave(place_ref, N)
    wave_y = []
    partial = wave_x * wave_x + wave_z * wave_z
    for b in range(2):
        wave = lane_waves(b, N)
        wave_y.append(twice(wave))
        square = partial + wave * wave
        nonzero = square > 0.0
        safe = jnp.where(nonzero, square, 1.0)
        data[b] = data[b] * twice(jnp.where(nonzero, TRACE / safe, 0.0))
    for power in range(3):
        if power:
            data = [data[b] * wave_y[b] for b in range(2)]
        line_ref[power, 0], line_ref[power, 1] = y_back(data[0], data[1], ahead_ref)
    plan = ((2, 0, 0), (0, 2, 0), (0, 1, 1), (1, 0, 1), (1, 1, 0))
    for f, (power_x, power_y, power_z) in enumerate(plan):
        real = line_ref[power_y, 0]
        imag = line_ref[power_y, 1]
        factor = None
        for wave in [wave_x] * power_x + [wave_z] * power_z:
            factor = wave if factor is None else factor * wave
        if factor is not None:
            real = real * twice(factor)
            imag = imag * twice(factor)
        x_back(real, imag, f, FIRST_ROWS, back_ref, plane_ref.at[f], out_ref)


def z_sweep_kernel(
    in_ref,
    cells_ref,
    edge_ref,
    mean_ref,
    back_ref,
    ahead_ref,
    past_ref,
    out_ref,
    strain_ref,
    spec_ref,
    tau_ref,
    sem,
):
    for f, component in enumerate(FIRST_FIELDS):
        spec = spec_ref.at[f]
        strain_ref[component] = z_back(in_ref, f, FIRST_ROWS, back_ref, spec)

    def block(b, slot):
        rows = pl.ds(pl.multiple_of(b * 8, 8), 8)
        conc = cells_ref[rows, :]
        source = source_of(conc) - mean_ref[...]
        trace = TRACE * (source - edge_ref[...])
        strain = [strain_ref[f, rows, :] for f in range(6) if f != 2]
        strain.insert(2, trace - strain[0] - strain[1])
        strain_ref[2, rows, :] = strain[2]
        normal = ((FIRST_LOW - FIRST_REF) + FIRST_RISE * conc) * trace + source
        excess = 2.0 * (SHEAR_LOW - SHEAR_REF) + 2.0 * SHEAR_RISE * conc
        for f in range(6):
            tau = excess * strain[f]
            tau_ref[f, rows, :] = tau + normal if f < 3 else tau

    each(N // 8, BLOCK_UNROLL, block)
    past = pltpu.make_async_copy(strain_ref, past_ref, sem)
    past.start()

    def ahead(f, slot):
        z_ahead(tau_ref[f], f, SWEEP_ROWS, 2, ahead_ref, out_ref)

    each(6, SWEEP_UNROLL, ahead)
    past.wait()


def plane_green_kernel(place_ref, in_ref, ahead_ref, back_ref, out_ref, plane_ref, spec_ref):
    def ahead(f, slot):
        spec_ref[f, 0], spec_ref[f, 1] = plane_spectrum(
            in_ref, f, SWEEP_ROWS, ahead_ref, back_ref, plane_ref.at[slot]
        )

    each(6, PLANE_UNROLL, ahead)

    waves_y = [lane_waves(branch, 8) for branch in range(2)]
    wave_z = depth_wave(place_ref, 8)

    def block(b, slot):
        start = pl.multiple_of(b * 8, 8)
        rows = pl.ds(start, 8)
        wave_x = row_waves(start, 8)
        partial = wave_x * wave_x + wave_z * wave_z
        for branch in range(2):
            wave_y = waves_y[branch]
            square = partial + wave_y * wave_y
            nonzero = square > 0.0
            inverse = 1.0 / jnp.where(nonzero, square, 1.0)
            scale = jnp.where(nonzero, inverse * (0.5 / SHEAR_REF), 0.0)
            inverse = inverse * BETA_REF
            for h in range(2):
                lanes = slice(h * LANES, (h + 1) * LANES)
                tau = [spec_ref[f, branch, rows, lanes] for f in range(6)]
                force_x = tau[0] * wave_x + tau[5] * wave_y + tau[4] * wave_z
                force_y = tau[5] * wave_x + tau[1] * wave_y + tau[3] * wave_z
                force_z = tau[4] * wave_x + tau[3] * wave_y + tau[2] * wave_z
                along = (wave_x * force_x + wave_y * force_y + wave_z * force_z) * inverse
                moved_x = scale * (along * wave_x - force_x)
                moved_y = scale * (along * wave_y - force_y)
                moved_z = scale * (along * wave_z - force_z)
                spec_ref[0, branch, rows, lanes] = (wave_x + wave_x) * moved_x
                spec_ref[1, branch, rows, lanes] = (wave_y + wave_y) * moved_y
                spec_ref[2, branch, rows, lanes] = (wave_z + wave_z) * moved_z
                spec_ref[3, branch, rows, lanes] = wave_y * moved_z + wave_z * moved_y
                spec_ref[4, branch, rows, lanes] = wave_x * moved_z + wave_z * moved_x
                spec_ref[5, branch, rows, lanes] = wave_x * moved_y + wave_y * moved_x

    each(N // 8, BLOCK_UNROLL, block)

    def back(f, slot):
        real, imag = y_back(spec_ref[f, 0], spec_ref[f, 1], ahead_ref)
        x_back(real, imag, f, SWEEP_ROWS, back_ref, plane_ref.at[slot], out_ref)

    each(6, PLANE_UNROLL, back)


def z_drive_kernel(
    in_ref,
    cells_ref,
    back_ref,
    ahead_ref,
    far_ref,
    out_ref,
    strain_ref,
    spec_ref,
    drive_ref,
    sems,
):
    def far(f):
        return pltpu.make_async_copy(strain_ref.at[f], far_ref.at[f], sems.at[f])

    def inverse(f, slot):
        strain_ref[f] = z_back(in_ref, f, SWEEP_ROWS, back_ref, spec_ref.at[slot])
        far(f).start()

    each(6, DRIVE_UNROLL, inverse)

    rise = -EIGEN_STRAIN * (3.0 * FIRST_RISE + 2.0 * SHEAR_RISE)
    low = -EIGEN_STRAIN * (3.0 * FIRST_LOW + 2.0 * SHEAR_LOW)

    def block(b, slot):
        rows = pl.ds(pl.multiple_of(b * 8, 8), 8)
        conc = cells_ref[rows, :]
        strain = [strain_ref[f, rows, :] for f in range(6)]
        dilation = EIGEN_STRAIN * conc
        part = [strain[f] - dilation for f in range(3)]
        trace = part[0] + part[1] + part[2]
        energy = (
            part[0] * part[0]
            + part[1] * part[1]
            + part[2] * part[2]
            + 2.0 * (strain[3] * strain[3] + strain[4] * strain[4] + strain[5] * strain[5])
        )
        chemical = 2.0 * WELL_HEIGHT * conc * (1.0 - conc) * (1.0 - 2.0 * conc)
        drive_ref[rows, :] = (
            chemical
            + 0.5 * FIRST_RISE * trace * trace
            + SHEAR_RISE * energy
            + (low + rise * conc) * trace
        )

    each(N // 8, BLOCK_UNROLL, block)
    z_ahead(drive_ref[...], 0, DRIVE_ROWS, 2, ahead_ref, out_ref)
    for f in range(6):
        far(f).wait()


def aside_kernel(
    now_ref,
    then_ref,
    source_ref,
    ahead_ref,
    back_ref,
    strain_ref,
    conc_ref,
    sums_ref,
    cells_ref,
    past_ref,
    data_ref,
    lines_ref,
    plane_ref,
    now_sems,
    then_sems,
    source_sem,
    out_sems,
):
    def now(f):
        return pltpu.make_async_copy(now_ref.at[f], cells_ref.at[f], now_sems.at[f])

    def then(f):
        return pltpu.make_async_copy(then_ref.at[f], past_ref.at[f], then_sems.at[f])

    for f in range(6):
        now(f).start()
        then(f).start()
    source = pltpu.make_async_copy(source_ref, data_ref, source_sem)
    source.start()

    def one(f, totals):
        def block(b, totals):
            rows = pl.ds(pl.multiple_of(b * 8, 8), 8)
            past = past_ref[f, rows, :]
            change = cells_ref[f, rows, :] - past
            return totals[0] + past * past, totals[1] + change * change

        now(f).wait()
        lines_ref[f] = cells_ref[f].T.reshape(LOW, HIGH, LY, N)
        for copy in copy_lines(strain_ref.at[f], lines_ref.at[f], out_sems.at[f], False):
            copy.start()
        then(f).wait()
        return lax.fori_loop(0, N // 8, block, totals)

    zero = jnp.zeros((8, CELLS), F32)
    totals = lax.fori_loop(0, 6, one, (zero, zero))
    lane = lax.broadcasted_iota(jnp.int32, (1, LANES), 1)
    sums = jnp.where(lane < LANES // 2, squares(totals[0]), squares(totals[1]))
    sums_ref[...] = jnp.broadcast_to(sums, (8, LANES))
    source.wait()
    conc_ref[0], conc_ref[1] = plane_spectrum(
        data_ref, 1, SOURCE_ROWS, ahead_ref, back_ref, plane_ref
    )
    for f in range(6):
        for copy in copy_lines(strain_ref.at[f], lines_ref.at[f], out_sems.at[f], False):
            copy.wait()


def plane_update_kernel(
    place_ref, in_ref, conc_ref, sums_ref, ahead_ref, back_ref, out_ref, plane_ref
):
    data = list(plane_spectrum(in_ref, 0, DRIVE_ROWS, ahead_ref, back_ref, plane_ref))
    wave_x = row_waves(0, N)
    wave_z = depth_wave(place_ref, N)
    partial = wave_x * wave_x + wave_z * wave_z
    for b in range(2):
        wave_y = lane_waves(b, N)
        square = partial + wave_y * wave_y
        inverse = 1.0 / (1.0 + TIME_STEP * GRADIENT_ENERGY * square * square)
        drive = TIME_STEP * square * inverse
        data[b] = conc_ref[b] * twice(inverse) - data[b] * twice(drive)
    real, imag = y_back(data[0], data[1], ahead_ref)
    x_back(real, imag, 0, LAST_ROWS, back_ref, plane_ref, out_ref)
    out_ref[peers_of(LOW, LAST_ROWS), :] = jnp.broadcast_to(sums_ref[:1, :], (DEVICES, LANES))


def z_last_kernel(in_ref, back_ref, out_ref, norm_ref, spec_ref, lines_ref, sems):
    lines = z_back(in_ref, 0, LAST_ROWS, back_ref, spec_ref).T
    lines_ref[...] = lines.reshape(LOW, HIGH, LY, N)
    copies = copy_lines(out_ref, lines_ref, sems, False)
    for copy in copies:
        copy.start()
    sums = in_ref[peers_of(LOW, LAST_ROWS), :]
    lane = lax.broadcasted_iota(jnp.int32, sums.shape, 1)
    row = lax.broadcasted_iota(jnp.int32, (8, LANES), 0)
    first = jnp.sum(jnp.where(lane < LANES // 2, sums, 0.0))
    second = jnp.sum(jnp.where(lane < LANES // 2, 0.0, sums))
    norms = jnp.sqrt(jnp.where(row == 0, first, second) * (1.0 / float(N) ** 3))
    norm_ref[0] = norms[0, 0]
    norm_ref[1] = norms[1, 0]
    for copy in copies:
        copy.wait()


SPACES = {"vmem": pltpu.VMEM, "smem": pltpu.SMEM, "hbm": pltpu.HBM}


def call(kernel, name, args, outs, scratch=(), sems=(), mib=24):
    operands = [
        pltpu.with_memory_space_constraint(value, pltpu.HBM) if space == "hbm" else value
        for space, value in args
    ]
    return pl.pallas_call(
        kernel,
        out_shape=[
            pltpu.HBM(shape, F32) if space == "hbm" else jax.ShapeDtypeStruct(shape, *kind or (F32,))
            for space, shape, *kind in outs
        ],
        in_specs=[pl.BlockSpec(memory_space=SPACES[space]) for space, _ in args],
        out_specs=[pl.BlockSpec(memory_space=SPACES[space]) for space, *_ in outs],
        scratch_shapes=[
            *[pltpu.VMEM(s, F32) if isinstance(s, tuple) else s for s in scratch],
            *[pltpu.SemaphoreType.DMA(shape) for shape in sems],
        ],
        name=name,
        interpret=INTERPRET,
        compiler_params=pltpu.CompilerParams(vmem_limit_bytes=mib * 1024 * 1024),
    )(*operands)


def exchange(array):
    rows = array.reshape(DEVICES, array.shape[0] // DEVICES * LANES)
    rows = lax.all_to_all(rows, AXES, split_axis=0, concat_axis=0, tiled=True)
    return rows.reshape(array.shape)


def wire(pitch):
    return (DEVICES * pitch, LANES)


BLOCK = (LX, LY, N)
CELL = (N, CELLS)
PLANE = (2, N, N)
LINES = (LOW, HIGH, LY, N)
SMALL = (8, CELLS)


def shards(concentration):
    tables = [jnp.asarray(table) for table in build_tables()]
    place = ("smem", lax.axis_index(AXES).astype(jnp.int32)[None])

    cells, data, edge, *tables = call(
        source_kernel,
        "source",
        [place, ("hbm", concentration), ("hbm", tables[1]), ("hbm", tables[0])],
        [
            ("vmem", CELL),
            ("vmem", wire(SOURCE_ROWS)),
            ("vmem", SMALL),
            ("vmem", (2, N, N), BF16),
            ("vmem", (3, N, N), BF16),
            ("vmem", (2, 2, N, N), BF16),
            ("vmem", (2, 2, N, N), BF16),
        ],
        [LINES],
        [(HIGH,), (), ()],
    )
    back, ahead, line_ahead, line_back = [("vmem", table) for table in tables]
    source = exchange(data)
    data, mean = call(
        plane_first_kernel,
        "plane_first",
        [place, ("vmem", source), line_ahead, line_back],
        [("vmem", wire(FIRST_ROWS)), ("vmem", SMALL)],
        [(6, *PLANE), (3, *PLANE)],
    )
    data = exchange(data)
    past, data = call(
        z_sweep_kernel,
        "z_sweep",
        [("vmem", data), ("vmem", cells), ("vmem", edge), ("vmem", mean), back, ahead],
        [("hbm", (6, *CELL)), ("vmem", wire(SWEEP_ROWS))],
        [(6, *CELL), (5, *CELL), (6, *CELL)],
        [()],
    )
    data = exchange(data)
    (data,) = call(
        plane_green_kernel,
        "plane_green",
        [place, ("vmem", data), line_ahead, line_back],
        [("vmem", wire(SWEEP_ROWS))],
        [(PLANE_UNROLL, *PLANE), (6, *PLANE)],
    )
    data = exchange(data)
    now, data = call(
        z_drive_kernel,
        "z_drive",
        [("vmem", data), ("vmem", cells), back, ahead],
        [("hbm", (6, *CELL)), ("vmem", wire(DRIVE_ROWS))],
        [(6, *CELL), (DRIVE_UNROLL, *CELL), CELL],
        [(6,)],
    )
    data = exchange(data)
    strain, conc_spec, sums = call(
        aside_kernel,
        "aside",
        [("hbm", now), ("hbm", past), ("hbm", source), line_ahead, line_back],
        [("hbm", (6, *BLOCK)), ("vmem", PLANE), ("vmem", (8, LANES))],
        [(6, *CELL), (6, *CELL), wire(SOURCE_ROWS), (6, *LINES), PLANE],
        [(6,), (6,), (), (6, HIGH)],
    )
    (data,) = call(
        plane_update_kernel,
        "plane_update",
        [place, ("vmem", data), ("vmem", conc_spec), ("vmem", sums), line_ahead, line_back],
        [("vmem", wire(LAST_ROWS))],
        [PLANE],
    )
    data = exchange(data)
    conc_next, norms = call(
        z_last_kernel,
        "z_last",
        [("vmem", data), back],
        [("hbm", BLOCK), ("smem", (2,))],
        [CELL, LINES],
        [(HIGH,)],
    )
    return conc_next, strain, norms


def solution(mesh):
    whole = Mesh(mesh.devices.reshape(4, 2, 4, 4), AXES)
    row, col = AXES[:2], AXES[2:]
    return jax.shard_map(
        shards,
        mesh=whole,
        in_specs=(P(row, col, None),),
        out_specs=(P(row, col, None), P(None, row, col, None), P()),
        check_vma=False,
    )
```

```python
import math
from functools import partial

import jax
import jax.numpy as jnp
import numpy as np
from jax import lax
from jax.experimental import pallas as pl
from jax.experimental.pallas import tpu as pltpu
from jax.sharding import Mesh
from jax.sharding import PartitionSpec as P

AXES = ("row_0", "row_1", "col_0", "col_1")

FIRST_LOW = 1.0
FIRST_RISE = 0.6
SHEAR_LOW = 0.7
SHEAR_RISE = 0.8
FIRST_REF = 1.3
SHEAR_REF = 1.1
BETA_REF = 2.4 / 3.5
EIGEN_STRAIN = 0.5
WELL_HEIGHT = 1.0
TIME_STEP = 0.5
GRADIENT_ENERGY = 0.5

N = 256
HALF = N // 2
ROWS = 8
COLS = 16
DEVICES = ROWS * COLS
LX = N // ROWS
LY = N // COLS
LOW = 8
HIGH = LX // LOW
CELLS = LX * LY
LANES = 128
UNIT = 2.0 * math.pi / N
F32 = jnp.float32
BF16 = jnp.bfloat16
INTERPRET = False
PLANE_UNROLL = 6
SWEEP_UNROLL = 3
DRIVE_UNROLL = 6
BLOCK_UNROLL = 2
SOURCE_ROWS = 2 * LOW
FIRST_ROWS = 5 * LOW
SWEEP_ROWS = 6 * LOW
DRIVE_ROWS = LOW
LAST_ROWS = LOW + 1
FIRST_FIELDS = (0, 1, 3, 4, 5)
TRACE = -(1.0 - BETA_REF) / SHEAR_REF


def pieces_of(table, count):
    rest = table.astype(np.float32)
    pieces = []
    for _ in range(count):
        piece = rest.astype(jnp.bfloat16)
        rest = rest - piece.astype(np.float32)
        pieces.append(piece)
    return np.stack(pieces)


def build_tables():
    index = np.arange(N)
    half = np.arange(HALF)
    angle = 2.0 * np.pi / N * (index[:, None] * index[None, :] % N)
    cosine = np.cos(angle)
    sine = np.sin(angle)
    lines = []
    for odd in range(2):
        angle = 2.0 * np.pi / N * ((2 * half[:, None] + odd) * half[None, :] % N)
        lines.append(
            np.block([[np.cos(angle), np.sin(angle)], [-np.sin(angle), np.cos(angle)]])
        )
    line_ahead = np.stack([pieces_of(line, 2) for line in lines])
    ahead = np.concatenate([cosine[:HALF], -sine[:HALF]], axis=0)
    return line_ahead, pieces_of(ahead, 3)


def split(value, count):
    pieces = []
    for i in range(count):
        piece = value.astype(BF16)
        pieces.append(piece)
        if i + 1 < count:
            value = value - piece.astype(F32)
    return pieces


def product(left, right):
    count = len(right)
    total = None
    for order in reversed(range(count)):
        for i in range(order + 1):
            term = jnp.dot(left[i], right[order - i], preferred_element_type=F32)
            total = term if total is None else total + term
    return total


def table(ref):
    return [ref[i] for i in range(ref.shape[0])]


def swap_lanes(parts, granule):
    parts = list(parts)
    axis = parts[0].ndim - 1
    lane = lax.broadcasted_iota(jnp.int32, parts[0].shape, axis)
    step = 1
    while step < len(parts):
        width = granule * step
        low = (lane & width) == 0
        for i in range(len(parts)):
            if i & step == 0:
                a, b = parts[i], parts[i + step]
                parts[i] = jnp.where(low, a, pltpu.roll(b, width, axis))
                parts[i + step] = jnp.where(low, pltpu.roll(a, LANES - width, axis), b)
        step *= 2
    return parts


def peers_of(row, pitch):
    return pl.ds(row, DEVICES, stride=pitch)


def z_ahead(value, f, pitch, pieces, ahead_ref, out_ref):
    spectrum = product(table(ahead_ref), split(value, pieces))
    for t in range(LOW // 2):
        lanes = slice(t * LANES, (t + 1) * LANES)
        parts = swap_lanes([spectrum[:HALF, lanes], spectrum[HALF:, lanes]], LANES // 2)
        for i in range(2):
            out_ref[peers_of(f * LOW + 2 * t + i, pitch), :] = parts[i]


def z_back(in_ref, f, pitch, back_ref, spec_ref):
    for t in range(LOW // 2):
        lanes = slice(t * LANES, (t + 1) * LANES)
        parts = [in_ref[peers_of(f * LOW + 2 * t + i, pitch), :] for i in range(2)]
        real, imag = swap_lanes(parts, LANES // 2)
        spec_ref[:HALF, lanes] = real
        spec_ref[HALF:, lanes] = imag
    return product(table(back_ref), split(spec_ref[...], 2))


def rows_of(peer, f, pitch):
    start = peer * pitch + f * LOW
    return pl.ds(start if isinstance(start, int) else pl.multiple_of(start, LOW), LOW)


def plane_row(part, i, high):
    return part * HALF + i % 4 * LX + high * LOW


def plane_ahead(in_ref, f, pitch, ahead_ref, plane_ref):
    for i in range(ROWS // 2):
        for h in range(2):
            near, far = [
                swap_lanes(
                    [in_ref[rows_of(k * COLS + h * 8 + j, f, pitch), :] for j in range(8)], LY
                )
                for k in (i, i + ROWS // 2)
            ]
            for g in range(8):
                row = plane_row(g // HIGH, i, g % HIGH)
                lanes = slice(h * LANES, (h + 1) * LANES)
                plane_ref[0, row : row + LOW, lanes] = near[g] + far[g]
                plane_ref[1, row : row + LOW, lanes] = near[g] - far[g]
    near, far = [], []
    for b in range(2):
        lines = product(table(ahead_ref.at[b]), split(plane_ref[b], 2))
        near.append(jnp.concatenate([lines[:HALF, :HALF], lines[HALF:, :HALF]], axis=1))
        far.append(jnp.concatenate([lines[:HALF, HALF:], lines[HALF:, HALF:]], axis=1))
    near = jnp.concatenate(near, axis=0)
    far = jnp.concatenate(far, axis=0)
    return near + far, near - far


def plane_spectrum(in_ref, f, pitch, ahead_ref, back_ref, plane_ref):
    even, odd = plane_ahead(in_ref, f, pitch, ahead_ref, plane_ref)
    return (
        product(split(even, 2), table(back_ref.at[0])),
        product(split(odd, 2), table(back_ref.at[1])),
    )


def y_back(even, odd, ahead_ref):
    even = product(split(even, 2), table(ahead_ref.at[0]))
    odd = product(split(odd, 2), table(ahead_ref.at[1]))
    near = even + odd
    far = even - odd
    return (
        jnp.concatenate([near[:, :HALF], far[:, :HALF]], axis=1),
        jnp.concatenate([near[:, HALF:], far[:, HALF:]], axis=1),
    )


def x_back(real, imag, f, pitch, back_ref, plane_ref, out_ref, mark=None):
    lines = []
    for b in range(2):
        rows = slice(b * HALF, (b + 1) * HALF)
        data = jnp.concatenate([real[rows], imag[rows]], axis=0)
        lines.append(product(table(back_ref.at[b]), split(data, 2)))
    plane_ref[0] = lines[0] + lines[1]
    plane_ref[1] = lines[0] - lines[1]
    if mark is not None:
        for half in range(2):
            plane_ref[half, HALF:] = jnp.where(mark[0], mark[1], plane_ref[half, HALF:])
    for i in range(ROWS):
        for h in range(2):
            parts = []
            for g in range(8):
                row = plane_row(g // HIGH, i, g % HIGH)
                parts.append(plane_ref[i // 4, row : row + LOW, h * LANES : (h + 1) * LANES])
            parts = swap_lanes(parts, LY)
            for j in range(8):
                out_ref[rows_of(i * COLS + h * 8 + j, f, pitch), :] = parts[j]


def each(count, unroll, body):
    def step(i, carry):
        for slot in range(unroll):
            body(i * unroll + slot, slot)
        return carry

    if count == unroll:
        step(0, 0)
    else:
        lax.fori_loop(0, count // unroll, step, 0)


def signed(index):
    return jnp.where(index < HALF, index, index - N).astype(F32) * UNIT


def row_waves(start, count):
    row = lax.broadcasted_iota(jnp.int32, (count, LANES), 0) + start
    return signed(2 * (row % HALF) + row // HALF)


def lane_waves(branch, count):
    return signed(2 * lax.broadcasted_iota(jnp.int32, (count, LANES), 1) + branch)


def depth_wave(place_ref, count):
    return jnp.full((count, LANES), place_ref[0], jnp.int32).astype(F32) * UNIT


def twice(half):
    return jnp.concatenate([half, half], axis=1)


def squares(total):
    total = sum(total[:, t * LANES : (t + 1) * LANES] for t in range(CELLS // LANES))
    total = jnp.sum(total, axis=0, keepdims=True)
    return total + pltpu.roll(total, LANES // 2, 1)


def source_of(conc):
    rise = -EIGEN_STRAIN * (3.0 * FIRST_RISE + 2.0 * SHEAR_RISE)
    low = -EIGEN_STRAIN * (3.0 * FIRST_LOW + 2.0 * SHEAR_LOW)
    return (low + rise * conc) * conc


def copy_lines(far, lines_ref, sems, inward):
    copies = []
    for high in range(HIGH):
        pair = (far.at[pl.ds(high * LOW, LOW)], lines_ref.at[:, high])
        source, target = pair if inward else pair[::-1]
        copies.append(pltpu.make_async_copy(source, target, sems.at[high]))
    return copies


def source_kernel(
    place_ref,
    conc_ref,
    far_ref,
    far_line_ref,
    cells_ref,
    out_ref,
    edge_ref,
    back_ref,
    ahead_ref,
    line_ref,
    line_back_ref,
    lines_ref,
    sems,
    far_sem,
    line_sem,
):
    copies = copy_lines(conc_ref, lines_ref, sems, True)
    copies.append(pltpu.make_async_copy(far_ref, ahead_ref, far_sem))
    line = pltpu.make_async_copy(far_line_ref, line_ref, line_sem)
    for copy in copies:
        copy.start()
    line.start()
    for copy in copies:
        copy.wait()
    conc = lines_ref[...].reshape(CELLS, N).T
    cells_ref[...] = conc
    source = source_of(conc)
    total = jnp.sum(source.reshape(N // 8, 8, CELLS), axis=0)
    row = lax.broadcasted_iota(jnp.int32, (8, CELLS), 0)
    edge = jnp.where(row % 2 == 0, total, -total)
    edge = jnp.sum(edge, axis=0, keepdims=True) * (1.0 / N)
    edge_ref[...] = jnp.where(row % 2 == 0, edge, -edge)
    z_ahead(source, 0, SOURCE_ROWS, 3, ahead_ref, out_ref)
    z_ahead(conc, 1, SOURCE_ROWS, 2, ahead_ref, out_ref)
    lane = lax.broadcasted_iota(jnp.int32, (N, N), 1)
    weight = jnp.where(lane % HALF == 0, 1.0, 2.0) * (1.0 / float(N) ** 3)
    for i in range(2):
        back_ref[i] = (ahead_ref[i].astype(F32).T * weight).astype(BF16)
    line.wait()
    for b in range(2):
        for i in range(2):
            line_back_ref[b, i] = line_ref[b, i].astype(F32).T.astype(BF16)


def plane_first_kernel(
    place_ref, in_ref, ahead_ref, back_ref, out_ref, plane_ref, line_ref
):
    data = list(plane_spectrum(in_ref, 0, SOURCE_ROWS, ahead_ref, back_ref, plane_ref.at[5]))
    mean = jnp.broadcast_to(data[0][:1, :1] * (1.0 / float(N) ** 3), (HALF, N))
    bottom = jnp.full((HALF, N), place_ref[0], jnp.int32) == 0
    wave_x = row_waves(0, N)
    wave_z = depth_wave(place_ref, N)
    wave_y = []
    partial = wave_x * wave_x + wave_z * wave_z
    for b in range(2):
        wave = lane_waves(b, N)
        wave_y.append(twice(wave))
        square = partial + wave * wave
        nonzero = square > 0.0
        safe = jnp.where(nonzero, square, 1.0)
        data[b] = data[b] * twice(jnp.where(nonzero, TRACE / safe, 0.0))
    for power in range(3):
        if power:
            data = [data[b] * wave_y[b] for b in range(2)]
        line_ref[power, 0], line_ref[power, 1] = y_back(data[0], data[1], ahead_ref)
    plan = ((2, 0, 0), (0, 2, 0), (0, 1, 1), (1, 0, 1), (1, 1, 0))
    for f, (power_x, power_y, power_z) in enumerate(plan):
        real = line_ref[power_y, 0]
        imag = line_ref[power_y, 1]
        factor = None
        for wave in [wave_x] * power_x + [wave_z] * power_z:
            factor = wave if factor is None else factor * wave
        if factor is not None:
            real = real * twice(factor)
            imag = imag * twice(factor)
        mark = (bottom, mean) if f == 0 else None
        x_back(real, imag, f, FIRST_ROWS, back_ref, plane_ref.at[f], out_ref, mark)


def z_sweep_kernel(
    in_ref,
    cells_ref,
    edge_ref,
    back_ref,
    ahead_ref,
    past_ref,
    out_ref,
    strain_ref,
    spec_ref,
    tau_ref,
    sem,
):
    for f, component in enumerate(FIRST_FIELDS):
        spec = spec_ref.at[f]
        strain_ref[component] = z_back(in_ref, f, FIRST_ROWS, back_ref, spec)

    mean = in_ref[:LOW, :]
    lane = lax.broadcasted_iota(jnp.int32, mean.shape, 1)
    mean = jnp.where(lane < LANES // 2, pltpu.roll(mean, LANES // 2, 1), mean)
    mean = jnp.concatenate([mean] * (CELLS // LANES), axis=1)

    def block(b, slot):
        rows = pl.ds(pl.multiple_of(b * 8, 8), 8)
        conc = cells_ref[rows, :]
        source = source_of(conc) - mean
        trace = TRACE * (source - edge_ref[...])
        strain = [strain_ref[f, rows, :] for f in range(6) if f != 2]
        strain.insert(2, trace - strain[0] - strain[1])
        strain_ref[2, rows, :] = strain[2]
        normal = ((FIRST_LOW - FIRST_REF) + FIRST_RISE * conc) * trace + source
        excess = 2.0 * (SHEAR_LOW - SHEAR_REF) + 2.0 * SHEAR_RISE * conc
        for f in range(6):
            tau = excess * strain[f]
            tau_ref[f, rows, :] = tau + normal if f < 3 else tau

    each(N // 8, BLOCK_UNROLL, block)
    past = pltpu.make_async_copy(strain_ref, past_ref, sem)
    past.start()

    def ahead(f, slot):
        z_ahead(tau_ref[f], f, SWEEP_ROWS, 2, ahead_ref, out_ref)

    each(6, SWEEP_UNROLL, ahead)
    past.wait()


def plane_green_kernel(place_ref, in_ref, ahead_ref, back_ref, out_ref, plane_ref, spec_ref):
    def ahead(f, slot):
        spec_ref[f, 0], spec_ref[f, 1] = plane_spectrum(
            in_ref, f, SWEEP_ROWS, ahead_ref, back_ref, plane_ref.at[slot]
        )

    each(6, PLANE_UNROLL, ahead)

    waves_y = [lane_waves(branch, 8) for branch in range(2)]
    wave_z = depth_wave(place_ref, 8)

    def block(b, slot):
        start = pl.multiple_of(b * 8, 8)
        rows = pl.ds(start, 8)
        wave_x = row_waves(start, 8)
        partial = wave_x * wave_x + wave_z * wave_z
        for branch in range(2):
            wave_y = waves_y[branch]
            square = partial + wave_y * wave_y
            nonzero = square > 0.0
            inverse = 1.0 / jnp.where(nonzero, square, 1.0)
            scale = jnp.where(nonzero, inverse * (0.5 / SHEAR_REF), 0.0)
            inverse = inverse * BETA_REF
            for h in range(2):
                lanes = slice(h * LANES, (h + 1) * LANES)
                tau = [spec_ref[f, branch, rows, lanes] for f in range(6)]
                force_x = tau[0] * wave_x + tau[5] * wave_y + tau[4] * wave_z
                force_y = tau[5] * wave_x + tau[1] * wave_y + tau[3] * wave_z
                force_z = tau[4] * wave_x + tau[3] * wave_y + tau[2] * wave_z
                along = (wave_x * force_x + wave_y * force_y + wave_z * force_z) * inverse
                moved_x = scale * (along * wave_x - force_x)
                moved_y = scale * (along * wave_y - force_y)
                moved_z = scale * (along * wave_z - force_z)
                spec_ref[0, branch, rows, lanes] = (wave_x + wave_x) * moved_x
                spec_ref[1, branch, rows, lanes] = (wave_y + wave_y) * moved_y
                spec_ref[2, branch, rows, lanes] = (wave_z + wave_z) * moved_z
                spec_ref[3, branch, rows, lanes] = wave_y * moved_z + wave_z * moved_y
                spec_ref[4, branch, rows, lanes] = wave_x * moved_z + wave_z * moved_x
                spec_ref[5, branch, rows, lanes] = wave_x * moved_y + wave_y * moved_x

    each(N // 8, BLOCK_UNROLL, block)

    def back(f, slot):
        real, imag = y_back(spec_ref[f, 0], spec_ref[f, 1], ahead_ref)
        x_back(real, imag, f, SWEEP_ROWS, back_ref, plane_ref.at[slot], out_ref)

    each(6, PLANE_UNROLL, back)


def z_drive_kernel(
    in_ref,
    cells_ref,
    back_ref,
    ahead_ref,
    far_ref,
    far_out_ref,
    strain_ref,
    spec_ref,
    drive_ref,
    out_ref,
    sems,
    out_sem,
):
    def far(f):
        return pltpu.make_async_copy(strain_ref.at[f], far_ref.at[f], sems.at[f])

    def inverse(f, slot):
        strain_ref[f] = z_back(in_ref, f, SWEEP_ROWS, back_ref, spec_ref.at[slot])
        far(f).start()

    each(6, DRIVE_UNROLL, inverse)

    rise = -EIGEN_STRAIN * (3.0 * FIRST_RISE + 2.0 * SHEAR_RISE)
    low = -EIGEN_STRAIN * (3.0 * FIRST_LOW + 2.0 * SHEAR_LOW)

    def block(b, slot):
        rows = pl.ds(pl.multiple_of(b * 8, 8), 8)
        conc = cells_ref[rows, :]
        strain = [strain_ref[f, rows, :] for f in range(6)]
        dilation = EIGEN_STRAIN * conc
        part = [strain[f] - dilation for f in range(3)]
        trace = part[0] + part[1] + part[2]
        energy = (
            part[0] * part[0]
            + part[1] * part[1]
            + part[2] * part[2]
            + 2.0 * (strain[3] * strain[3] + strain[4] * strain[4] + strain[5] * strain[5])
        )
        chemical = 2.0 * WELL_HEIGHT * conc * (1.0 - conc) * (1.0 - 2.0 * conc)
        drive_ref[rows, :] = (
            chemical
            + 0.5 * FIRST_RISE * trace * trace
            + SHEAR_RISE * energy
            + (low + rise * conc) * trace
        )

    each(N // 8, BLOCK_UNROLL, block)
    z_ahead(drive_ref[...], 0, DRIVE_ROWS, 2, ahead_ref, out_ref)
    out = pltpu.make_async_copy(out_ref, far_out_ref, out_sem)
    out.start()
    for f in range(6):
        far(f).wait()
    out.wait()


def aside_kernel(
    now_ref,
    then_ref,
    source_ref,
    ahead_ref,
    back_ref,
    strain_ref,
    conc_ref,
    sums_ref,
    cells_ref,
    past_ref,
    data_ref,
    lines_ref,
    plane_ref,
    now_sems,
    then_sems,
    source_sem,
    out_sems,
):
    def now(f):
        return pltpu.make_async_copy(now_ref.at[f], cells_ref.at[f], now_sems.at[f])

    def then(f):
        return pltpu.make_async_copy(then_ref.at[f], past_ref.at[f], then_sems.at[f])

    for f in range(6):
        now(f).start()
        then(f).start()
    source = pltpu.make_async_copy(source_ref, data_ref, source_sem)
    source.start()

    def one(f, totals):
        def block(b, totals):
            rows = pl.ds(pl.multiple_of(b * 8, 8), 8)
            past = past_ref[f, rows, :]
            change = cells_ref[f, rows, :] - past
            return totals[0] + past * past, totals[1] + change * change

        now(f).wait()
        lines_ref[f] = cells_ref[f].T.reshape(LOW, HIGH, LY, N)
        for copy in copy_lines(strain_ref.at[f], lines_ref.at[f], out_sems.at[f], False):
            copy.start()
        then(f).wait()
        return lax.fori_loop(0, N // 8, block, totals)

    zero = jnp.zeros((8, CELLS), F32)
    totals = lax.fori_loop(0, 6, one, (zero, zero))
    lane = lax.broadcasted_iota(jnp.int32, (1, LANES), 1)
    sums = jnp.where(lane < LANES // 2, squares(totals[0]), squares(totals[1]))
    sums_ref[...] = jnp.broadcast_to(sums, (8, LANES))
    source.wait()
    conc_ref[0], conc_ref[1] = plane_spectrum(
        data_ref, 1, SOURCE_ROWS, ahead_ref, back_ref, plane_ref
    )
    for f in range(6):
        for copy in copy_lines(strain_ref.at[f], lines_ref.at[f], out_sems.at[f], False):
            copy.wait()


def plane_update_kernel(
    place_ref, in_ref, conc_ref, sums_ref, ahead_ref, back_ref, out_ref, plane_ref
):
    data = list(plane_spectrum(in_ref, 0, DRIVE_ROWS, ahead_ref, back_ref, plane_ref))
    wave_x = row_waves(0, N)
    wave_z = depth_wave(place_ref, N)
    partial = wave_x * wave_x + wave_z * wave_z
    for b in range(2):
        wave_y = lane_waves(b, N)
        square = partial + wave_y * wave_y
        inverse = 1.0 / (1.0 + TIME_STEP * GRADIENT_ENERGY * square * square)
        drive = TIME_STEP * square * inverse
        data[b] = conc_ref[b] * twice(inverse) - data[b] * twice(drive)
    real, imag = y_back(data[0], data[1], ahead_ref)
    x_back(real, imag, 0, LAST_ROWS, back_ref, plane_ref, out_ref)
    out_ref[peers_of(LOW, LAST_ROWS), :] = jnp.broadcast_to(sums_ref[:1, :], (DEVICES, LANES))


def z_last_kernel(in_ref, back_ref, out_ref, norm_ref, spec_ref, lines_ref, sems):
    lines = z_back(in_ref, 0, LAST_ROWS, back_ref, spec_ref).T
    lines_ref[...] = lines.reshape(LOW, HIGH, LY, N)
    copies = copy_lines(out_ref, lines_ref, sems, False)
    for copy in copies:
        copy.start()
    sums = in_ref[peers_of(LOW, LAST_ROWS), :]
    lane = lax.broadcasted_iota(jnp.int32, sums.shape, 1)
    row = lax.broadcasted_iota(jnp.int32, (8, LANES), 0)
    first = jnp.sum(jnp.where(lane < LANES // 2, sums, 0.0))
    second = jnp.sum(jnp.where(lane < LANES // 2, 0.0, sums))
    norms = jnp.sqrt(jnp.where(row == 0, first, second) * (1.0 / float(N) ** 3))
    norm_ref[0] = norms[0, 0]
    norm_ref[1] = norms[1, 0]
    for copy in copies:
        copy.wait()


SPACES = {"vmem": pltpu.VMEM, "smem": pltpu.SMEM, "hbm": pltpu.HBM}


def call(kernel, name, args, outs, scratch=(), sems=(), mib=24):
    operands = [
        pltpu.with_memory_space_constraint(value, pltpu.HBM) if space == "hbm" else value
        for space, value in args
    ]
    return pl.pallas_call(
        kernel,
        out_shape=[
            pltpu.HBM(shape, F32) if space == "hbm" else jax.ShapeDtypeStruct(shape, *kind or (F32,))
            for space, shape, *kind in outs
        ],
        in_specs=[pl.BlockSpec(memory_space=SPACES[space]) for space, _ in args],
        out_specs=[pl.BlockSpec(memory_space=SPACES[space]) for space, *_ in outs],
        scratch_shapes=[
            *[pltpu.VMEM(s, F32) if isinstance(s, tuple) else s for s in scratch],
            *[pltpu.SemaphoreType.DMA(shape) for shape in sems],
        ],
        name=name,
        interpret=INTERPRET,
        compiler_params=pltpu.CompilerParams(vmem_limit_bytes=mib * 1024 * 1024),
    )(*operands)


def exchange(array):
    rows = array.reshape(DEVICES, array.shape[0] // DEVICES * LANES)
    rows = lax.all_to_all(rows, AXES, split_axis=0, concat_axis=0, tiled=True)
    return rows.reshape(array.shape)


def wire(pitch):
    return (DEVICES * pitch, LANES)


BLOCK = (LX, LY, N)
CELL = (N, CELLS)
PLANE = (2, N, N)
LINES = (LOW, HIGH, LY, N)
SMALL = (8, CELLS)


def shards(concentration):
    tables = [jnp.asarray(table) for table in build_tables()]
    place = ("smem", lax.axis_index(AXES).astype(jnp.int32)[None])

    cells, data, edge, *tables = call(
        source_kernel,
        "source",
        [place, ("hbm", concentration), ("hbm", tables[1]), ("hbm", tables[0])],
        [
            ("vmem", CELL),
            ("vmem", wire(SOURCE_ROWS)),
            ("vmem", SMALL),
            ("vmem", (2, N, N), BF16),
            ("vmem", (3, N, N), BF16),
            ("vmem", (2, 2, N, N), BF16),
            ("vmem", (2, 2, N, N), BF16),
        ],
        [LINES],
        [(HIGH,), (), ()],
    )
    back, ahead, line_ahead, line_back = [("vmem", table) for table in tables]
    source = exchange(data)
    (data,) = call(
        plane_first_kernel,
        "plane_first",
        [place, ("vmem", source), line_ahead, line_back],
        [("vmem", wire(FIRST_ROWS))],
        [(6, *PLANE), (3, *PLANE)],
    )
    data = exchange(data)
    past, data = call(
        z_sweep_kernel,
        "z_sweep",
        [("vmem", data), ("vmem", cells), ("vmem", edge), back, ahead],
        [("hbm", (6, *CELL)), ("vmem", wire(SWEEP_ROWS))],
        [(6, *CELL), (5, *CELL), (6, *CELL)],
        [()],
    )
    data = exchange(data)
    (data,) = call(
        plane_green_kernel,
        "plane_green",
        [place, ("vmem", data), line_ahead, line_back],
        [("vmem", wire(SWEEP_ROWS))],
        [(PLANE_UNROLL, *PLANE), (6, *PLANE)],
    )
    data = exchange(data)
    now, data = call(
        z_drive_kernel,
        "z_drive",
        [("vmem", data), ("vmem", cells), back, ahead],
        [("hbm", (6, *CELL)), ("hbm", wire(DRIVE_ROWS))],
        [(6, *CELL), (DRIVE_UNROLL, *CELL), CELL, wire(DRIVE_ROWS)],
        [(6,), ()],
    )
    data = exchange(data)
    strain, conc_spec, sums = call(
        aside_kernel,
        "aside",
        [("hbm", now), ("hbm", past), ("hbm", source), line_ahead, line_back],
        [("hbm", (6, *BLOCK)), ("vmem", PLANE), ("vmem", (8, LANES))],
        [(6, *CELL), (6, *CELL), wire(SOURCE_ROWS), (6, *LINES), PLANE],
        [(6,), (6,), (), (6, HIGH)],
    )
    (data,) = call(
        plane_update_kernel,
        "plane_update",
        [place, ("vmem", data), ("vmem", conc_spec), ("vmem", sums), line_ahead, line_back],
        [("vmem", wire(LAST_ROWS))],
        [PLANE],
    )
    data = exchange(data)
    conc_next, norms = call(
        z_last_kernel,
        "z_last",
        [("vmem", data), back],
        [("hbm", BLOCK), ("smem", (2,))],
        [CELL, LINES],
        [(HIGH,)],
    )
    return conc_next, strain, norms


def solution(mesh):
    whole = Mesh(mesh.devices.reshape(4, 2, 4, 4), AXES)
    row, col = AXES[:2], AXES[2:]
    return jax.shard_map(
        shards,
        mesh=whole,
        in_specs=(P(row, col, None),),
        out_specs=(P(row, col, None), P(None, row, col, None), P()),
        check_vma=False,
    )
```

```python
import math
from functools import partial

import jax
import jax.numpy as jnp
import numpy as np
from jax import lax
from jax.experimental import pallas as pl
from jax.experimental.pallas import tpu as pltpu
from jax.sharding import Mesh
from jax.sharding import PartitionSpec as P

AXES = ("row_0", "row_1", "col_0", "col_1")

FIRST_LOW = 1.0
FIRST_RISE = 0.6
SHEAR_LOW = 0.7
SHEAR_RISE = 0.8
FIRST_REF = 1.3
SHEAR_REF = 1.1
BETA_REF = 2.4 / 3.5
EIGEN_STRAIN = 0.5
WELL_HEIGHT = 1.0
TIME_STEP = 0.5
GRADIENT_ENERGY = 0.5

N = 256
HALF = N // 2
ROWS = 8
COLS = 16
DEVICES = ROWS * COLS
LX = N // ROWS
LY = N // COLS
LOW = 8
HIGH = LX // LOW
CELLS = LX * LY
LANES = 128
UNIT = 2.0 * math.pi / N
F32 = jnp.float32
BF16 = jnp.bfloat16
INTERPRET = False
PLANE_UNROLL = 6
SWEEP_UNROLL = 3
DRIVE_UNROLL = 6
BLOCK_UNROLL = 2
SOURCE_ROWS = 2 * LOW
FIRST_ROWS = 5 * LOW
SWEEP_ROWS = 6 * LOW
DRIVE_ROWS = LOW
LAST_ROWS = LOW + 1
FIRST_FIELDS = (0, 1, 3, 4, 5)
TRACE = -(1.0 - BETA_REF) / SHEAR_REF


def pieces_of(table, count):
    rest = table.astype(np.float32)
    pieces = []
    for _ in range(count):
        piece = rest.astype(jnp.bfloat16)
        rest = rest - piece.astype(np.float32)
        pieces.append(piece)
    return np.stack(pieces)


def build_tables():
    index = np.arange(N)
    half = np.arange(HALF)
    angle = 2.0 * np.pi / N * (index[:, None] * index[None, :] % N)
    cosine = np.cos(angle)
    sine = np.sin(angle)
    lines = []
    for odd in range(2):
        angle = 2.0 * np.pi / N * ((2 * half[:, None] + odd) * half[None, :] % N)
        lines.append(
            np.block([[np.cos(angle), np.sin(angle)], [-np.sin(angle), np.cos(angle)]])
        )
    line_ahead = np.stack([pieces_of(line, 2) for line in lines])
    ahead = np.concatenate([cosine[:HALF], -sine[:HALF]], axis=0)
    return line_ahead, pieces_of(ahead, 3)


def split(value, count):
    pieces = []
    for i in range(count):
        piece = value.astype(BF16)
        pieces.append(piece)
        if i + 1 < count:
            value = value - piece.astype(F32)
    return pieces


def product(left, right):
    count = len(right)
    total = None
    for order in reversed(range(count)):
        for i in range(order + 1):
            term = jnp.dot(left[i], right[order - i], preferred_element_type=F32)
            total = term if total is None else total + term
    return total


def table(ref):
    return [ref[i] for i in range(ref.shape[0])]


def swap_lanes(parts, granule):
    parts = list(parts)
    axis = parts[0].ndim - 1
    lane = lax.broadcasted_iota(jnp.int32, parts[0].shape, axis)
    step = 1
    while step < len(parts):
        width = granule * step
        low = (lane & width) == 0
        for i in range(len(parts)):
            if i & step == 0:
                a, b = parts[i], parts[i + step]
                if len(parts) > 2 and 2 * width == LANES:
                    moved = pltpu.roll(jnp.where(low, b, a), width, axis)
                    parts[i] = jnp.where(low, a, moved)
                    parts[i + step] = jnp.where(low, moved, b)
                    continue
                parts[i] = jnp.where(low, a, pltpu.roll(b, width, axis))
                parts[i + step] = jnp.where(low, pltpu.roll(a, LANES - width, axis), b)
        step *= 2
    return parts


def peers_of(row, pitch):
    return pl.ds(row, DEVICES, stride=pitch)


def z_ahead(value, f, pitch, pieces, ahead_ref, out_ref):
    spectrum = product(table(ahead_ref), split(value, pieces))
    for t in range(LOW // 2):
        lanes = slice(t * LANES, (t + 1) * LANES)
        parts = swap_lanes([spectrum[:HALF, lanes], spectrum[HALF:, lanes]], LANES // 2)
        for i in range(2):
            out_ref[peers_of(f * LOW + 2 * t + i, pitch), :] = parts[i]


def z_back(in_ref, f, pitch, back_ref, spec_ref):
    for t in range(LOW // 2):
        lanes = slice(t * LANES, (t + 1) * LANES)
        parts = [in_ref[peers_of(f * LOW + 2 * t + i, pitch), :] for i in range(2)]
        real, imag = swap_lanes(parts, LANES // 2)
        spec_ref[:HALF, lanes] = real
        spec_ref[HALF:, lanes] = imag
    return product(table(back_ref), split(spec_ref[...], 2))


def rows_of(peer, f, pitch):
    start = peer * pitch + f * LOW
    return pl.ds(start if isinstance(start, int) else pl.multiple_of(start, LOW), LOW)


def plane_row(part, i, high):
    return part * HALF + i % 4 * LX + high * LOW


def plane_ahead(in_ref, f, pitch, ahead_ref, plane_ref):
    for i in range(ROWS // 2):
        for h in range(2):
            near, far = [
                swap_lanes(
                    [in_ref[rows_of(k * COLS + h * 8 + j, f, pitch), :] for j in range(8)], LY
                )
                for k in (i, i + ROWS // 2)
            ]
            for g in range(8):
                row = plane_row(g // HIGH, i, g % HIGH)
                lanes = slice(h * LANES, (h + 1) * LANES)
                plane_ref[0, row : row + LOW, lanes] = near[g] + far[g]
                plane_ref[1, row : row + LOW, lanes] = near[g] - far[g]
    near, far = [], []
    for b in range(2):
        lines = product(table(ahead_ref.at[b]), split(plane_ref[b], 2))
        near.append(jnp.concatenate([lines[:HALF, :HALF], lines[HALF:, :HALF]], axis=1))
        far.append(jnp.concatenate([lines[:HALF, HALF:], lines[HALF:, HALF:]], axis=1))
    near = jnp.concatenate(near, axis=0)
    far = jnp.concatenate(far, axis=0)
    return near + far, near - far


def plane_spectrum(in_ref, f, pitch, ahead_ref, back_ref, plane_ref):
    even, odd = plane_ahead(in_ref, f, pitch, ahead_ref, plane_ref)
    return (
        product(split(even, 2), table(back_ref.at[0])),
        product(split(odd, 2), table(back_ref.at[1])),
    )


def y_back(even, odd, ahead_ref):
    even = product(split(even, 2), table(ahead_ref.at[0]))
    odd = product(split(odd, 2), table(ahead_ref.at[1]))
    near = even + odd
    far = even - odd
    return (
        jnp.concatenate([near[:, :HALF], far[:, :HALF]], axis=1),
        jnp.concatenate([near[:, HALF:], far[:, HALF:]], axis=1),
    )


def x_back(real, imag, f, pitch, back_ref, plane_ref, out_ref, mark=None):
    lines = []
    for b in range(2):
        rows = slice(b * HALF, (b + 1) * HALF)
        data = jnp.concatenate([real[rows], imag[rows]], axis=0)
        lines.append(product(table(back_ref.at[b]), split(data, 2)))
    plane_ref[0] = lines[0] + lines[1]
    plane_ref[1] = lines[0] - lines[1]
    if mark is not None:
        for half in range(2):
            plane_ref[half, HALF:] = jnp.where(mark[0], mark[1], plane_ref[half, HALF:])
    for i in range(ROWS):
        for h in range(2):
            parts = []
            for g in range(8):
                row = plane_row(g // HIGH, i, g % HIGH)
                parts.append(plane_ref[i // 4, row : row + LOW, h * LANES : (h + 1) * LANES])
            parts = swap_lanes(parts, LY)
            for j in range(8):
                out_ref[rows_of(i * COLS + h * 8 + j, f, pitch), :] = parts[j]


def each(count, unroll, body):
    def step(i, carry):
        for slot in range(unroll):
            body(i * unroll + slot, slot)
        return carry

    if count == unroll:
        step(0, 0)
    else:
        lax.fori_loop(0, count // unroll, step, 0)


def signed(index):
    return jnp.where(index < HALF, index, index - N).astype(F32) * UNIT


def row_waves(start, count):
    row = lax.broadcasted_iota(jnp.int32, (count, LANES), 0) + start
    return signed(2 * (row % HALF) + row // HALF)


def lane_waves(branch, count):
    return signed(2 * lax.broadcasted_iota(jnp.int32, (count, LANES), 1) + branch)


def depth_wave(place_ref, count):
    return jnp.full((count, LANES), place_ref[0], jnp.int32).astype(F32) * UNIT


def twice(half):
    return jnp.concatenate([half, half], axis=1)


def squares(total):
    total = sum(total[:, t * LANES : (t + 1) * LANES] for t in range(CELLS // LANES))
    total = jnp.sum(total, axis=0, keepdims=True)
    return total + pltpu.roll(total, LANES // 2, 1)


def source_of(conc):
    rise = -EIGEN_STRAIN * (3.0 * FIRST_RISE + 2.0 * SHEAR_RISE)
    low = -EIGEN_STRAIN * (3.0 * FIRST_LOW + 2.0 * SHEAR_LOW)
    return (low + rise * conc) * conc


def copy_lines(far, lines_ref, sems, inward):
    copies = []
    for high in range(HIGH):
        pair = (far.at[pl.ds(high * LOW, LOW)], lines_ref.at[:, high])
        source, target = pair if inward else pair[::-1]
        copies.append(pltpu.make_async_copy(source, target, sems.at[high]))
    return copies


def source_kernel(
    place_ref,
    conc_ref,
    far_ref,
    far_line_ref,
    cells_ref,
    out_ref,
    edge_ref,
    back_ref,
    ahead_ref,
    line_ref,
    line_back_ref,
    lines_ref,
    sems,
    far_sem,
    line_sem,
):
    copies = copy_lines(conc_ref, lines_ref, sems, True)
    copies.append(pltpu.make_async_copy(far_ref, ahead_ref, far_sem))
    line = pltpu.make_async_copy(far_line_ref, line_ref, line_sem)
    for copy in copies:
        copy.start()
    line.start()
    for copy in copies:
        copy.wait()
    conc = lines_ref[...].reshape(CELLS, N).T
    cells_ref[...] = conc
    source = source_of(conc)
    total = jnp.sum(source.reshape(N // 8, 8, CELLS), axis=0)
    row = lax.broadcasted_iota(jnp.int32, (8, CELLS), 0)
    edge = jnp.where(row % 2 == 0, total, -total)
    edge = jnp.sum(edge, axis=0, keepdims=True) * (1.0 / N)
    edge_ref[...] = jnp.where(row % 2 == 0, edge, -edge)
    z_ahead(source, 0, SOURCE_ROWS, 3, ahead_ref, out_ref)
    z_ahead(conc, 1, SOURCE_ROWS, 2, ahead_ref, out_ref)
    lane = lax.broadcasted_iota(jnp.int32, (N, N), 1)
    weight = jnp.where(lane % HALF == 0, 1.0, 2.0) * (1.0 / float(N) ** 3)
    for i in range(2):
        back_ref[i] = (ahead_ref[i].astype(F32).T * weight).astype(BF16)
    line.wait()
    for b in range(2):
        for i in range(2):
            line_back_ref[b, i] = line_ref[b, i].astype(F32).T.astype(BF16)


def plane_first_kernel(
    place_ref, in_ref, ahead_ref, back_ref, out_ref, plane_ref, line_ref
):
    data = list(plane_spectrum(in_ref, 0, SOURCE_ROWS, ahead_ref, back_ref, plane_ref.at[5]))
    mean = jnp.broadcast_to(data[0][:1, :1] * (1.0 / float(N) ** 3), (HALF, N))
    bottom = jnp.full((HALF, N), place_ref[0], jnp.int32) == 0
    wave_x = row_waves(0, N)
    wave_z = depth_wave(place_ref, N)
    wave_y = []
    partial = wave_x * wave_x + wave_z * wave_z
    for b in range(2):
        wave = lane_waves(b, N)
        wave_y.append(twice(wave))
        square = partial + wave * wave
        nonzero = square > 0.0
        safe = jnp.where(nonzero, square, 1.0)
        data[b] = data[b] * twice(jnp.where(nonzero, TRACE / safe, 0.0))
    for power in range(3):
        if power:
            data = [data[b] * wave_y[b] for b in range(2)]
        line_ref[power, 0], line_ref[power, 1] = y_back(data[0], data[1], ahead_ref)
    plan = ((2, 0, 0), (0, 2, 0), (0, 1, 1), (1, 0, 1), (1, 1, 0))
    for f, (power_x, power_y, power_z) in enumerate(plan):
        real = line_ref[power_y, 0]
        imag = line_ref[power_y, 1]
        factor = None
        for wave in [wave_x] * power_x + [wave_z] * power_z:
            factor = wave if factor is None else factor * wave
        if factor is not None:
            real = real * twice(factor)
            imag = imag * twice(factor)
        mark = (bottom, mean) if f == 0 else None
        x_back(real, imag, f, FIRST_ROWS, back_ref, plane_ref.at[f], out_ref, mark)


def z_sweep_kernel(
    in_ref,
    cells_ref,
    edge_ref,
    back_ref,
    ahead_ref,
    past_ref,
    out_ref,
    strain_ref,
    spec_ref,
    tau_ref,
    sem,
):
    for f, component in enumerate(FIRST_FIELDS):
        spec = spec_ref.at[f]
        strain_ref[component] = z_back(in_ref, f, FIRST_ROWS, back_ref, spec)

    mean = in_ref[:LOW, :]
    lane = lax.broadcasted_iota(jnp.int32, mean.shape, 1)
    mean = jnp.where(lane < LANES // 2, pltpu.roll(mean, LANES // 2, 1), mean)
    mean = jnp.concatenate([mean] * (CELLS // LANES), axis=1)

    def block(b, slot):
        rows = pl.ds(pl.multiple_of(b * 8, 8), 8)
        conc = cells_ref[rows, :]
        source = source_of(conc) - mean
        trace = TRACE * (source - edge_ref[...])
        strain = [strain_ref[f, rows, :] for f in range(6) if f != 2]
        strain.insert(2, trace - strain[0] - strain[1])
        strain_ref[2, rows, :] = strain[2]
        normal = ((FIRST_LOW - FIRST_REF) + FIRST_RISE * conc) * trace + source
        excess = 2.0 * (SHEAR_LOW - SHEAR_REF) + 2.0 * SHEAR_RISE * conc
        for f in range(6):
            tau = excess * strain[f]
            tau_ref[f, rows, :] = tau + normal if f < 3 else tau

    each(N // 8, BLOCK_UNROLL, block)
    past = pltpu.make_async_copy(strain_ref, past_ref, sem)
    past.start()

    def ahead(f, slot):
        z_ahead(tau_ref[f], f, SWEEP_ROWS, 2, ahead_ref, out_ref)

    each(6, SWEEP_UNROLL, ahead)
    past.wait()


def plane_green_kernel(place_ref, in_ref, ahead_ref, back_ref, out_ref, plane_ref, spec_ref):
    def ahead(f, slot):
        spec_ref[f, 0], spec_ref[f, 1] = plane_spectrum(
            in_ref, f, SWEEP_ROWS, ahead_ref, back_ref, plane_ref.at[slot]
        )

    each(6, PLANE_UNROLL, ahead)

    waves_y = [lane_waves(branch, 8) for branch in range(2)]
    wave_z = depth_wave(place_ref, 8)

    def block(b, slot):
        start = pl.multiple_of(b * 8, 8)
        rows = pl.ds(start, 8)
        wave_x = row_waves(start, 8)
        partial = wave_x * wave_x + wave_z * wave_z
        for branch in range(2):
            wave_y = waves_y[branch]
            square = partial + wave_y * wave_y
            nonzero = square > 0.0
            inverse = 1.0 / jnp.where(nonzero, square, 1.0)
            scale = jnp.where(nonzero, inverse * (0.5 / SHEAR_REF), 0.0)
            inverse = inverse * BETA_REF
            for h in range(2):
                lanes = slice(h * LANES, (h + 1) * LANES)
                tau = [spec_ref[f, branch, rows, lanes] for f in range(6)]
                force_x = tau[0] * wave_x + tau[5] * wave_y + tau[4] * wave_z
                force_y = tau[5] * wave_x + tau[1] * wave_y + tau[3] * wave_z
                force_z = tau[4] * wave_x + tau[3] * wave_y + tau[2] * wave_z
                along = (wave_x * force_x + wave_y * force_y + wave_z * force_z) * inverse
                moved_x = scale * (along * wave_x - force_x)
                moved_y = scale * (along * wave_y - force_y)
                moved_z = scale * (along * wave_z - force_z)
                spec_ref[0, branch, rows, lanes] = (wave_x + wave_x) * moved_x
                spec_ref[1, branch, rows, lanes] = (wave_y + wave_y) * moved_y
                spec_ref[2, branch, rows, lanes] = (wave_z + wave_z) * moved_z
                spec_ref[3, branch, rows, lanes] = wave_y * moved_z + wave_z * moved_y
                spec_ref[4, branch, rows, lanes] = wave_x * moved_z + wave_z * moved_x
                spec_ref[5, branch, rows, lanes] = wave_x * moved_y + wave_y * moved_x

    each(N // 8, BLOCK_UNROLL, block)

    def back(f, slot):
        real, imag = y_back(spec_ref[f, 0], spec_ref[f, 1], ahead_ref)
        x_back(real, imag, f, SWEEP_ROWS, back_ref, plane_ref.at[slot], out_ref)

    each(6, PLANE_UNROLL, back)


def z_drive_kernel(
    in_ref,
    cells_ref,
    back_ref,
    ahead_ref,
    far_ref,
    far_out_ref,
    strain_ref,
    spec_ref,
    drive_ref,
    out_ref,
    sems,
    out_sem,
):
    def far(f):
        return pltpu.make_async_copy(strain_ref.at[f], far_ref.at[f], sems.at[f])

    def inverse(f, slot):
        strain_ref[f] = z_back(in_ref, f, SWEEP_ROWS, back_ref, spec_ref.at[slot])
        far(f).start()

    each(6, DRIVE_UNROLL, inverse)

    rise = -EIGEN_STRAIN * (3.0 * FIRST_RISE + 2.0 * SHEAR_RISE)
    low = -EIGEN_STRAIN * (3.0 * FIRST_LOW + 2.0 * SHEAR_LOW)

    def block(b, slot):
        rows = pl.ds(pl.multiple_of(b * 8, 8), 8)
        conc = cells_ref[rows, :]
        strain = [strain_ref[f, rows, :] for f in range(6)]
        dilation = EIGEN_STRAIN * conc
        part = [strain[f] - dilation for f in range(3)]
        trace = part[0] + part[1] + part[2]
        energy = (
            part[0] * part[0]
            + part[1] * part[1]
            + part[2] * part[2]
            + 2.0 * (strain[3] * strain[3] + strain[4] * strain[4] + strain[5] * strain[5])
        )
        chemical = 2.0 * WELL_HEIGHT * conc * (1.0 - conc) * (1.0 - 2.0 * conc)
        drive_ref[rows, :] = (
            chemical
            + 0.5 * FIRST_RISE * trace * trace
            + SHEAR_RISE * energy
            + (low + rise * conc) * trace
        )

    each(N // 8, BLOCK_UNROLL, block)
    z_ahead(drive_ref[...], 0, DRIVE_ROWS, 2, ahead_ref, out_ref)
    out = pltpu.make_async_copy(out_ref, far_out_ref, out_sem)
    out.start()
    for f in range(6):
        far(f).wait()
    out.wait()


def aside_kernel(
    now_ref,
    then_ref,
    source_ref,
    ahead_ref,
    back_ref,
    strain_ref,
    conc_ref,
    sums_ref,
    cells_ref,
    past_ref,
    data_ref,
    lines_ref,
    plane_ref,
    now_sems,
    then_sems,
    source_sem,
    out_sems,
):
    def now(f):
        return pltpu.make_async_copy(now_ref.at[f], cells_ref.at[f], now_sems.at[f])

    def then(f):
        return pltpu.make_async_copy(then_ref.at[f], past_ref.at[f], then_sems.at[f])

    for f in range(6):
        now(f).start()
        then(f).start()
    source = pltpu.make_async_copy(source_ref, data_ref, source_sem)
    source.start()

    def one(f, totals):
        def block(b, totals):
            rows = pl.ds(pl.multiple_of(b * 8, 8), 8)
            past = past_ref[f, rows, :]
            change = cells_ref[f, rows, :] - past
            return totals[0] + past * past, totals[1] + change * change

        now(f).wait()
        lines_ref[f] = cells_ref[f].T.reshape(LOW, HIGH, LY, N)
        for copy in copy_lines(strain_ref.at[f], lines_ref.at[f], out_sems.at[f], False):
            copy.start()
        then(f).wait()
        return lax.fori_loop(0, N // 8, block, totals)

    zero = jnp.zeros((8, CELLS), F32)
    totals = lax.fori_loop(0, 6, one, (zero, zero))
    lane = lax.broadcasted_iota(jnp.int32, (1, LANES), 1)
    sums = jnp.where(lane < LANES // 2, squares(totals[0]), squares(totals[1]))
    sums_ref[...] = jnp.broadcast_to(sums, (8, LANES))
    source.wait()
    conc_ref[0], conc_ref[1] = plane_spectrum(
        data_ref, 1, SOURCE_ROWS, ahead_ref, back_ref, plane_ref
    )
    for f in range(6):
        for copy in copy_lines(strain_ref.at[f], lines_ref.at[f], out_sems.at[f], False):
            copy.wait()


def plane_update_kernel(
    place_ref, in_ref, conc_ref, sums_ref, ahead_ref, back_ref, out_ref, plane_ref
):
    data = list(plane_spectrum(in_ref, 0, DRIVE_ROWS, ahead_ref, back_ref, plane_ref))
    wave_x = row_waves(0, N)
    wave_z = depth_wave(place_ref, N)
    partial = wave_x * wave_x + wave_z * wave_z
    for b in range(2):
        wave_y = lane_waves(b, N)
        square = partial + wave_y * wave_y
        inverse = 1.0 / (1.0 + TIME_STEP * GRADIENT_ENERGY * square * square)
        drive = TIME_STEP * square * inverse
        data[b] = conc_ref[b] * twice(inverse) - data[b] * twice(drive)
    real, imag = y_back(data[0], data[1], ahead_ref)
    x_back(real, imag, 0, LAST_ROWS, back_ref, plane_ref, out_ref)
    out_ref[peers_of(LOW, LAST_ROWS), :] = jnp.broadcast_to(sums_ref[:1, :], (DEVICES, LANES))


def z_last_kernel(in_ref, back_ref, out_ref, norm_ref, spec_ref, lines_ref, sems):
    lines = z_back(in_ref, 0, LAST_ROWS, back_ref, spec_ref).T
    lines_ref[...] = lines.reshape(LOW, HIGH, LY, N)
    copies = copy_lines(out_ref, lines_ref, sems, False)
    for copy in copies:
        copy.start()
    sums = in_ref[peers_of(LOW, LAST_ROWS), :]
    lane = lax.broadcasted_iota(jnp.int32, sums.shape, 1)
    row = lax.broadcasted_iota(jnp.int32, (8, LANES), 0)
    first = jnp.sum(jnp.where(lane < LANES // 2, sums, 0.0))
    second = jnp.sum(jnp.where(lane < LANES // 2, 0.0, sums))
    norms = jnp.sqrt(jnp.where(row == 0, first, second) * (1.0 / float(N) ** 3))
    norm_ref[0] = norms[0, 0]
    norm_ref[1] = norms[1, 0]
    for copy in copies:
        copy.wait()


SPACES = {"vmem": pltpu.VMEM, "smem": pltpu.SMEM, "hbm": pltpu.HBM}


def call(kernel, name, args, outs, scratch=(), sems=(), mib=24):
    operands = [
        pltpu.with_memory_space_constraint(value, pltpu.HBM) if space == "hbm" else value
        for space, value in args
    ]
    return pl.pallas_call(
        kernel,
        out_shape=[
            pltpu.HBM(shape, F32) if space == "hbm" else jax.ShapeDtypeStruct(shape, *kind or (F32,))
            for space, shape, *kind in outs
        ],
        in_specs=[pl.BlockSpec(memory_space=SPACES[space]) for space, _ in args],
        out_specs=[pl.BlockSpec(memory_space=SPACES[space]) for space, *_ in outs],
        scratch_shapes=[
            *[pltpu.VMEM(s, F32) if isinstance(s, tuple) else s for s in scratch],
            *[pltpu.SemaphoreType.DMA(shape) for shape in sems],
        ],
        name=name,
        interpret=INTERPRET,
        compiler_params=pltpu.CompilerParams(vmem_limit_bytes=mib * 1024 * 1024),
    )(*operands)


def exchange(array):
    rows = array.reshape(DEVICES, array.shape[0] // DEVICES * LANES)
    rows = lax.all_to_all(rows, AXES, split_axis=0, concat_axis=0, tiled=True)
    return rows.reshape(array.shape)


def wire(pitch):
    return (DEVICES * pitch, LANES)


BLOCK = (LX, LY, N)
CELL = (N, CELLS)
PLANE = (2, N, N)
LINES = (LOW, HIGH, LY, N)
SMALL = (8, CELLS)


def shards(concentration):
    tables = [jnp.asarray(table) for table in build_tables()]
    place = ("smem", lax.axis_index(AXES).astype(jnp.int32)[None])

    cells, data, edge, *tables = call(
        source_kernel,
        "source",
        [place, ("hbm", concentration), ("hbm", tables[1]), ("hbm", tables[0])],
        [
            ("vmem", CELL),
            ("vmem", wire(SOURCE_ROWS)),
            ("vmem", SMALL),
            ("vmem", (2, N, N), BF16),
            ("vmem", (3, N, N), BF16),
            ("vmem", (2, 2, N, N), BF16),
            ("vmem", (2, 2, N, N), BF16),
        ],
        [LINES],
        [(HIGH,), (), ()],
    )
    back, ahead, line_ahead, line_back = [("vmem", table) for table in tables]
    source = exchange(data)
    (data,) = call(
        plane_first_kernel,
        "plane_first",
        [place, ("vmem", source), line_ahead, line_back],
        [("vmem", wire(FIRST_ROWS))],
        [(6, *PLANE), (3, *PLANE)],
    )
    data = exchange(data)
    past, data = call(
        z_sweep_kernel,
        "z_sweep",
        [("vmem", data), ("vmem", cells), ("vmem", edge), back, ahead],
        [("hbm", (6, *CELL)), ("vmem", wire(SWEEP_ROWS))],
        [(6, *CELL), (5, *CELL), (6, *CELL)],
        [()],
    )
    data = exchange(data)
    (data,) = call(
        plane_green_kernel,
        "plane_green",
        [place, ("vmem", data), line_ahead, line_back],
        [("vmem", wire(SWEEP_ROWS))],
        [(PLANE_UNROLL, *PLANE), (6, *PLANE)],
    )
    data = exchange(data)
    now, data = call(
        z_drive_kernel,
        "z_drive",
        [("vmem", data), ("vmem", cells), back, ahead],
        [("hbm", (6, *CELL)), ("hbm", wire(DRIVE_ROWS))],
        [(6, *CELL), (DRIVE_UNROLL, *CELL), CELL, wire(DRIVE_ROWS)],
        [(6,), ()],
    )
    data = exchange(data)
    strain, conc_spec, sums = call(
        aside_kernel,
        "aside",
        [("hbm", now), ("hbm", past), ("hbm", source), line_ahead, line_back],
        [("hbm", (6, *BLOCK)), ("vmem", PLANE), ("vmem", (8, LANES))],
        [(6, *CELL), (6, *CELL), wire(SOURCE_ROWS), (6, *LINES), PLANE],
        [(6,), (6,), (), (6, HIGH)],
    )
    (data,) = call(
        plane_update_kernel,
        "plane_update",
        [place, ("vmem", data), ("vmem", conc_spec), ("vmem", sums), line_ahead, line_back],
        [("vmem", wire(LAST_ROWS))],
        [PLANE],
    )
    data = exchange(data)
    conc_next, norms = call(
        z_last_kernel,
        "z_last",
        [("vmem", data), back],
        [("hbm", BLOCK), ("smem", (2,))],
        [CELL, LINES],
        [(HIGH,)],
    )
    return conc_next, strain, norms


def solution(mesh):
    whole = Mesh(mesh.devices.reshape(4, 2, 4, 4), AXES)
    row, col = AXES[:2], AXES[2:]
    return jax.shard_map(
        shards,
        mesh=whole,
        in_specs=(P(row, col, None),),
        out_specs=(P(row, col, None), P(None, row, col, None), P()),
        check_vma=False,
    )
```

```python
import math
from functools import partial

import jax
import jax.numpy as jnp
import numpy as np
from jax import lax
from jax.experimental import pallas as pl
from jax.experimental.pallas import tpu as pltpu
from jax.sharding import Mesh
from jax.sharding import PartitionSpec as P

AXES = ("row_0", "row_1", "col_0", "col_1")

FIRST_LOW = 1.0
FIRST_RISE = 0.6
SHEAR_LOW = 0.7
SHEAR_RISE = 0.8
FIRST_REF = 1.3
SHEAR_REF = 1.1
BETA_REF = 2.4 / 3.5
EIGEN_STRAIN = 0.5
WELL_HEIGHT = 1.0
TIME_STEP = 0.5
GRADIENT_ENERGY = 0.5

N = 256
HALF = N // 2
ROWS = 8
COLS = 16
DEVICES = ROWS * COLS
LX = N // ROWS
LY = N // COLS
LOW = 8
HIGH = LX // LOW
CELLS = LX * LY
LANES = 128
UNIT = 2.0 * math.pi / N
F32 = jnp.float32
BF16 = jnp.bfloat16
INTERPRET = False
PLANE_UNROLL = 6
SWEEP_UNROLL = 3
DRIVE_UNROLL = 6
BLOCK_UNROLL = 4
SOURCE_ROWS = 2 * LOW
FIRST_ROWS = 5 * LOW
SWEEP_ROWS = 6 * LOW
DRIVE_ROWS = LOW
LAST_ROWS = LOW + 1
FIRST_FIELDS = (0, 1, 3, 4, 5)
TRACE = -(1.0 - BETA_REF) / SHEAR_REF


def pieces_of(table, count):
    rest = table.astype(np.float32)
    pieces = []
    for _ in range(count):
        piece = rest.astype(jnp.bfloat16)
        rest = rest - piece.astype(np.float32)
        pieces.append(piece)
    return np.stack(pieces)


def build_tables():
    index = np.arange(N)
    half = np.arange(HALF)
    angle = 2.0 * np.pi / N * (index[:, None] * index[None, :] % N)
    cosine = np.cos(angle)
    sine = np.sin(angle)
    lines = []
    for odd in range(2):
        angle = 2.0 * np.pi / N * ((2 * half[:, None] + odd) * half[None, :] % N)
        lines.append(
            np.block([[np.cos(angle), np.sin(angle)], [-np.sin(angle), np.cos(angle)]])
        )
    line_ahead = np.stack([pieces_of(line, 2) for line in lines])
    ahead = np.concatenate([cosine[:HALF], -sine[:HALF]], axis=0)
    return line_ahead, pieces_of(ahead, 3)


def split(value, count):
    pieces = []
    for i in range(count):
        piece = value.astype(BF16)
        pieces.append(piece)
        if i + 1 < count:
            value = value - piece.astype(F32)
    return pieces


def product(left, right):
    count = len(right)
    total = None
    for order in reversed(range(count)):
        for i in range(order + 1):
            term = jnp.dot(left[i], right[order - i], preferred_element_type=F32)
            total = term if total is None else total + term
    return total


def table(ref):
    return [ref[i] for i in range(ref.shape[0])]


def swap_lanes(parts, granule):
    parts = list(parts)
    axis = parts[0].ndim - 1
    lane = lax.broadcasted_iota(jnp.int32, parts[0].shape, axis)
    step = 1
    while step < len(parts):
        width = granule * step
        low = (lane & width) == 0
        for i in range(len(parts)):
            if i & step == 0:
                a, b = parts[i], parts[i + step]
                if len(parts) > 2 and 2 * width == LANES:
                    moved = pltpu.roll(jnp.where(low, b, a), width, axis)
                    parts[i] = jnp.where(low, a, moved)
                    parts[i + step] = jnp.where(low, moved, b)
                    continue
                parts[i] = jnp.where(low, a, pltpu.roll(b, width, axis))
                parts[i + step] = jnp.where(low, pltpu.roll(a, LANES - width, axis), b)
        step *= 2
    return parts


def peers_of(row, pitch):
    return pl.ds(row, DEVICES, stride=pitch)


def z_ahead(value, f, pitch, pieces, ahead_ref, out_ref):
    spectrum = product(table(ahead_ref), split(value, pieces))
    for t in range(LOW // 2):
        lanes = slice(t * LANES, (t + 1) * LANES)
        parts = swap_lanes([spectrum[:HALF, lanes], spectrum[HALF:, lanes]], LANES // 2)
        for i in range(2):
            out_ref[peers_of(f * LOW + 2 * t + i, pitch), :] = parts[i]


def z_back(in_ref, f, pitch, back_ref, spec_ref):
    for t in range(LOW // 2):
        lanes = slice(t * LANES, (t + 1) * LANES)
        parts = [in_ref[peers_of(f * LOW + 2 * t + i, pitch), :] for i in range(2)]
        real, imag = swap_lanes(parts, LANES // 2)
        spec_ref[:HALF, lanes] = real
        spec_ref[HALF:, lanes] = imag
    return product(table(back_ref), split(spec_ref[...], 2))


def rows_of(peer, f, pitch):
    start = peer * pitch + f * LOW
    return pl.ds(start if isinstance(start, int) else pl.multiple_of(start, LOW), LOW)


def plane_row(part, i, high):
    return part * HALF + i % 4 * LX + high * LOW


def plane_ahead(in_ref, f, pitch, ahead_ref, plane_ref):
    for i in range(ROWS // 2):
        for h in range(2):
            near, far = [
                swap_lanes(
                    [in_ref[rows_of(k * COLS + h * 8 + j, f, pitch), :] for j in range(8)], LY
                )
                for k in (i, i + ROWS // 2)
            ]
            for g in range(8):
                row = plane_row(g // HIGH, i, g % HIGH)
                lanes = slice(h * LANES, (h + 1) * LANES)
                plane_ref[0, row : row + LOW, lanes] = near[g] + far[g]
                plane_ref[1, row : row + LOW, lanes] = near[g] - far[g]
    near, far = [], []
    for b in range(2):
        lines = product(table(ahead_ref.at[b]), split(plane_ref[b], 2))
        near.append(jnp.concatenate([lines[:HALF, :HALF], lines[HALF:, :HALF]], axis=1))
        far.append(jnp.concatenate([lines[:HALF, HALF:], lines[HALF:, HALF:]], axis=1))
    near = jnp.concatenate(near, axis=0)
    far = jnp.concatenate(far, axis=0)
    return near + far, near - far


def plane_spectrum(in_ref, f, pitch, ahead_ref, back_ref, plane_ref):
    even, odd = plane_ahead(in_ref, f, pitch, ahead_ref, plane_ref)
    return (
        product(split(even, 2), table(back_ref.at[0])),
        product(split(odd, 2), table(back_ref.at[1])),
    )


def y_back(even, odd, ahead_ref):
    even = product(split(even, 2), table(ahead_ref.at[0]))
    odd = product(split(odd, 2), table(ahead_ref.at[1]))
    near = even + odd
    far = even - odd
    return (
        jnp.concatenate([near[:, :HALF], far[:, :HALF]], axis=1),
        jnp.concatenate([near[:, HALF:], far[:, HALF:]], axis=1),
    )


def x_back(real, imag, f, pitch, back_ref, plane_ref, out_ref, mark=None):
    lines = []
    for b in range(2):
        rows = slice(b * HALF, (b + 1) * HALF)
        data = jnp.concatenate([real[rows], imag[rows]], axis=0)
        lines.append(product(table(back_ref.at[b]), split(data, 2)))
    plane_ref[0] = lines[0] + lines[1]
    plane_ref[1] = lines[0] - lines[1]
    if mark is not None:
        for half in range(2):
            plane_ref[half, HALF:] = jnp.where(mark[0], mark[1], plane_ref[half, HALF:])
    for i in range(ROWS):
        for h in range(2):
            parts = []
            for g in range(8):
                row = plane_row(g // HIGH, i, g % HIGH)
                parts.append(plane_ref[i // 4, row : row + LOW, h * LANES : (h + 1) * LANES])
            parts = swap_lanes(parts, LY)
            for j in range(8):
                out_ref[rows_of(i * COLS + h * 8 + j, f, pitch), :] = parts[j]


def each(count, unroll, body):
    def step(i, carry):
        for slot in range(unroll):
            body(i * unroll + slot, slot)
        return carry

    if count == unroll:
        step(0, 0)
    else:
        lax.fori_loop(0, count // unroll, step, 0)


def signed(index):
    return jnp.where(index < HALF, index, index - N).astype(F32) * UNIT


def row_waves(start, count):
    row = lax.broadcasted_iota(jnp.int32, (count, LANES), 0) + start
    return signed(2 * (row % HALF) + row // HALF)


def lane_waves(branch, count):
    return signed(2 * lax.broadcasted_iota(jnp.int32, (count, LANES), 1) + branch)


def depth_wave(place_ref, count):
    return jnp.full((count, LANES), place_ref[0], jnp.int32).astype(F32) * UNIT


def twice(half):
    return jnp.concatenate([half, half], axis=1)


def squares(total):
    total = sum(total[:, t * LANES : (t + 1) * LANES] for t in range(CELLS // LANES))
    total = jnp.sum(total, axis=0, keepdims=True)
    return total + pltpu.roll(total, LANES // 2, 1)


def source_of(conc):
    rise = -EIGEN_STRAIN * (3.0 * FIRST_RISE + 2.0 * SHEAR_RISE)
    low = -EIGEN_STRAIN * (3.0 * FIRST_LOW + 2.0 * SHEAR_LOW)
    return (low + rise * conc) * conc


def copy_lines(far, lines_ref, sems, inward):
    copies = []
    for high in range(HIGH):
        pair = (far.at[pl.ds(high * LOW, LOW)], lines_ref.at[:, high])
        source, target = pair if inward else pair[::-1]
        copies.append(pltpu.make_async_copy(source, target, sems.at[high]))
    return copies


def source_kernel(
    place_ref,
    conc_ref,
    far_ref,
    far_line_ref,
    cells_ref,
    out_ref,
    edge_ref,
    back_ref,
    ahead_ref,
    line_ref,
    line_back_ref,
    lines_ref,
    sems,
    far_sem,
    line_sem,
):
    copies = copy_lines(conc_ref, lines_ref, sems, True)
    copies.append(pltpu.make_async_copy(far_ref, ahead_ref, far_sem))
    line = pltpu.make_async_copy(far_line_ref, line_ref, line_sem)
    for copy in copies:
        copy.start()
    line.start()
    for copy in copies:
        copy.wait()
    conc = lines_ref[...].reshape(CELLS, N).T
    cells_ref[...] = conc
    source = source_of(conc)
    total = jnp.sum(source.reshape(N // 8, 8, CELLS), axis=0)
    row = lax.broadcasted_iota(jnp.int32, (8, CELLS), 0)
    edge = jnp.where(row % 2 == 0, total, -total)
    edge = jnp.sum(edge, axis=0, keepdims=True) * (1.0 / N)
    edge_ref[...] = jnp.where(row % 2 == 0, edge, -edge)
    z_ahead(source, 0, SOURCE_ROWS, 3, ahead_ref, out_ref)
    z_ahead(conc, 1, SOURCE_ROWS, 2, ahead_ref, out_ref)
    lane = lax.broadcasted_iota(jnp.int32, (N, N), 1)
    weight = jnp.where(lane % HALF == 0, 1.0, 2.0) * (1.0 / float(N) ** 3)
    for i in range(2):
        back_ref[i] = (ahead_ref[i].astype(F32).T * weight).astype(BF16)
    line.wait()
    for b in range(2):
        for i in range(2):
            line_back_ref[b, i] = line_ref[b, i].astype(F32).T.astype(BF16)


def plane_first_kernel(
    place_ref, in_ref, ahead_ref, back_ref, out_ref, plane_ref, line_ref
):
    data = list(plane_spectrum(in_ref, 0, SOURCE_ROWS, ahead_ref, back_ref, plane_ref.at[5]))
    mean = jnp.broadcast_to(data[0][:1, :1] * (1.0 / float(N) ** 3), (HALF, N))
    bottom = jnp.full((HALF, N), place_ref[0], jnp.int32) == 0
    wave_x = row_waves(0, N)
    wave_z = depth_wave(place_ref, N)
    wave_y = []
    partial = wave_x * wave_x + wave_z * wave_z
    for b in range(2):
        wave = lane_waves(b, N)
        wave_y.append(twice(wave))
        square = partial + wave * wave
        nonzero = square > 0.0
        safe = jnp.where(nonzero, square, 1.0)
        data[b] = data[b] * twice(jnp.where(nonzero, TRACE / safe, 0.0))
    for power in range(3):
        if power:
            data = [data[b] * wave_y[b] for b in range(2)]
        line_ref[power, 0], line_ref[power, 1] = y_back(data[0], data[1], ahead_ref)
    plan = ((2, 0, 0), (0, 2, 0), (0, 1, 1), (1, 0, 1), (1, 1, 0))
    for f, (power_x, power_y, power_z) in enumerate(plan):
        real = line_ref[power_y, 0]
        imag = line_ref[power_y, 1]
        factor = None
        for wave in [wave_x] * power_x + [wave_z] * power_z:
            factor = wave if factor is None else factor * wave
        if factor is not None:
            real = real * twice(factor)
            imag = imag * twice(factor)
        mark = (bottom, mean) if f == 0 else None
        x_back(real, imag, f, FIRST_ROWS, back_ref, plane_ref.at[f], out_ref, mark)


def z_sweep_kernel(
    in_ref,
    cells_ref,
    edge_ref,
    back_ref,
    ahead_ref,
    past_ref,
    out_ref,
    strain_ref,
    spec_ref,
    tau_ref,
    sem,
):
    for f, component in enumerate(FIRST_FIELDS):
        spec = spec_ref.at[f]
        strain_ref[component] = z_back(in_ref, f, FIRST_ROWS, back_ref, spec)

    mean = in_ref[:LOW, :]
    lane = lax.broadcasted_iota(jnp.int32, mean.shape, 1)
    mean = jnp.where(lane < LANES // 2, pltpu.roll(mean, LANES // 2, 1), mean)
    mean = jnp.concatenate([mean] * (CELLS // LANES), axis=1)

    def block(b, slot):
        rows = pl.ds(pl.multiple_of(b * 8, 8), 8)
        conc = cells_ref[rows, :]
        source = source_of(conc) - mean
        trace = TRACE * (source - edge_ref[...])
        strain = [strain_ref[f, rows, :] for f in range(6) if f != 2]
        strain.insert(2, trace - strain[0] - strain[1])
        strain_ref[2, rows, :] = strain[2]
        normal = ((FIRST_LOW - FIRST_REF) + FIRST_RISE * conc) * trace + source
        excess = 2.0 * (SHEAR_LOW - SHEAR_REF) + 2.0 * SHEAR_RISE * conc
        for f in range(6):
            tau = excess * strain[f]
            tau_ref[f, rows, :] = tau + normal if f < 3 else tau

    each(N // 8, BLOCK_UNROLL, block)
    past = pltpu.make_async_copy(strain_ref, past_ref, sem)
    past.start()

    def ahead(f, slot):
        z_ahead(tau_ref[f], f, SWEEP_ROWS, 2, ahead_ref, out_ref)

    each(6, SWEEP_UNROLL, ahead)
    past.wait()


def plane_green_kernel(place_ref, in_ref, ahead_ref, back_ref, out_ref, plane_ref, spec_ref):
    def ahead(f, slot):
        spec_ref[f, 0], spec_ref[f, 1] = plane_spectrum(
            in_ref, f, SWEEP_ROWS, ahead_ref, back_ref, plane_ref.at[slot]
        )

    each(6, PLANE_UNROLL, ahead)

    waves_y = [lane_waves(branch, 8) for branch in range(2)]
    wave_z = depth_wave(place_ref, 8)

    def block(b, slot):
        start = pl.multiple_of(b * 8, 8)
        rows = pl.ds(start, 8)
        wave_x = row_waves(start, 8)
        partial = wave_x * wave_x + wave_z * wave_z
        for branch in range(2):
            wave_y = waves_y[branch]
            square = partial + wave_y * wave_y
            nonzero = square > 0.0
            inverse = 1.0 / jnp.where(nonzero, square, 1.0)
            scale = jnp.where(nonzero, inverse * (0.5 / SHEAR_REF), 0.0)
            inverse = inverse * BETA_REF
            for h in range(2):
                lanes = slice(h * LANES, (h + 1) * LANES)
                tau = [spec_ref[f, branch, rows, lanes] for f in range(6)]
                force_x = tau[0] * wave_x + tau[5] * wave_y + tau[4] * wave_z
                force_y = tau[5] * wave_x + tau[1] * wave_y + tau[3] * wave_z
                force_z = tau[4] * wave_x + tau[3] * wave_y + tau[2] * wave_z
                along = (wave_x * force_x + wave_y * force_y + wave_z * force_z) * inverse
                moved_x = scale * (along * wave_x - force_x)
                moved_y = scale * (along * wave_y - force_y)
                moved_z = scale * (along * wave_z - force_z)
                spec_ref[0, branch, rows, lanes] = (wave_x + wave_x) * moved_x
                spec_ref[1, branch, rows, lanes] = (wave_y + wave_y) * moved_y
                spec_ref[2, branch, rows, lanes] = (wave_z + wave_z) * moved_z
                spec_ref[3, branch, rows, lanes] = wave_y * moved_z + wave_z * moved_y
                spec_ref[4, branch, rows, lanes] = wave_x * moved_z + wave_z * moved_x
                spec_ref[5, branch, rows, lanes] = wave_x * moved_y + wave_y * moved_x

    each(N // 8, BLOCK_UNROLL, block)

    def back(f, slot):
        real, imag = y_back(spec_ref[f, 0], spec_ref[f, 1], ahead_ref)
        x_back(real, imag, f, SWEEP_ROWS, back_ref, plane_ref.at[slot], out_ref)

    each(6, PLANE_UNROLL, back)


def z_drive_kernel(
    in_ref,
    cells_ref,
    back_ref,
    ahead_ref,
    far_ref,
    far_out_ref,
    strain_ref,
    spec_ref,
    drive_ref,
    out_ref,
    sems,
    out_sem,
):
    def far(f):
        return pltpu.make_async_copy(strain_ref.at[f], far_ref.at[f], sems.at[f])

    def inverse(f, slot):
        strain_ref[f] = z_back(in_ref, f, SWEEP_ROWS, back_ref, spec_ref.at[slot])
        far(f).start()

    each(6, DRIVE_UNROLL, inverse)

    rise = -EIGEN_STRAIN * (3.0 * FIRST_RISE + 2.0 * SHEAR_RISE)
    low = -EIGEN_STRAIN * (3.0 * FIRST_LOW + 2.0 * SHEAR_LOW)

    def block(b, slot):
        rows = pl.ds(pl.multiple_of(b * 8, 8), 8)
        conc = cells_ref[rows, :]
        strain = [strain_ref[f, rows, :] for f in range(6)]
        dilation = EIGEN_STRAIN * conc
        part = [strain[f] - dilation for f in range(3)]
        trace = part[0] + part[1] + part[2]
        energy = (
            part[0] * part[0]
            + part[1] * part[1]
            + part[2] * part[2]
            + 2.0 * (strain[3] * strain[3] + strain[4] * strain[4] + strain[5] * strain[5])
        )
        chemical = 2.0 * WELL_HEIGHT * conc * (1.0 - conc) * (1.0 - 2.0 * conc)
        drive_ref[rows, :] = (
            chemical
            + 0.5 * FIRST_RISE * trace * trace
            + SHEAR_RISE * energy
            + (low + rise * conc) * trace
        )

    each(N // 8, BLOCK_UNROLL, block)
    z_ahead(drive_ref[...], 0, DRIVE_ROWS, 2, ahead_ref, out_ref)
    out = pltpu.make_async_copy(out_ref, far_out_ref, out_sem)
    out.start()
    for f in range(6):
        far(f).wait()
    out.wait()


def aside_kernel(
    now_ref,
    then_ref,
    source_ref,
    ahead_ref,
    back_ref,
    strain_ref,
    conc_ref,
    sums_ref,
    cells_ref,
    past_ref,
    data_ref,
    lines_ref,
    plane_ref,
    now_sems,
    then_sems,
    source_sem,
    out_sems,
):
    def now(f):
        return pltpu.make_async_copy(now_ref.at[f], cells_ref.at[f], now_sems.at[f])

    def then(f):
        return pltpu.make_async_copy(then_ref.at[f], past_ref.at[f], then_sems.at[f])

    for f in range(6):
        now(f).start()
        then(f).start()
    source = pltpu.make_async_copy(source_ref, data_ref, source_sem)
    source.start()

    def one(f, totals):
        def block(b, totals):
            rows = pl.ds(pl.multiple_of(b * 8, 8), 8)
            past = past_ref[f, rows, :]
            change = cells_ref[f, rows, :] - past
            return totals[0] + past * past, totals[1] + change * change

        now(f).wait()
        lines_ref[f] = cells_ref[f].T.reshape(LOW, HIGH, LY, N)
        for copy in copy_lines(strain_ref.at[f], lines_ref.at[f], out_sems.at[f], False):
            copy.start()
        then(f).wait()
        return lax.fori_loop(0, N // 8, block, totals)

    zero = jnp.zeros((8, CELLS), F32)
    totals = lax.fori_loop(0, 6, one, (zero, zero))
    lane = lax.broadcasted_iota(jnp.int32, (1, LANES), 1)
    sums = jnp.where(lane < LANES // 2, squares(totals[0]), squares(totals[1]))
    sums_ref[...] = jnp.broadcast_to(sums, (8, LANES))
    source.wait()
    conc_ref[0], conc_ref[1] = plane_spectrum(
        data_ref, 1, SOURCE_ROWS, ahead_ref, back_ref, plane_ref
    )
    for f in range(6):
        for copy in copy_lines(strain_ref.at[f], lines_ref.at[f], out_sems.at[f], False):
            copy.wait()


def plane_update_kernel(
    place_ref, in_ref, conc_ref, sums_ref, ahead_ref, back_ref, out_ref, plane_ref
):
    data = list(plane_spectrum(in_ref, 0, DRIVE_ROWS, ahead_ref, back_ref, plane_ref))
    wave_x = row_waves(0, N)
    wave_z = depth_wave(place_ref, N)
    partial = wave_x * wave_x + wave_z * wave_z
    for b in range(2):
        wave_y = lane_waves(b, N)
        square = partial + wave_y * wave_y
        inverse = 1.0 / (1.0 + TIME_STEP * GRADIENT_ENERGY * square * square)
        drive = TIME_STEP * square * inverse
        data[b] = conc_ref[b] * twice(inverse) - data[b] * twice(drive)
    real, imag = y_back(data[0], data[1], ahead_ref)
    x_back(real, imag, 0, LAST_ROWS, back_ref, plane_ref, out_ref)
    out_ref[peers_of(LOW, LAST_ROWS), :] = jnp.broadcast_to(sums_ref[:1, :], (DEVICES, LANES))


def z_last_kernel(in_ref, back_ref, out_ref, norm_ref, spec_ref, lines_ref, sems):
    lines = z_back(in_ref, 0, LAST_ROWS, back_ref, spec_ref).T
    lines_ref[...] = lines.reshape(LOW, HIGH, LY, N)
    copies = copy_lines(out_ref, lines_ref, sems, False)
    for copy in copies:
        copy.start()
    sums = in_ref[peers_of(LOW, LAST_ROWS), :]
    lane = lax.broadcasted_iota(jnp.int32, sums.shape, 1)
    row = lax.broadcasted_iota(jnp.int32, (8, LANES), 0)
    first = jnp.sum(jnp.where(lane < LANES // 2, sums, 0.0))
    second = jnp.sum(jnp.where(lane < LANES // 2, 0.0, sums))
    norms = jnp.sqrt(jnp.where(row == 0, first, second) * (1.0 / float(N) ** 3))
    norm_ref[0] = norms[0, 0]
    norm_ref[1] = norms[1, 0]
    for copy in copies:
        copy.wait()


SPACES = {"vmem": pltpu.VMEM, "smem": pltpu.SMEM, "hbm": pltpu.HBM}


def call(kernel, name, args, outs, scratch=(), sems=(), mib=24):
    operands = [
        pltpu.with_memory_space_constraint(value, pltpu.HBM) if space == "hbm" else value
        for space, value in args
    ]
    return pl.pallas_call(
        kernel,
        out_shape=[
            pltpu.HBM(shape, F32) if space == "hbm" else jax.ShapeDtypeStruct(shape, *kind or (F32,))
            for space, shape, *kind in outs
        ],
        in_specs=[pl.BlockSpec(memory_space=SPACES[space]) for space, _ in args],
        out_specs=[pl.BlockSpec(memory_space=SPACES[space]) for space, *_ in outs],
        scratch_shapes=[
            *[pltpu.VMEM(s, F32) if isinstance(s, tuple) else s for s in scratch],
            *[pltpu.SemaphoreType.DMA(shape) for shape in sems],
        ],
        name=name,
        interpret=INTERPRET,
        compiler_params=pltpu.CompilerParams(vmem_limit_bytes=mib * 1024 * 1024),
    )(*operands)


def exchange(array):
    rows = array.reshape(DEVICES, array.shape[0] // DEVICES * LANES)
    rows = lax.all_to_all(rows, AXES, split_axis=0, concat_axis=0, tiled=True)
    return rows.reshape(array.shape)


def wire(pitch):
    return (DEVICES * pitch, LANES)


BLOCK = (LX, LY, N)
CELL = (N, CELLS)
PLANE = (2, N, N)
LINES = (LOW, HIGH, LY, N)
SMALL = (8, CELLS)


def shards(concentration):
    tables = [jnp.asarray(table) for table in build_tables()]
    place = ("smem", lax.axis_index(AXES).astype(jnp.int32)[None])

    cells, data, edge, *tables = call(
        source_kernel,
        "source",
        [place, ("hbm", concentration), ("hbm", tables[1]), ("hbm", tables[0])],
        [
            ("vmem", CELL),
            ("vmem", wire(SOURCE_ROWS)),
            ("vmem", SMALL),
            ("vmem", (2, N, N), BF16),
            ("vmem", (3, N, N), BF16),
            ("vmem", (2, 2, N, N), BF16),
            ("vmem", (2, 2, N, N), BF16),
        ],
        [LINES],
        [(HIGH,), (), ()],
    )
    back, ahead, line_ahead, line_back = [("vmem", table) for table in tables]
    source = exchange(data)
    (data,) = call(
        plane_first_kernel,
        "plane_first",
        [place, ("vmem", source), line_ahead, line_back],
        [("vmem", wire(FIRST_ROWS))],
        [(6, *PLANE), (3, *PLANE)],
    )
    data = exchange(data)
    past, data = call(
        z_sweep_kernel,
        "z_sweep",
        [("vmem", data), ("vmem", cells), ("vmem", edge), back, ahead],
        [("hbm", (6, *CELL)), ("vmem", wire(SWEEP_ROWS))],
        [(6, *CELL), (5, *CELL), (6, *CELL)],
        [()],
    )
    data = exchange(data)
    (data,) = call(
        plane_green_kernel,
        "plane_green",
        [place, ("vmem", data), line_ahead, line_back],
        [("vmem", wire(SWEEP_ROWS))],
        [(PLANE_UNROLL, *PLANE), (6, *PLANE)],
    )
    data = exchange(data)
    now, data = call(
        z_drive_kernel,
        "z_drive",
        [("vmem", data), ("vmem", cells), back, ahead],
        [("hbm", (6, *CELL)), ("hbm", wire(DRIVE_ROWS))],
        [(6, *CELL), (DRIVE_UNROLL, *CELL), CELL, wire(DRIVE_ROWS)],
        [(6,), ()],
    )
    data = exchange(data)
    strain, conc_spec, sums = call(
        aside_kernel,
        "aside",
        [("hbm", now), ("hbm", past), ("hbm", source), line_ahead, line_back],
        [("hbm", (6, *BLOCK)), ("vmem", PLANE), ("vmem", (8, LANES))],
        [(6, *CELL), (6, *CELL), wire(SOURCE_ROWS), (6, *LINES), PLANE],
        [(6,), (6,), (), (6, HIGH)],
    )
    (data,) = call(
        plane_update_kernel,
        "plane_update",
        [place, ("vmem", data), ("vmem", conc_spec), ("vmem", sums), line_ahead, line_back],
        [("vmem", wire(LAST_ROWS))],
        [PLANE],
    )
    data = exchange(data)
    conc_next, norms = call(
        z_last_kernel,
        "z_last",
        [("vmem", data), back],
        [("hbm", BLOCK), ("smem", (2,))],
        [CELL, LINES],
        [(HIGH,)],
    )
    return conc_next, strain, norms


def solution(mesh):
    whole = Mesh(mesh.devices.reshape(4, 2, 4, 4), AXES)
    row, col = AXES[:2], AXES[2:]
    return jax.shard_map(
        shards,
        mesh=whole,
        in_specs=(P(row, col, None),),
        out_specs=(P(row, col, None), P(None, row, col, None), P()),
        check_vma=False,
    )
```
